32 devices in a mesh: cuts: 2 (over x), wide: 8 (over z, y), narrow: 2 (over core).
Axes of the slice: x: 2, y: 2, z: 4, core: 2. Of those that a mesh axis runs over, the one named last changes fastest.
Arguments:
- stem_tensor: float32 [2, 16384, 512], P(None, ('cuts', 'wide', 'narrow')), parts along dimension 1, may hold values from -6 to 6
- leaves: bfloat16 [16, 4, 2, 512, 512], P(('cuts', 'wide')), parts along dimension 0, may hold values from -1 to 1
- root_devices: int32 [4], replicated, may hold values from 0 to 7, as said below
- mode_orders: int32 [4, 9], replicated, may hold values from 0 to 8, each once within a row
Outputs:
- contracted: float32 [2, 16384, 512], P(None, ('cuts', 'wide', 'narrow')), parts along dimension 1
The draws below stay inside these ranges and needn't reach their ends.
There are 2 independent parts, one for each index of `cuts`. The reference program is written for one: setup_inputs(seed, part) draws one part's arguments, and reference() takes and returns one part's arrays. A program takes and returns all parts, laid end to end along the dimension named above; an argument that names none is the same for every part. Nothing has to cross between parts.
Inputs may be any that keep to these rules, and one draw needn't show every extreme that they name: `root_devices`: the roots include 0, 4 and 7. `mode_orders`: each row holds every number of 0 to 8 once.
All inputs are finite; a program needn't handle non-finite values.
Results may differ from the reference program's by a relative error of at most 0.0081.
Values may be sent and summed in bfloat16 or wider, within the bound.
A program may use at most 64 MiB of HBM per device.

```python
import math
import jax
import jax.numpy as jnp
from jax import lax

MODES = 9
BRANCH = 512
ROWS_DEV = 512
STEPS = 4
ROWS = 8192
N_WIDE = 8
N_NARROW = 2


def draw_root_devices(key, part):
    order = jax.random.permutation(jax.random.fold_in(key, 11), STEPS)
    extra = jax.random.randint(jax.random.fold_in(key, 12), (STEPS,), 0, N_WIDE, dtype=jnp.int32)
    position = jnp.arange(STEPS, dtype=jnp.int32)
    fixed_roots = jnp.where(position == 0, 0, jnp.where(position == 1, N_WIDE // 2, N_WIDE - 1)).astype(jnp.int32)
    chosen = jnp.where(position < 3, fixed_roots, extra).astype(jnp.int32)
    return chosen[order].astype(jnp.int32)


def phase_pair(key, count):
    angles = jax.random.uniform(key, (count,), jnp.float32, -math.pi, math.pi)
    return (jnp.cos(angles), jnp.sin(angles))


def unitary_leaf(key):
    count = BRANCH
    index = jnp.arange(count, dtype=jnp.int32)
    table = index[:, None] * index[None, :] % count
    angle = table.astype(jnp.float32) * (2.0 * math.pi / count)
    scale = 1.0 / math.sqrt(count)
    fourier_re = jnp.cos(angle) * scale
    fourier_im = -jnp.sin(angle) * scale
    first_re, first_im = phase_pair(jax.random.fold_in(key, 1), count)
    middle_re, middle_im = phase_pair(jax.random.fold_in(key, 2), count)
    last_re, last_im = phase_pair(jax.random.fold_in(key, 3), count)
    shuffle = jax.random.permutation(jax.random.fold_in(key, 4), count)
    right_re = fourier_re * last_re[None, :] - fourier_im * last_im[None, :]
    right_im = fourier_re * last_im[None, :] + fourier_im * last_re[None, :]
    right_re = right_re[shuffle]
    right_im = right_im[shuffle]
    moved_re = middle_re[:, None] * right_re - middle_im[:, None] * right_im
    moved_im = middle_re[:, None] * right_im + middle_im[:, None] * right_re
    highest = lax.Precision.HIGHEST
    product_re = jnp.dot(fourier_re, moved_re, precision=highest) - jnp.dot(fourier_im, moved_im, precision=highest)
    product_im = jnp.dot(fourier_re, moved_im, precision=highest) + jnp.dot(fourier_im, moved_re, precision=highest)
    final_re = first_re[:, None] * product_re - first_im[:, None] * product_im
    final_im = first_re[:, None] * product_im + first_im[:, None] * product_re
    return jnp.clip(jnp.stack([final_re, final_im]), -1.0, 1.0)


def draw_leaves(key, part):
    keys = jax.random.split(jax.random.fold_in(key, 21), N_WIDE * STEPS)
    matrices = lax.map(unitary_leaf, keys)
    return matrices.reshape(N_WIDE, STEPS, 2, BRANCH, BRANCH).astype(jnp.bfloat16)


def shard_levels(key, dims, cuts, least, top_value):
    def one(dim, parts):
        draws = jax.random.uniform(jax.random.fold_in(jax.random.fold_in(key, 6), dim), (parts,), jnp.float32, least / len(cuts), top_value / len(cuts))
        return jnp.repeat(jnp.exp(draws), dims[dim] // parts).reshape((-1,) + (1,) * (len(dims) - dim - 1))

    loudness = one(*cuts[0])
    for cut in cuts[1:]:
        loudness = loudness * one(*cut)
    return loudness


def scatter_about(own_key, extent, width, most, cuts=(), held_as=jnp.bfloat16):
    array = width * jax.random.normal(own_key, extent, jnp.float32)
    if cuts:
        array = array * shard_levels(own_key, extent, cuts, -0.22, 0.18)
    return jnp.clip(array, -most, most).astype(held_as)


def setup_inputs(seed: int = 0, part: int = 0) -> dict:
    key_of = jax.random.split(jax.random.key(seed), 5)
    own_keys = jax.random.split(jax.random.fold_in(key_of[4], part), 5)
    stem_tensor = scatter_about(own_keys[0], (2, ROWS, BRANCH), 1.0, 6.0, ((1, 16),), jnp.float32)
    leaves = draw_leaves(jax.random.fold_in(jax.random.fold_in(key_of[4], part), 71), part)
    root_devices = draw_root_devices(jax.random.fold_in(key_of[4], 71), part)
    mode_orders = jax.vmap(lambda own: jax.random.permutation(own, MODES))(jax.random.split(key_of[3], STEPS)).reshape((STEPS, MODES)).astype(jnp.int32)
    return {"stem_tensor": stem_tensor, "leaves": leaves, "root_devices": root_devices, "mode_orders": mode_orders}


def complex_product(left_matrix, right_matrix, precision=None):
    real_part = jnp.dot(left_matrix[0], right_matrix[0], preferred_element_type=jnp.float32, precision=precision) - jnp.dot(left_matrix[1], right_matrix[1], preferred_element_type=jnp.float32, precision=precision)
    imag_part = jnp.dot(left_matrix[0], right_matrix[1], preferred_element_type=jnp.float32, precision=precision) + jnp.dot(left_matrix[1], right_matrix[0], preferred_element_type=jnp.float32, precision=precision)
    return jnp.stack([real_part, imag_part])


def column_source(order_row, branch_width):
    column = jnp.arange(branch_width, dtype=jnp.int32)
    mode_count = order_row.shape[0]
    powers = jnp.left_shift(jnp.int32(1), jnp.arange(mode_count, dtype=jnp.int32))
    bit_table = (column[:, None] // powers[None, :]) % 2
    weights = jnp.left_shift(jnp.int32(1), order_row.astype(jnp.int32))
    return jnp.sum(bit_table * weights[None, :], axis=1).astype(jnp.int32)


def reference(stem_tensor, leaves, root_devices, mode_orders):
    network = stem_tensor
    for step_index in range(STEPS):
        group_start = (root_devices[step_index] // 4 * 4).astype(jnp.int32)
        leaf_group = lax.dynamic_slice_in_dim(leaves, group_start, 4, 0)[:, step_index]
        pair_low = complex_product(leaf_group[0], leaf_group[1]).astype(jnp.bfloat16)
        pair_high = complex_product(leaf_group[2], leaf_group[3]).astype(jnp.bfloat16)
        branch = complex_product(pair_low, pair_high)
        ordered = jnp.take(branch, column_source(mode_orders[step_index], BRANCH), axis=2)
        network = complex_product(network, ordered, lax.Precision.HIGHEST)
        if step_index % 2 == 0:
            stem_view = network.reshape(2, N_WIDE, N_NARROW, ROWS_DEV, N_NARROW, BRANCH // N_NARROW)
            network = jnp.swapaxes(stem_view, 2, 4).reshape(network.shape)
    return network
```

```python
import functools

import jax
import jax.numpy as jnp
from jax import lax
from jax.experimental import pallas as pl
from jax.experimental.pallas import tpu as pltpu
from jax.sharding import PartitionSpec as P

GROUP = 4
CHUNKS = 8
FLIGHT = 2
TILE = 128
BF16 = jnp.bfloat16
F32 = jnp.float32


def dot(x, y):
    return jnp.dot(x, y, preferred_element_type=F32)


def complex_product(ar, ai, br, bi):
    left = jnp.concatenate([ar, ai], axis=1)
    return (
        dot(left, jnp.concatenate([br, -bi], axis=0)),
        dot(left, jnp.concatenate([bi, br], axis=0)),
    )


def remote(src, dst, send_sem, recv_sem, device):
    return pltpu.make_async_remote_copy(
        src_ref=src,
        dst_ref=dst,
        send_sem=send_sem,
        recv_sem=recv_sem,
        device_id=device,
        device_id_type=pl.DeviceIdType.MESH,
    )


def kernel(
    rounds, roots, orders, stem_in, leaves_in, net_out, last_out,
    leaf, pair, away, high, chosen, held, crossed, branches, stem, net1, net2, net3, swap,
    local_sem, leaf_s, leaf_r, fwd_s, fwd_r, pair_s, pair_r, high_s, high_r,
    cross_s, cross_r, z_s, z_r, y_s, y_r, core_s, core_r, swap_s, swap_r,
):
    width = stem.shape[2]
    rows = stem.shape[1]
    half = width // 2
    part = half // CHUNKS
    core = lax.axis_index("narrow")
    wide = lax.axis_index("wide")
    member = wide % GROUP
    y = member % 2
    z = member // 2
    other = {"narrow": 1 - core}
    over_y = {"wide": wide + 1 - 2 * y}
    over_z = {"wide": wide + 2 - 4 * z}
    bits = [(wide // (GROUP << r)) % 2 for r in range(rounds)]
    over_group = [{"wide": wide + (GROUP << r) * (1 - 2 * bits[r])} for r in range(rounds)]

    barrier = pltpu.get_barrier_semaphore()
    for peer in [other, over_y, over_z] + over_group:
        pl.semaphore_signal(barrier, inc=1, device_id=peer, device_id_type=pl.DeviceIdType.MESH)
    own_rows = pl.ds(pl.multiple_of(core * half, half), half)
    own_copies = [
        pltpu.make_async_copy(leaves_in.at[0, 2 * s + y], leaf.at[s, y], local_sem.at[s])
        for s in range(2)
    ]
    stem_copy = pltpu.make_async_copy(stem_in, stem, local_sem.at[2])
    pl.semaphore_wait(barrier, 3 + rounds)

    phases = [1 - z, z]
    leaf_copies = []
    for i, s in enumerate(phases):
        copy = remote(
            leaves_in.at[0, 2 * s + 1 - y, :, own_rows],
            leaf.at[s, y, :, own_rows],
            leaf_s.at[i], leaf_r.at[i], over_y,
        )
        leaf_copies.append(copy)
    leaf_copies[0].start()
    for copy in own_copies:
        copy.start()
    stem_copy.start()

    def choose(i, carry):
        column = lax.broadcasted_iota(jnp.int32, (TILE, width), 1)
        source = jnp.zeros((TILE, width), jnp.int32)
        for b in range(orders.shape[1]):
            weight = jnp.left_shift(jnp.int32(1), orders[member, b])
            source = source + (jnp.right_shift(column, b) & 1) * weight
        row = lax.broadcasted_iota(jnp.int32, (TILE, width), 0) + i * TILE
        at = pl.ds(pl.multiple_of(i * TILE, TILE), TILE)
        chosen[at] = jnp.where(row == source, 1.0, 0.0).astype(F32).astype(BF16)
        return carry

    lax.fori_loop(0, width // TILE, choose, 0)
    for copy in own_copies:
        copy.wait()

    pair_copy = remote(away, pair.at[z], pair_s, pair_r, over_z)
    leaf_copies[0].wait_send()
    leaf_copies[1].start()
    for i, s in enumerate(phases):
        leaf_copies[i].wait_recv()
        forward = remote(
            leaf.at[s, 1 - y, :, own_rows], leaf.at[s, 1 - y, :, own_rows],
            fwd_s.at[i], fwd_r.at[i], other,
        )
        forward.start()
        forward.wait()

        def pair_tile(t, carry, s=s, i=i):
            at = pl.ds(pl.multiple_of(t * half, half), half)
            real, imag = complex_product(
                leaf[s, 0, 0, own_rows], leaf[s, 0, 1, own_rows],
                leaf[s, 1, 0, :, at], leaf[s, 1, 1, :, at],
            )
            target = away if i == 0 else pair.at[z]
            target[0, :, at] = real.astype(BF16)
            target[1, :, at] = imag.astype(BF16)
            return carry

        lax.fori_loop(0, width // half, pair_tile, 0)
        if i == 0:
            pair_copy.start()
    pair_copy.wait_recv()

    def high_tile(t, carry):
        at = pl.ds(pl.multiple_of(t * half, half), half)
        for c in range(2):
            high[c, own_rows, at] = dot(pair[1, c], chosen[:, at]).astype(BF16)
        return carry

    lax.fori_loop(0, width // half, high_tile, 0)
    high_copy = remote(high.at[:, own_rows], high.at[:, own_rows], high_s, high_r, other)
    high_copy.start()
    high_copy.wait()

    def rows_of(c):
        return pl.ds(pl.multiple_of(core * half + c * part, part), part)

    def cross_copy(r, c):
        return remote(held.at[r, c], crossed.at[r, c], cross_s.at[r, c], cross_r.at[r, c], over_group[r])

    def place(origin, c):
        return branches.at[origin, :, rows_of(c)]

    origins = [member, member + 2 - 4 * z, member + 1 - 2 * y, GROUP - 1 - member]

    def z_copy(c):
        return remote(place(origins[0], c), place(origins[0], c), z_s.at[c], z_r.at[c], over_z)

    def y_copy(i, c):
        return remote(place(origins[i], c), place(origins[i], c), y_s.at[i, c], y_r.at[i, c], over_y)

    def core_copy(i, c):
        return remote(place(origins[i], c), place(origins[i], c), core_s.at[i, c], core_r.at[i, c], other)

    def spread(c):
        z_copy(c).start()
        y_copy(0, c).start()
        core_copy(0, c).start()

    def select(r, c):
        cross_copy(r, c).wait_recv()
        cross_copy(r, c).wait_send()
        if c + FLIGHT < CHUNKS:
            cross_copy(r, c + FLIGHT).start()
        root_bit = (roots[member] // (GROUP << r)) % 2
        for p in range(2):
            here = held[r, c, p].astype(F32)
            there = crossed[r, c, p].astype(F32)
            same = jnp.full(here.shape, root_bit, jnp.int32) == bits[r]
            picked = jnp.where(same, here, there).astype(BF16)
            if r + 1 < rounds:
                held[r + 1, c, p] = picked
            else:
                branches[member, p, rows_of(c)] = picked
        if r + 1 < rounds:
            if c < FLIGHT:
                cross_copy(r + 1, c).start()
        else:
            spread(c)

    def on_z(c):
        z_copy(c).wait_recv()
        y_copy(1, c).start()
        core_copy(1, c).start()

    def on_y(i, c):
        y_copy(i, c).wait_recv()
        core_copy(2 + i, c).start()

    for c in range(CHUNKS):
        at = pl.ds(c * part, part)
        real, imag = complex_product(pair[0, 0, at], pair[0, 1, at], high[0], high[1])
        if rounds:
            held[0, c, 0] = real.astype(BF16)
            held[0, c, 1] = imag.astype(BF16)
            if c < FLIGHT:
                cross_copy(0, c).start()
        else:
            branches[member, 0, rows_of(c)] = real.astype(BF16)
            branches[member, 1, rows_of(c)] = imag.astype(BF16)
            spread(c)

    for r in range(rounds - 1):
        for c in range(CHUNKS):
            select(r, c)
    for c in range(CHUNKS + 2):
        if rounds and c < CHUNKS:
            select(rounds - 1, c)
        if 1 <= c <= CHUNKS:
            on_z(c - 1)
            on_y(0, c - 1)
        if c >= 2:
            on_y(1, c - 2)
    stem_copy.wait()
    for c in range(CHUNKS):
        for i in range(4):
            core_copy(i, c).wait_recv()
    last_copy = pltpu.make_async_copy(branches.at[GROUP - 1], last_out, local_sem.at[3])
    last_copy.start()

    def columns(block):
        return pl.ds(pl.multiple_of(block * half, half), half)

    def swapped(step, index, read, target):
        copy = remote(swap.at[index], target.at[core], swap_s.at[index], swap_r.at[index], other)
        for keep in range(2):
            block = core if keep else 1 - core

            def tile(t, carry, keep=keep, block=block):
                at = pl.ds(pl.multiple_of(t * half, half), half)
                nr, ni = read(at)
                real, imag = complex_product(
                    nr, ni, branches[step, 0, :, columns(block)], branches[step, 1, :, columns(block)]
                )
                place = target.at[core] if keep else swap.at[index]
                place[0, at] = real.astype(BF16)
                place[1, at] = imag.astype(BF16)
                return carry

            lax.fori_loop(0, rows // half, tile, 0)
            if not keep:
                copy.start()
        copy.wait()

    def plain(step, source, target):
        for block in range(width // half):
            across = pl.ds(block * half, half)

            def tile(t, carry, across=across):
                at = pl.ds(pl.multiple_of(t * half, half), half)
                real, imag = complex_product(
                    jnp.concatenate([source[0, 0, at], source[1, 0, at]], axis=1),
                    jnp.concatenate([source[0, 1, at], source[1, 1, at]], axis=1),
                    branches[step, 0, :, across], branches[step, 1, :, across],
                )
                target[0, at, across] = real.astype(target.dtype)
                target[1, at, across] = imag.astype(target.dtype)
                return carry

            lax.fori_loop(0, rows // half, tile, 0)

    swapped(0, 0, lambda at: (stem[0, at].astype(BF16), stem[1, at].astype(BF16)), net1)
    plain(1, net1, net2)
    swapped(2, 1, lambda at: (net2[0, at], net2[1, at]), net3)
    net_copy = pltpu.make_async_copy(net3, net_out, local_sem.at[4])
    net_copy.start()
    net_copy.wait()
    last_copy.wait()

    leaf_copies[1].wait_send()
    pair_copy.wait_send()
    for c in range(CHUNKS):
        z_copy(c).wait_send()
        for i in range(2):
            y_copy(i, c).wait_send()
        for i in range(4):
            core_copy(i, c).wait_send()


def finish(net, branch, out):
    half = net.shape[3]
    for block in range(branch.shape[2] // half):
        across = pl.ds(block * half, half)
        real, imag = complex_product(
            jnp.concatenate([net[0, 0], net[1, 0]], axis=1),
            jnp.concatenate([net[0, 1], net[1, 1]], axis=1),
            branch[0, :, across], branch[1, :, across],
        )
        out[0, :, across] = real
        out[1, :, across] = imag


LEAF = 4
SPREAD = 8


def matching(roots, group):
    seen = jnp.int32(0)
    found = []
    for k in range(roots.shape[0]):
        holds = jnp.where(roots[k] // GROUP == group, 1, 0)
        found.append((holds, seen))
        seen = seen + holds
    return found


def step_of(roots, group, rank):
    total = jnp.int32(0)
    for k, (holds, seen) in enumerate(matching(roots, group)):
        total = total + jnp.where(seen == rank, holds * k, 0)
    return total


def two_groups(
    roots, orders, stem_in, leaves_in, net_out, last_out,
    leaf, outgoing, arrived, mine, chosen, pair, branches, stem, stems, net1, net2, net3, swap, final,
    local_sem, leaf_s, leaf_r, fwd_s, fwd_r, pair_s, pair_r, high_s, high_r,
    y_s, y_r, core_s, core_r, mid_s, end_s, far_r, stem_s, stem_r, swap_s, swap_r,
):
    width = stem.shape[2]
    rows = stem.shape[1]
    half = width // 2
    part = half // SPREAD
    core = lax.axis_index("narrow")
    wide = lax.axis_index("wide")
    group = wide // GROUP
    member = wide % GROUP
    y = member % 2
    z = member // 2
    inner = group + z
    other = {"narrow": 1 - core}
    over_y = {"wide": wide + 1 - 2 * y}
    over_z = {"wide": wide + 2 - 4 * z}
    over_mid = {"wide": wide + 2 - 4 * group}
    MESH = pl.DeviceIdType.MESH

    fetch = pltpu.make_async_copy(leaves_in.at[0], leaf, local_sem.at[0])
    stem_copy = pltpu.make_async_copy(stem_in, stem, local_sem.at[1])
    fetch.start()
    stem_copy.start()
    barrier = pltpu.get_barrier_semaphore()
    for peer in [other, over_y, over_z]:
        pl.semaphore_signal(barrier, inc=1, device_id=peer, device_id_type=MESH)

    @pl.when(inner == 1)
    def _():
        pl.semaphore_signal(barrier, inc=1, device_id=over_mid, device_id_type=MESH)
        pl.semaphore_wait(barrier, 4)

    @pl.when(inner != 1)
    def _():
        pl.semaphore_wait(barrier, 3)

    k_right = step_of(roots, group, 0)
    k_left = step_of(roots, group, 1)
    k_own = jnp.where(y == 1, k_right, k_left)
    k_send = jnp.where(y == 1, k_left, k_right)

    def own_rows(j=0, n=1):
        size = half // n
        return pl.ds(pl.multiple_of(core * half + j * size, size), size)

    def one_hot(k):
        column = lax.broadcasted_iota(jnp.int32, (8, width), 1)
        source = jnp.zeros((8, width), jnp.int32)
        for b in range(orders.shape[1]):
            weight = jnp.left_shift(jnp.int32(1), orders[k, b])
            source = source + (jnp.right_shift(column, b) & 1) * weight

        def tile(i, carry):
            row = lax.broadcasted_iota(jnp.int32, (TILE, width), 0) + i * TILE
            at = pl.ds(pl.multiple_of(i * TILE, TILE), TILE)
            same = row == jnp.broadcast_to(source[0:1], (TILE, width))
            chosen[at] = jnp.where(same, 1.0, 0.0).astype(F32).astype(BF16)
            return carry

        lax.fori_loop(0, width // TILE, tile, 0)

    wide_part = width // LEAF

    def chunk(j, by_rows):
        if by_rows:
            return own_rows(j, LEAF), slice(None)
        return own_rows(), pl.ds(j * wide_part, wide_part)

    def leaf_copy(j, by_rows):
        size = half // LEAF
        at = (pl.ds(j * size, size), slice(None)) if by_rows else (slice(None), pl.ds(j * wide_part, wide_part))
        to = chunk(j, by_rows)
        return remote(
            outgoing.at[:, at[0], at[1]], arrived.at[:, to[0], to[1]],
            leaf_s.at[j], leaf_r.at[j], over_y,
        )

    permuted = z * y
    fetch.wait()

    @pl.when(permuted == 0)
    def _():
        for c in range(2):
            outgoing[c] = leaf[k_send, c, own_rows()]

    @pl.when(permuted == 1)
    def _():
        one_hot(k_send)
        for c in range(2):
            outgoing[c] = dot(leaf[k_send, c, own_rows()], chosen[...]).astype(BF16)

    @pl.when(y == 0)
    def _():
        for j in range(LEAF):
            leaf_copy(j, True).start()

    @pl.when(y == 1)
    def _():
        for j in range(LEAF):
            leaf_copy(j, False).start()

    @pl.when(permuted == 0)
    def _():
        for c in range(2):
            mine[c] = leaf[k_own, c]

    @pl.when(permuted == 1)
    def _():
        one_hot(k_own)
        for c in range(2):
            mine[c] = dot(leaf[k_own, c], chosen[...]).astype(BF16)

    stem_copy.wait()
    for c in range(2):
        stems[core, c] = stem[c].astype(BF16)
    stem_share = remote(stems.at[core], stems.at[core], stem_s, stem_r, other)
    stem_share.start()

    def pair_copy(j, by_rows):
        at = chunk(j, by_rows)
        place = pair.at[z, :, at[0], at[1]]
        return remote(place, place, pair_s.at[j], pair_r.at[j], over_z)

    def high_copy(j, by_rows):
        at = chunk(j, by_rows)
        place = pair.at[1, :, at[0], at[1]]
        return remote(place, place, high_s.at[j], high_r.at[j], other)

    def put_pair(j, by_rows, real, imag):
        at = chunk(j, by_rows)
        pair[z, 0, at[0], at[1]] = real.astype(BF16)
        pair[z, 1, at[0], at[1]] = imag.astype(BF16)
        pair_copy(j, by_rows).start()

        @pl.when(z == 1)
        def _():
            high_copy(j, by_rows).start()

    def join(by_rows):
        for j in range(LEAF):
            pair_copy(j, by_rows).wait_recv()

            @pl.when(z == 0)
            def _():
                high_copy(j, by_rows).start()

        for j in range(LEAF):
            high_copy(j, by_rows).wait_recv()

    @pl.when(y == 1)
    def _():
        for j in range(LEAF):
            leaf_copy(j, True).wait_recv()
            at = own_rows(j, LEAF)
            put_pair(j, True, *complex_product(arrived[0, at], arrived[1, at], mine[0], mine[1]))
        join(True)

    @pl.when(y == 0)
    def _():
        def forward(j):
            at = chunk(j, False)
            place = arrived.at[:, at[0], at[1]]
            return remote(place, place, fwd_s.at[j], fwd_r.at[j], other)

        for j in range(LEAF + 1):
            if j < LEAF:
                leaf_copy(j, False).wait_recv()
                forward(j).start()
            if j:
                forward(j - 1).wait_recv()
                at = pl.ds((j - 1) * wide_part, wide_part)
                put_pair(j - 1, False, *complex_product(
                    mine[0, own_rows()], mine[1, own_rows()], arrived[0, :, at], arrived[1, :, at]
                ))
        join(False)
        for j in range(LEAF):
            forward(j).wait_send()

    here = 2 * (1 - y) + group
    far = 2 * (1 - y) + 1 - group
    beside = 2 * y + group
    beyond = 2 * y + 1 - group

    def place(t, r):
        return branches.at[t, :, own_rows(r, SPREAD)]

    def y_copy(i, r):
        t = [here, far][i]
        return remote(place(t, r), place(t, r), y_s.at[i, r], y_r.at[i, r], over_y)

    def core_copy(i, r):
        t = [here, far, beside, beyond][i]
        return remote(place(t, r), place(t, r), core_s.at[i, r], core_r.at[i, r], other)

    def mid_copy(r):
        return remote(place(here, r), place(here, r), mid_s.at[r], far_r.at[r], over_mid)

    def end_copy(r):
        return remote(place(far, r), place(far, r), end_s.at[r], far_r.at[r], over_z)

    for b in range(2):
        at = own_rows(b, 2)
        real, imag = complex_product(pair[0, 0, at], pair[0, 1, at], pair[1, 0], pair[1, 1])
        branches[here, 0, at] = real.astype(BF16)
        branches[here, 1, at] = imag.astype(BF16)
        for r in range(b * SPREAD // 2, (b + 1) * SPREAD // 2):

            @pl.when(inner == 1)
            def _():
                mid_copy(r).start()

            y_copy(0, r).start()
            core_copy(0, r).start()

    for r in range(SPREAD):
        far_copy = mid_copy(r)
        far_copy.wait_recv()

        @pl.when(inner == 1)
        def _():
            end_copy(r).start()

        y_copy(1, r).start()
        core_copy(1, r).start()
        y_copy(0, r).wait_recv()
        core_copy(2, r).start()
    for r in range(SPREAD):
        y_copy(1, r).wait_recv()
        core_copy(3, r).start()
    stem_share.wait()
    for i in range(4):
        for r in range(SPREAD):
            core_copy(i, r).wait_recv()

    source = []
    zeros = matching(roots, 0)
    ones = matching(roots, 1)
    for k in range(roots.shape[0]):
        place_of = jnp.where(zeros[k][0] == 1, 2 * zeros[k][1], 1 + 2 * ones[k][1])
        source.append(jnp.minimum(place_of, 3))

    def columns(block):
        return pl.ds(pl.multiple_of(block * half, half), half)

    for c in range(2):
        final[c] = branches[source[3], c]
    last_copy = pltpu.make_async_copy(final, last_out, local_sem.at[2])
    last_copy.start()

    def first(i, carry):
        real, imag = complex_product(
            stems[i, 0], stems[i, 1],
            branches[source[0], 0, :, columns(core)], branches[source[0], 1, :, columns(core)],
        )
        net1[i, 0] = real.astype(BF16)
        net1[i, 1] = imag.astype(BF16)
        return carry

    lax.fori_loop(0, 2, first, 0)

    def second(block, carry):
        real, imag = complex_product(
            jnp.concatenate([net1[0, 0], net1[1, 0]], axis=1),
            jnp.concatenate([net1[0, 1], net1[1, 1]], axis=1),
            branches[source[1], 0, :, columns(block)], branches[source[1], 1, :, columns(block)],
        )
        net2[0, :, columns(block)] = real.astype(BF16)
        net2[1, :, columns(block)] = imag.astype(BF16)
        return carry

    lax.fori_loop(0, 2, second, 0)

    swap_copy = remote(swap, net3.at[core], swap_s, swap_r, other)
    for keep in range(2):
        block = core if keep else 1 - core
        real, imag = complex_product(
            net2[0], net2[1], branches[source[2], 0, :, columns(block)], branches[source[2], 1, :, columns(block)]
        )
        target = net3.at[core] if keep else swap
        target[0] = real.astype(BF16)
        target[1] = imag.astype(BF16)
        if not keep:
            swap_copy.start()
    swap_copy.wait()
    net_copy = pltpu.make_async_copy(net3, net_out, local_sem.at[3])
    net_copy.start()
    net_copy.wait()
    last_copy.wait()

    for j in range(LEAF):
        leaf_copy(j, True).wait_send()
        pair_copy(j, True).wait_send()
        high_copy(j, True).wait_send()
    for r in range(SPREAD):

        @pl.when(inner == 1)
        def _():
            mid_copy(r).wait_send()
            end_copy(r).wait_send()

        for i in range(2):
            y_copy(i, r).wait_send()
        for i in range(4):
            core_copy(i, r).wait_send()


def general(stem_tensor, leaves, root_devices, mode_orders):
    _, rows, width = stem_tensor.shape
    half = width // 2
    part = half // CHUNKS
    groups = lax.axis_size("wide") // GROUP
    rounds = groups.bit_length() - 1
    vmem = pltpu.VMEM
    dma = pltpu.SemaphoreType.DMA
    network, last = pl.pallas_call(
        functools.partial(kernel, rounds),
        out_shape=(
            jax.ShapeDtypeStruct((2, 2, rows, half), BF16),
            jax.ShapeDtypeStruct((2, width, width), BF16),
        ),
        in_specs=[pl.BlockSpec(memory_space=pltpu.SMEM)] * 2
        + [pl.BlockSpec(memory_space=pl.ANY)] * 2,
        out_specs=[pl.BlockSpec(memory_space=pl.ANY)] * 2,
        scratch_shapes=[
            vmem((2, 2, 2, width, width), BF16),
            vmem((2, 2, half, width), BF16),
            vmem((2, half, width), BF16),
            vmem((2, width, width), BF16),
            vmem((width, width), BF16),
            vmem((max(rounds, 1), CHUNKS, 2, part, width), BF16),
            vmem((max(rounds, 1), CHUNKS, 2, part, width), BF16),
            vmem((GROUP, 2, width, width), BF16),
            vmem((2, rows, width), F32),
            vmem((2, 2, rows, half), BF16),
            vmem((2, rows, width), BF16),
            vmem((2, 2, rows, half), BF16),
            vmem((2, 2, rows, half), BF16),
            dma((5,)),
            dma((2,)), dma((2,)), dma((2,)), dma((2,)),
            dma, dma, dma, dma,
            dma((max(rounds, 1), CHUNKS)), dma((max(rounds, 1), CHUNKS)),
            dma((CHUNKS,)), dma((CHUNKS,)),
            dma((2, CHUNKS)), dma((2, CHUNKS)),
            dma((4, CHUNKS)), dma((4, CHUNKS)),
            dma((2,)), dma((2,)),
        ],
        compiler_params=pltpu.CompilerParams(collective_id=0, has_side_effects=True),
    )(root_devices, mode_orders, stem_tensor, leaves)
    return network, last


def closing(network, last, stem_tensor):
    _, rows, width = stem_tensor.shape
    half = width // 2
    return pl.pallas_call(
        finish,
        grid=(rows // half,),
        out_shape=jax.ShapeDtypeStruct(stem_tensor.shape, F32),
        in_specs=[
            pl.BlockSpec((2, 2, half, half), lambda i: (0, 0, i, 0)),
            pl.BlockSpec((2, width, width), lambda i: (0, 0, 0)),
        ],
        out_specs=pl.BlockSpec((2, half, width), lambda i: (0, i, 0)),
    )(network, last)


def split(stem_tensor, leaves, root_devices, mode_orders):
    _, rows, width = stem_tensor.shape
    half = width // 2
    vmem = pltpu.VMEM
    dma = pltpu.SemaphoreType.DMA
    network, last = pl.pallas_call(
        two_groups,
        out_shape=(
            jax.ShapeDtypeStruct((2, 2, rows, half), BF16),
            jax.ShapeDtypeStruct((2, width, width), BF16),
        ),
        in_specs=[pl.BlockSpec(memory_space=pltpu.SMEM)] * 2
        + [pl.BlockSpec(memory_space=pl.ANY)] * 2,
        out_specs=[pl.BlockSpec(memory_space=pl.ANY)] * 2,
        scratch_shapes=[
            vmem((leaves.shape[1], 2, width, width), BF16),
            vmem((2, half, width), BF16),
            vmem((2, width, width), BF16),
            vmem((2, width, width), BF16),
            vmem((width, width), BF16),
            vmem((2, 2, width, width), BF16),
            vmem((4, 2, width, width), BF16),
            vmem((2, rows, width), F32),
            vmem((2, 2, rows, width), BF16),
            vmem((2, 2, rows, half), BF16),
            vmem((2, rows, width), BF16),
            vmem((2, 2, rows, half), BF16),
            vmem((2, rows, half), BF16),
            vmem((2, width, width), BF16),
            dma((4,)),
            dma((LEAF,)), dma((LEAF,)), dma((LEAF,)), dma((LEAF,)),
            dma((LEAF,)), dma((LEAF,)), dma((LEAF,)), dma((LEAF,)),
            dma((2, SPREAD)), dma((2, SPREAD)),
            dma((4, SPREAD)), dma((4, SPREAD)),
            dma((SPREAD,)), dma((SPREAD,)), dma((SPREAD,)),
            dma, dma, dma, dma,
        ],
        compiler_params=pltpu.CompilerParams(collective_id=1, has_side_effects=True),
    )(root_devices, mode_orders, stem_tensor, leaves)
    return network, last


def local(stem_tensor, leaves, root_devices, mode_orders):
    arrays = (stem_tensor, leaves, root_devices, mode_orders)
    if lax.axis_size("wide") // GROUP == 2:
        even = jnp.sum((root_devices // GROUP).astype(jnp.int32)) == 2
        network, last = lax.cond(even, split, general, *arrays)
    else:
        network, last = general(*arrays)
    return closing(network, last, stem_tensor)


def solution(mesh):
    stem_spec = P(None, ("cuts", "wide", "narrow"), None)
    return jax.shard_map(
        local,
        mesh=mesh,
        in_specs=(stem_spec, P(("cuts", "wide"), None, None, None, None), P(), P()),
        out_specs=stem_spec,
        check_vma=False,
    )
```

```python
import functools

import jax
import jax.numpy as jnp
from jax import lax
from jax.experimental import pallas as pl
from jax.experimental.pallas import tpu as pltpu
from jax.sharding import PartitionSpec as P

GROUP = 4
CHUNKS = 8
FLIGHT = 2
TILE = 128
BF16 = jnp.bfloat16
F32 = jnp.float32


def dot(x, y):
    return jnp.dot(x, y, preferred_element_type=F32)


def complex_product(ar, ai, br, bi):
    left = jnp.concatenate([ar, ai], axis=1)
    return (
        dot(left, jnp.concatenate([br, -bi], axis=0)),
        dot(left, jnp.concatenate([bi, br], axis=0)),
    )


def remote(src, dst, send_sem, recv_sem, device):
    return pltpu.make_async_remote_copy(
        src_ref=src,
        dst_ref=dst,
        send_sem=send_sem,
        recv_sem=recv_sem,
        device_id=device,
        device_id_type=pl.DeviceIdType.MESH,
    )


def kernel(
    rounds, roots, orders, stem_in, leaves_in, net_out, last_out,
    leaf, pair, away, high, chosen, held, crossed, branches, stem, net1, net2, net3, swap,
    local_sem, leaf_s, leaf_r, fwd_s, fwd_r, pair_s, pair_r, high_s, high_r,
    cross_s, cross_r, z_s, z_r, y_s, y_r, core_s, core_r, swap_s, swap_r,
):
    width = stem.shape[2]
    rows = stem.shape[1]
    half = width // 2
    part = half // CHUNKS
    core = lax.axis_index("narrow")
    wide = lax.axis_index("wide")
    member = wide % GROUP
    y = member % 2
    z = member // 2
    other = {"narrow": 1 - core}
    over_y = {"wide": wide + 1 - 2 * y}
    over_z = {"wide": wide + 2 - 4 * z}
    bits = [(wide // (GROUP << r)) % 2 for r in range(rounds)]
    over_group = [{"wide": wide + (GROUP << r) * (1 - 2 * bits[r])} for r in range(rounds)]

    barrier = pltpu.get_barrier_semaphore()
    for peer in [other, over_y, over_z] + over_group:
        pl.semaphore_signal(barrier, inc=1, device_id=peer, device_id_type=pl.DeviceIdType.MESH)
    own_rows = pl.ds(pl.multiple_of(core * half, half), half)
    own_copies = [
        pltpu.make_async_copy(leaves_in.at[0, 2 * s + y], leaf.at[s, y], local_sem.at[s])
        for s in range(2)
    ]
    stem_copy = pltpu.make_async_copy(stem_in, stem, local_sem.at[2])
    pl.semaphore_wait(barrier, 3 + rounds)

    phases = [1 - z, z]
    leaf_copies = []
    for i, s in enumerate(phases):
        copy = remote(
            leaves_in.at[0, 2 * s + 1 - y, :, own_rows],
            leaf.at[s, y, :, own_rows],
            leaf_s.at[i], leaf_r.at[i], over_y,
        )
        leaf_copies.append(copy)
    leaf_copies[0].start()
    for copy in own_copies:
        copy.start()
    stem_copy.start()

    def choose(i, carry):
        column = lax.broadcasted_iota(jnp.int32, (TILE, width), 1)
        source = jnp.zeros((TILE, width), jnp.int32)
        for b in range(orders.shape[1]):
            weight = jnp.left_shift(jnp.int32(1), orders[member, b])
            source = source + (jnp.right_shift(column, b) & 1) * weight
        row = lax.broadcasted_iota(jnp.int32, (TILE, width), 0) + i * TILE
        at = pl.ds(pl.multiple_of(i * TILE, TILE), TILE)
        chosen[at] = jnp.where(row == source, 1.0, 0.0).astype(F32).astype(BF16)
        return carry

    lax.fori_loop(0, width // TILE, choose, 0)
    for copy in own_copies:
        copy.wait()

    pair_copy = remote(away, pair.at[z], pair_s, pair_r, over_z)
    leaf_copies[0].wait_send()
    leaf_copies[1].start()
    for i, s in enumerate(phases):
        leaf_copies[i].wait_recv()
        forward = remote(
            leaf.at[s, 1 - y, :, own_rows], leaf.at[s, 1 - y, :, own_rows],
            fwd_s.at[i], fwd_r.at[i], other,
        )
        forward.start()
        forward.wait()

        def pair_tile(t, carry, s=s, i=i):
            at = pl.ds(pl.multiple_of(t * half, half), half)
            real, imag = complex_product(
                leaf[s, 0, 0, own_rows], leaf[s, 0, 1, own_rows],
                leaf[s, 1, 0, :, at], leaf[s, 1, 1, :, at],
            )
            target = away if i == 0 else pair.at[z]
            target[0, :, at] = real.astype(BF16)
            target[1, :, at] = imag.astype(BF16)
            return carry

        lax.fori_loop(0, width // half, pair_tile, 0)
        if i == 0:
            pair_copy.start()
    pair_copy.wait_recv()

    def high_tile(t, carry):
        at = pl.ds(pl.multiple_of(t * half, half), half)
        for c in range(2):
            high[c, own_rows, at] = dot(pair[1, c], chosen[:, at]).astype(BF16)
        return carry

    lax.fori_loop(0, width // half, high_tile, 0)
    high_copy = remote(high.at[:, own_rows], high.at[:, own_rows], high_s, high_r, other)
    high_copy.start()
    high_copy.wait()

    def rows_of(c):
        return pl.ds(pl.multiple_of(core * half + c * part, part), part)

    def cross_copy(r, c):
        return remote(held.at[r, c], crossed.at[r, c], cross_s.at[r, c], cross_r.at[r, c], over_group[r])

    def place(origin, c):
        return branches.at[origin, :, rows_of(c)]

    origins = [member, member + 2 - 4 * z, member + 1 - 2 * y, GROUP - 1 - member]

    def z_copy(c):
        return remote(place(origins[0], c), place(origins[0], c), z_s.at[c], z_r.at[c], over_z)

    def y_copy(i, c):
        return remote(place(origins[i], c), place(origins[i], c), y_s.at[i, c], y_r.at[i, c], over_y)

    def core_copy(i, c):
        return remote(place(origins[i], c), place(origins[i], c), core_s.at[i, c], core_r.at[i, c], other)

    def spread(c):
        z_copy(c).start()
        y_copy(0, c).start()
        core_copy(0, c).start()

    def select(r, c):
        cross_copy(r, c).wait_recv()
        cross_copy(r, c).wait_send()
        if c + FLIGHT < CHUNKS:
            cross_copy(r, c + FLIGHT).start()
        root_bit = (roots[member] // (GROUP << r)) % 2
        for p in range(2):
            here = held[r, c, p].astype(F32)
            there = crossed[r, c, p].astype(F32)
            same = jnp.full(here.shape, root_bit, jnp.int32) == bits[r]
            picked = jnp.where(same, here, there).astype(BF16)
            if r + 1 < rounds:
                held[r + 1, c, p] = picked
            else:
                branches[member, p, rows_of(c)] = picked
        if r + 1 < rounds:
            if c < FLIGHT:
                cross_copy(r + 1, c).start()
        else:
            spread(c)

    def on_z(c):
        z_copy(c).wait_recv()
        y_copy(1, c).start()
        core_copy(1, c).start()

    def on_y(i, c):
        y_copy(i, c).wait_recv()
        core_copy(2 + i, c).start()

    for c in range(CHUNKS):
        at = pl.ds(c * part, part)
        real, imag = complex_product(pair[0, 0, at], pair[0, 1, at], high[0], high[1])
        if rounds:
            held[0, c, 0] = real.astype(BF16)
            held[0, c, 1] = imag.astype(BF16)
            if c < FLIGHT:
                cross_copy(0, c).start()
        else:
            branches[member, 0, rows_of(c)] = real.astype(BF16)
            branches[member, 1, rows_of(c)] = imag.astype(BF16)
            spread(c)

    for r in range(rounds - 1):
        for c in range(CHUNKS):
            select(r, c)
    for c in range(CHUNKS + 2):
        if rounds and c < CHUNKS:
            select(rounds - 1, c)
        if 1 <= c <= CHUNKS:
            on_z(c - 1)
            on_y(0, c - 1)
        if c >= 2:
            on_y(1, c - 2)
    stem_copy.wait()
    for c in range(CHUNKS):
        for i in range(4):
            core_copy(i, c).wait_recv()
    last_copy = pltpu.make_async_copy(branches.at[GROUP - 1], last_out, local_sem.at[3])
    last_copy.start()

    def columns(block):
        return pl.ds(pl.multiple_of(block * half, half), half)

    def swapped(step, index, read, target):
        copy = remote(swap.at[index], target.at[core], swap_s.at[index], swap_r.at[index], other)
        for keep in range(2):
            block = core if keep else 1 - core

            def tile(t, carry, keep=keep, block=block):
                at = pl.ds(pl.multiple_of(t * half, half), half)
                nr, ni = read(at)
                real, imag = complex_product(
                    nr, ni, branches[step, 0, :, columns(block)], branches[step, 1, :, columns(block)]
                )
                place = target.at[core] if keep else swap.at[index]
                place[0, at] = real.astype(BF16)
                place[1, at] = imag.astype(BF16)
                return carry

            lax.fori_loop(0, rows // half, tile, 0)
            if not keep:
                copy.start()
        copy.wait()

    def plain(step, source, target):
        for block in range(width // half):
            across = pl.ds(block * half, half)

            def tile(t, carry, across=across):
                at = pl.ds(pl.multiple_of(t * half, half), half)
                real, imag = complex_product(
                    jnp.concatenate([source[0, 0, at], source[1, 0, at]], axis=1),
                    jnp.concatenate([source[0, 1, at], source[1, 1, at]], axis=1),
                    branches[step, 0, :, across], branches[step, 1, :, across],
                )
                target[0, at, across] = real.astype(target.dtype)
                target[1, at, across] = imag.astype(target.dtype)
                return carry

            lax.fori_loop(0, rows // half, tile, 0)

    swapped(0, 0, lambda at: (stem[0, at].astype(BF16), stem[1, at].astype(BF16)), net1)
    plain(1, net1, net2)
    swapped(2, 1, lambda at: (net2[0, at], net2[1, at]), net3)
    net_copy = pltpu.make_async_copy(net3, net_out, local_sem.at[4])
    net_copy.start()
    net_copy.wait()
    last_copy.wait()

    leaf_copies[1].wait_send()
    pair_copy.wait_send()
    for c in range(CHUNKS):
        z_copy(c).wait_send()
        for i in range(2):
            y_copy(i, c).wait_send()
        for i in range(4):
            core_copy(i, c).wait_send()


def finish(net, branch, out):
    half = net.shape[3]
    for block in range(branch.shape[2] // half):
        across = pl.ds(block * half, half)
        real, imag = complex_product(
            jnp.concatenate([net[0, 0], net[1, 0]], axis=1),
            jnp.concatenate([net[0, 1], net[1, 1]], axis=1),
            branch[0, :, across], branch[1, :, across],
        )
        out[0, :, across] = real
        out[1, :, across] = imag


BY_ROWS = 8
BY_COLUMNS = 4
SPREAD = 8


def matching(roots, group):
    seen = jnp.int32(0)
    found = []
    for k in range(roots.shape[0]):
        holds = jnp.where(roots[k] // GROUP == group, 1, 0)
        found.append((holds, seen))
        seen = seen + holds
    return found


def step_of(roots, group, rank):
    total = jnp.int32(0)
    for k, (holds, seen) in enumerate(matching(roots, group)):
        total = total + jnp.where(seen == rank, holds * k, 0)
    return total


def two_groups(
    third, roots, orders, stem_in, leaves_in, net_out, last_out,
    leaf, outgoing, arrived, mine, chosen, pair, branches, stem, stems, net1, net2, net3, swap, final,
    local_sem, leaf_s, leaf_r, fwd_s, fwd_r, pair_s, pair_r, high_s, high_r,
    y_s, y_r, core_s, core_r, mid_s, end_s, far_r, stem_s, stem_r, swap_s, swap_r,
):
    width = stem.shape[2]
    half = width // 2
    core = lax.axis_index("narrow")
    wide = lax.axis_index("wide")
    group = wide // GROUP
    member = wide % GROUP
    y = member % 2
    z = member // 2
    inner = group + z == 1
    other = {"narrow": 1 - core}
    over_y = {"wide": wide + 1 - 2 * y}
    over_z = {"wide": wide + 2 - 4 * z}
    over_mid = {"wide": wide + 2 - 4 * group}
    MESH = pl.DeviceIdType.MESH
    sets = 2 if third else 1
    left = group == 1 if third else group >= 0

    fetch = pltpu.make_async_copy(leaves_in.at[0], leaf, local_sem.at[0])
    stem_copy = pltpu.make_async_copy(stem_in, stem, local_sem.at[1])
    fetch.start()
    barrier = pltpu.get_barrier_semaphore()
    for peer in [other, over_y, over_z]:
        pl.semaphore_signal(barrier, inc=1, device_id=peer, device_id_type=MESH)

    @pl.when(inner)
    def _():
        pl.semaphore_signal(barrier, inc=1, device_id=over_mid, device_id_type=MESH)

    k_right = step_of(roots, group, 0)
    k_left = [step_of(roots, group, 1 + e) for e in range(sets)]

    def own_rows(j=0, n=1):
        size = half // n
        return pl.ds(pl.multiple_of(core * half + j * size, size), size)

    def one_hot(k):
        column = lax.broadcasted_iota(jnp.int32, (8, width), 1)
        source = jnp.zeros((8, width), jnp.int32)
        for b in range(orders.shape[1]):
            weight = jnp.left_shift(jnp.int32(1), orders[k, b])
            source = source + (jnp.right_shift(column, b) & 1) * weight

        def tile(i, carry):
            row = lax.broadcasted_iota(jnp.int32, (TILE, width), 0) + i * TILE
            at = pl.ds(pl.multiple_of(i * TILE, TILE), TILE)
            same = row == jnp.broadcast_to(source[0:1], (TILE, width))
            chosen[at] = jnp.where(same, 1.0, 0.0).astype(F32).astype(BF16)
            return carry

        lax.fori_loop(0, width // TILE, tile, 0)

    def count(by_rows):
        return BY_ROWS if by_rows else BY_COLUMNS

    def chunk(j, by_rows):
        if by_rows:
            return own_rows(j, BY_ROWS), slice(None)
        size = width // BY_COLUMNS
        return own_rows(), pl.ds(j * size, size)

    def leaf_copy(e, j, by_rows):
        to = chunk(j, by_rows)
        size = half // BY_ROWS
        at = (pl.ds(j * size, size), slice(None)) if by_rows else (slice(None), to[1])
        return remote(
            outgoing.at[e, :, at[0], at[1]], arrived.at[e, :, to[0], to[1]],
            leaf_s.at[e, j], leaf_r.at[e, j], over_y,
        )

    last_leaf = z == 1

    @pl.when(inner)
    def _():
        pl.semaphore_wait(barrier, 4)

    @pl.when(jnp.logical_not(inner))
    def _():
        pl.semaphore_wait(barrier, 3)

    @pl.when(y == 0)
    def _():
        fetch.wait()
        for c in range(2):
            outgoing[0, c] = leaf[k_right, c, own_rows()]
        for j in range(BY_ROWS):
            leaf_copy(0, j, True).start()
        for e in range(sets):
            for c in range(2):
                mine[e, c, own_rows()] = leaf[k_left[e], c, own_rows()]

    @pl.when(jnp.logical_and(y == 1, jnp.logical_not(last_leaf)))
    def _():
        fetch.wait()

        @pl.when(left)
        def _():
            for e in range(sets):
                for c in range(2):
                    outgoing[e, c] = leaf[k_left[e], c, own_rows()]
                for j in range(BY_COLUMNS):
                    leaf_copy(e, j, False).start()

        for c in range(2):
            mine[0, c] = leaf[k_right, c]

    @pl.when(jnp.logical_and(y == 1, last_leaf))
    def _():
        if third:
            fetch.wait()

        @pl.when(left)
        def _():
            for e in range(sets):
                one_hot(k_left[e])
                if not third:
                    fetch.wait()
                for c in range(2):
                    outgoing[e, c] = dot(leaf[k_left[e], c, own_rows()], chosen[...]).astype(BF16)
                for j in range(BY_COLUMNS):
                    leaf_copy(e, j, False).start()

        one_hot(k_right)
        for c in range(2):
            mine[0, c] = dot(leaf[k_right, c], chosen[...]).astype(BF16)

    stem_copy.start()
    stem_copy.wait()
    for c in range(2):
        stems[core, c] = stem[c].astype(BF16)
    stem_share = remote(stems.at[core], stems.at[core], stem_s, stem_r, other)
    stem_share.start()

    def pair_copy(e, j, by_rows):
        at = chunk(j, by_rows)
        place = pair.at[e, z, :, at[0], at[1]]
        return remote(place, place, pair_s.at[e, j], pair_r.at[e, j], over_z)

    def high_copy(e, j, by_rows):
        at = chunk(j, by_rows)
        place = pair.at[e, 1, :, at[0], at[1]]
        return remote(place, place, high_s.at[e, j], high_r.at[e, j], other)

    def forward(e, j):
        at = chunk(j, False)
        place = arrived.at[e, :, at[0], at[1]]
        return remote(place, place, fwd_s.at[e, j], fwd_r.at[e, j], other)

    def put_pair(e, j, by_rows, real, imag):
        at = chunk(j, by_rows)
        pair[e, z, 0, at[0], at[1]] = real.astype(BF16)
        pair[e, z, 1, at[0], at[1]] = imag.astype(BF16)
        pair_copy(e, j, by_rows).start()

        @pl.when(z == 1)
        def _():
            high_copy(e, j, by_rows).start()

    def join(e, by_rows):
        for j in range(count(by_rows)):
            pair_copy(e, j, by_rows).wait_recv()

            @pl.when(z == 0)
            def _():
                high_copy(e, j, by_rows).start()

        for j in range(count(by_rows)):
            high_copy(e, j, by_rows).wait_recv()

    def pairs_by_rows():
        for j in range(BY_ROWS):
            leaf_copy(0, j, True).wait_recv()
            at = own_rows(j, BY_ROWS)
            put_pair(0, j, True, *complex_product(arrived[0, 0, at], arrived[0, 1, at], mine[0, 0], mine[0, 1]))
        join(0, True)

    def pairs_by_columns(e):
        for j in range(BY_COLUMNS + 1):
            if j < BY_COLUMNS:
                leaf_copy(e, j, False).wait_recv()
                forward(e, j).start()
            if j:
                forward(e, j - 1).wait_recv()
                at = chunk(j - 1, False)[1]
                put_pair(e, j - 1, False, *complex_product(
                    mine[e, 0, own_rows()], mine[e, 1, own_rows()], arrived[e, 0, :, at], arrived[e, 1, :, at]
                ))
        join(e, False)

    def place(t, r):
        return branches.at[t, :, own_rows(r, SPREAD)]

    def y_copy(t, r):
        return remote(place(t, r), place(t, r), y_s.at[t, r], y_r.at[t, r], over_y)

    def core_copy(t, r):
        return remote(place(t, r), place(t, r), core_s.at[t, r], core_r.at[t, r], other)

    def mid_copy(t, r):
        return remote(place(t, r), place(t, r), mid_s.at[t, r], far_r.at[t, r], over_mid)

    def end_copy(t, r):
        return remote(place(t, r), place(t, r), end_s.at[t, r], far_r.at[t, r], over_z)

    sent = []

    def send(copy, t, r):
        copy(t, r).start()
        sent.append((copy, t, r, False))

    def send_inner(copy, t, r):
        @pl.when(inner)
        def _():
            copy(t, r).start()

        sent.append((copy, t, r, True))

    def own(e, t):
        for b in range(2):
            at = own_rows(b, 2)
            real, imag = complex_product(pair[e, 0, 0, at], pair[e, 0, 1, at], pair[e, 1, 0], pair[e, 1, 1])
            branches[t, 0, at] = real.astype(BF16)
            branches[t, 1, at] = imag.astype(BF16)
            for r in range(b * SPREAD // 2, (b + 1) * SPREAD // 2):
                send_inner(mid_copy, t, r)
                send(y_copy, t, r)
                send(core_copy, t, r)

    def receive(*turns):
        for r in range(SPREAD):
            for t, origin, onward in turns:
                if origin == "z":
                    mid_copy(t, r).wait_recv()
                    send_inner(end_copy, t, r)
                    if onward:
                        send(y_copy, t, r)
                else:
                    y_copy(t, r).wait_recv()
                    if onward:
                        send_inner(mid_copy, t, r)
                send(core_copy, t, r)

    A, C, D, E = range(4)

    def role_right_low():
        pairs_by_rows()
        own(0, A)
        if third:
            receive((C, "z", True))
            receive((E, "y", False))
            receive((D, "y", False))
        else:
            receive((C, "z", True), (D, "y", False))
            receive((E, "y", False))

    def role_right_high():
        pairs_by_rows()
        own(0, C)
        receive((A, "z", not third), (E, "y", False))
        receive((D, "y", False))

    def role_left_low():
        if third:
            receive((A, "y", True), (E, "z", True))
            receive((C, "y", False))
            receive((D, "z", True))
        else:
            pairs_by_columns(0)
            own(0, D)
            receive((E, "z", True), (A, "y", False))
            receive((C, "y", False))

    def role_left_high():
        pairs_by_columns(0)
        own(0, E)
        if third:
            pairs_by_columns(1)
            own(1, D)
            receive((A, "z", False))
            receive((C, "y", False))
        else:
            receive((D, "z", True), (C, "y", False))
            receive((A, "y", False))

    roles = [(1, 0, role_right_low), (1, 1, role_right_high), (0, 0, role_left_low), (0, 1, role_left_high)]
    drains = []
    for at_y, at_group, role in roles:
        sent.clear()
        here = jnp.logical_and(y == at_y, group == at_group)
        pl.when(here)(role)
        drains.append((here, list(sent)))

    stem_share.wait()
    for r in range(SPREAD):
        for t in range(4):
            core_copy(t, r).wait_recv()

    zeros = matching(roots, 0)
    ones = matching(roots, 1)
    source = []
    for k in range(roots.shape[0]):
        high = jnp.where(ones[k][1] == 2, D, C + 2 * ones[k][1])
        at = jnp.where(zeros[k][0] == 1, A + 2 * zeros[k][1], high)
        source.append(jnp.minimum(at, 3))

    def columns(block):
        return pl.ds(pl.multiple_of(block * half, half), half)

    for c in range(2):
        final[c] = branches[source[3], c]
    last_copy = pltpu.make_async_copy(final, last_out, local_sem.at[2])
    last_copy.start()

    def first(i, carry):
        real, imag = complex_product(
            stems[i, 0], stems[i, 1],
            branches[source[0], 0, :, columns(core)], branches[source[0], 1, :, columns(core)],
        )
        net1[i, 0] = real.astype(BF16)
        net1[i, 1] = imag.astype(BF16)
        return carry

    lax.fori_loop(0, 2, first, 0)

    def second(block, carry):
        real, imag = complex_product(
            jnp.concatenate([net1[0, 0], net1[1, 0]], axis=1),
            jnp.concatenate([net1[0, 1], net1[1, 1]], axis=1),
            branches[source[1], 0, :, columns(block)], branches[source[1], 1, :, columns(block)],
        )
        net2[0, :, columns(block)] = real.astype(BF16)
        net2[1, :, columns(block)] = imag.astype(BF16)
        return carry

    lax.fori_loop(0, 2, second, 0)

    swap_copy = remote(swap, net3.at[core], swap_s, swap_r, other)
    for keep in range(2):
        block = core if keep else 1 - core
        real, imag = complex_product(
            net2[0], net2[1], branches[source[2], 0, :, columns(block)], branches[source[2], 1, :, columns(block)]
        )
        target = net3.at[core] if keep else swap
        target[0] = real.astype(BF16)
        target[1] = imag.astype(BF16)
        if not keep:
            swap_copy.start()
    swap_copy.wait()
    net_copy = pltpu.make_async_copy(net3, net_out, local_sem.at[3])
    net_copy.start()
    net_copy.wait()
    last_copy.wait()

    @pl.when(y == 0)
    def _():
        for j in range(BY_ROWS):
            leaf_copy(0, j, True).wait_send()

        @pl.when(left)
        def _():
            for e in range(sets):
                for j in range(BY_COLUMNS):
                    forward(e, j).wait_send()
                    pair_copy(e, j, False).wait_send()
                    high_copy(e, j, False).wait_send()

    @pl.when(y == 1)
    def _():
        for j in range(BY_ROWS):
            pair_copy(0, j, True).wait_send()
            high_copy(0, j, True).wait_send()

        @pl.when(left)
        def _():
            for e in range(sets):
                for j in range(BY_COLUMNS):
                    leaf_copy(e, j, False).wait_send()

    for here, copies in drains:

        @pl.when(here)
        def _(copies=copies):
            for copy, t, r, only_inner in copies:
                if not only_inner:
                    copy(t, r).wait_send()

            @pl.when(inner)
            def _():
                for copy, t, r, only_inner in copies:
                    if only_inner:
                        copy(t, r).wait_send()


def general(stem_tensor, leaves, root_devices, mode_orders):
    _, rows, width = stem_tensor.shape
    half = width // 2
    part = half // CHUNKS
    groups = lax.axis_size("wide") // GROUP
    rounds = groups.bit_length() - 1
    vmem = pltpu.VMEM
    dma = pltpu.SemaphoreType.DMA
    network, last = pl.pallas_call(
        functools.partial(kernel, rounds),
        out_shape=(
            jax.ShapeDtypeStruct((2, 2, rows, half), BF16),
            jax.ShapeDtypeStruct((2, width, width), BF16),
        ),
        in_specs=[pl.BlockSpec(memory_space=pltpu.SMEM)] * 2
        + [pl.BlockSpec(memory_space=pl.ANY)] * 2,
        out_specs=[pl.BlockSpec(memory_space=pl.ANY)] * 2,
        scratch_shapes=[
            vmem((2, 2, 2, width, width), BF16),
            vmem((2, 2, half, width), BF16),
            vmem((2, half, width), BF16),
            vmem((2, width, width), BF16),
            vmem((width, width), BF16),
            vmem((max(rounds, 1), CHUNKS, 2, part, width), BF16),
            vmem((max(rounds, 1), CHUNKS, 2, part, width), BF16),
            vmem((GROUP, 2, width, width), BF16),
            vmem((2, rows, width), F32),
            vmem((2, 2, rows, half), BF16),
            vmem((2, rows, width), BF16),
            vmem((2, 2, rows, half), BF16),
            vmem((2, 2, rows, half), BF16),
            dma((5,)),
            dma((2,)), dma((2,)), dma((2,)), dma((2,)),
            dma, dma, dma, dma,
            dma((max(rounds, 1), CHUNKS)), dma((max(rounds, 1), CHUNKS)),
            dma((CHUNKS,)), dma((CHUNKS,)),
            dma((2, CHUNKS)), dma((2, CHUNKS)),
            dma((4, CHUNKS)), dma((4, CHUNKS)),
            dma((2,)), dma((2,)),
        ],
        compiler_params=pltpu.CompilerParams(collective_id=0, has_side_effects=True),
    )(root_devices, mode_orders, stem_tensor, leaves)
    return network, last


def closing(network, last, stem_tensor):
    _, rows, width = stem_tensor.shape
    half = width // 2
    return pl.pallas_call(
        finish,
        grid=(rows // half,),
        out_shape=jax.ShapeDtypeStruct(stem_tensor.shape, F32),
        in_specs=[
            pl.BlockSpec((2, 2, half, half), lambda i: (0, 0, i, 0)),
            pl.BlockSpec((2, width, width), lambda i: (0, 0, 0)),
        ],
        out_specs=pl.BlockSpec((2, half, width), lambda i: (0, i, 0)),
    )(network, last)


def split(third, stem_tensor, leaves, root_devices, mode_orders):
    _, rows, width = stem_tensor.shape
    half = width // 2
    sets = 2 if third else 1
    vmem = pltpu.VMEM
    dma = pltpu.SemaphoreType.DMA
    return pl.pallas_call(
        functools.partial(two_groups, third),
        out_shape=(
            jax.ShapeDtypeStruct((2, 2, rows, half), BF16),
            jax.ShapeDtypeStruct((2, width, width), BF16),
        ),
        in_specs=[pl.BlockSpec(memory_space=pltpu.SMEM)] * 2
        + [pl.BlockSpec(memory_space=pl.ANY)] * 2,
        out_specs=[pl.BlockSpec(memory_space=pl.ANY)] * 2,
        scratch_shapes=[
            vmem((leaves.shape[1], 2, width, width), BF16),
            vmem((sets, 2, half, width), BF16),
            vmem((sets, 2, width, width), BF16),
            vmem((sets, 2, width, width), BF16),
            vmem((width, width), BF16),
            vmem((sets, 2, 2, width, width), BF16),
            vmem((4, 2, width, width), BF16),
            vmem((2, rows, width), F32),
            vmem((2, 2, rows, width), BF16),
            vmem((2, 2, rows, half), BF16),
            vmem((2, rows, width), BF16),
            vmem((2, 2, rows, half), BF16),
            vmem((2, rows, half), BF16),
            vmem((2, width, width), BF16),
            dma((4,)),
        ]
        + [dma((sets, BY_ROWS))] * 8
        + [dma((4, SPREAD))] * 7
        + [dma] * 4,
        compiler_params=pltpu.CompilerParams(collective_id=2 if third else 1, has_side_effects=True),
    )(root_devices, mode_orders, stem_tensor, leaves)


def local(stem_tensor, leaves, root_devices, mode_orders):
    arrays = (stem_tensor, leaves, root_devices, mode_orders)
    if lax.axis_size("wide") // GROUP == 2:
        even = jnp.sum((root_devices // GROUP).astype(jnp.int32)) == 2
        network, last = lax.cond(
            even, functools.partial(split, False), functools.partial(split, True), *arrays
        )
    else:
        network, last = general(*arrays)
    return closing(network, last, stem_tensor)


def solution(mesh):
    stem_spec = P(None, ("cuts", "wide", "narrow"), None)
    return jax.shard_map(
        local,
        mesh=mesh,
        in_specs=(stem_spec, P(("cuts", "wide"), None, None, None, None), P(), P()),
        out_specs=stem_spec,
        check_vma=False,
    )
```

```python
import functools

import jax
import jax.numpy as jnp
from jax import lax
from jax.experimental import pallas as pl
from jax.experimental.pallas import tpu as pltpu
from jax.sharding import PartitionSpec as P

GROUP = 4
CHUNKS = 8
FLIGHT = 2
TILE = 128
BF16 = jnp.bfloat16
F32 = jnp.float32


def dot(x, y):
    return jnp.dot(x, y, preferred_element_type=F32)


def complex_product(ar, ai, br, bi):
    left = jnp.concatenate([ar, ai], axis=1)
    return (
        dot(left, jnp.concatenate([br, -bi], axis=0)),
        dot(left, jnp.concatenate([bi, br], axis=0)),
    )


def remote(src, dst, send_sem, recv_sem, device):
    return pltpu.make_async_remote_copy(
        src_ref=src,
        dst_ref=dst,
        send_sem=send_sem,
        recv_sem=recv_sem,
        device_id=device,
        device_id_type=pl.DeviceIdType.MESH,
    )


def kernel(
    rounds, roots, orders, stem_in, leaves_in, net_out, last_out,
    leaf, pair, away, high, chosen, held, crossed, branches, stem, net1, net2, net3, swap,
    local_sem, leaf_s, leaf_r, fwd_s, fwd_r, pair_s, pair_r, high_s, high_r,
    cross_s, cross_r, z_s, z_r, y_s, y_r, core_s, core_r, swap_s, swap_r,
):
    width = stem.shape[2]
    rows = stem.shape[1]
    half = width // 2
    part = half // CHUNKS
    core = lax.axis_index("narrow")
    wide = lax.axis_index("wide")
    member = wide % GROUP
    y = member % 2
    z = member // 2
    other = {"narrow": 1 - core}
    over_y = {"wide": wide + 1 - 2 * y}
    over_z = {"wide": wide + 2 - 4 * z}
    bits = [(wide // (GROUP << r)) % 2 for r in range(rounds)]
    over_group = [{"wide": wide + (GROUP << r) * (1 - 2 * bits[r])} for r in range(rounds)]

    barrier = pltpu.get_barrier_semaphore()
    for peer in [other, over_y, over_z] + over_group:
        pl.semaphore_signal(barrier, inc=1, device_id=peer, device_id_type=pl.DeviceIdType.MESH)
    own_rows = pl.ds(pl.multiple_of(core * half, half), half)
    own_copies = [
        pltpu.make_async_copy(leaves_in.at[0, 2 * s + y], leaf.at[s, y], local_sem.at[s])
        for s in range(2)
    ]
    stem_copy = pltpu.make_async_copy(stem_in, stem, local_sem.at[2])
    pl.semaphore_wait(barrier, 3 + rounds)

    phases = [1 - z, z]
    leaf_copies = []
    for i, s in enumerate(phases):
        copy = remote(
            leaves_in.at[0, 2 * s + 1 - y, :, own_rows],
            leaf.at[s, y, :, own_rows],
            leaf_s.at[i], leaf_r.at[i], over_y,
        )
        leaf_copies.append(copy)
    leaf_copies[0].start()
    for copy in own_copies:
        copy.start()
    stem_copy.start()

    def choose(i, carry):
        column = lax.broadcasted_iota(jnp.int32, (TILE, width), 1)
        source = jnp.zeros((TILE, width), jnp.int32)
        for b in range(orders.shape[1]):
            weight = jnp.left_shift(jnp.int32(1), orders[member, b])
            source = source + (jnp.right_shift(column, b) & 1) * weight
        row = lax.broadcasted_iota(jnp.int32, (TILE, width), 0) + i * TILE
        at = pl.ds(pl.multiple_of(i * TILE, TILE), TILE)
        chosen[at] = jnp.where(row == source, 1.0, 0.0).astype(F32).astype(BF16)
        return carry

    lax.fori_loop(0, width // TILE, choose, 0)
    for copy in own_copies:
        copy.wait()

    pair_copy = remote(away, pair.at[z], pair_s, pair_r, over_z)
    leaf_copies[0].wait_send()
    leaf_copies[1].start()
    for i, s in enumerate(phases):
        leaf_copies[i].wait_recv()
        forward = remote(
            leaf.at[s, 1 - y, :, own_rows], leaf.at[s, 1 - y, :, own_rows],
            fwd_s.at[i], fwd_r.at[i], other,
        )
        forward.start()
        forward.wait()

        def pair_tile(t, carry, s=s, i=i):
            at = pl.ds(pl.multiple_of(t * half, half), half)
            real, imag = complex_product(
                leaf[s, 0, 0, own_rows], leaf[s, 0, 1, own_rows],
                leaf[s, 1, 0, :, at], leaf[s, 1, 1, :, at],
            )
            target = away if i == 0 else pair.at[z]
            target[0, :, at] = real.astype(BF16)
            target[1, :, at] = imag.astype(BF16)
            return carry

        lax.fori_loop(0, width // half, pair_tile, 0)
        if i == 0:
            pair_copy.start()
    pair_copy.wait_recv()

    def high_tile(t, carry):
        at = pl.ds(pl.multiple_of(t * half, half), half)
        for c in range(2):
            high[c, own_rows, at] = dot(pair[1, c], chosen[:, at]).astype(BF16)
        return carry

    lax.fori_loop(0, width // half, high_tile, 0)
    high_copy = remote(high.at[:, own_rows], high.at[:, own_rows], high_s, high_r, other)
    high_copy.start()
    high_copy.wait()

    def rows_of(c):
        return pl.ds(pl.multiple_of(core * half + c * part, part), part)

    def cross_copy(r, c):
        return remote(held.at[r, c], crossed.at[r, c], cross_s.at[r, c], cross_r.at[r, c], over_group[r])

    def place(origin, c):
        return branches.at[origin, :, rows_of(c)]

    origins = [member, member + 2 - 4 * z, member + 1 - 2 * y, GROUP - 1 - member]

    def z_copy(c):
        return remote(place(origins[0], c), place(origins[0], c), z_s.at[c], z_r.at[c], over_z)

    def y_copy(i, c):
        return remote(place(origins[i], c), place(origins[i], c), y_s.at[i, c], y_r.at[i, c], over_y)

    def core_copy(i, c):
        return remote(place(origins[i], c), place(origins[i], c), core_s.at[i, c], core_r.at[i, c], other)

    def spread(c):
        z_copy(c).start()
        y_copy(0, c).start()
        core_copy(0, c).start()

    def select(r, c):
        cross_copy(r, c).wait_recv()
        cross_copy(r, c).wait_send()
        if c + FLIGHT < CHUNKS:
            cross_copy(r, c + FLIGHT).start()
        root_bit = (roots[member] // (GROUP << r)) % 2
        for p in range(2):
            here = held[r, c, p].astype(F32)
            there = crossed[r, c, p].astype(F32)
            same = jnp.full(here.shape, root_bit, jnp.int32) == bits[r]
            picked = jnp.where(same, here, there).astype(BF16)
            if r + 1 < rounds:
                held[r + 1, c, p] = picked
            else:
                branches[member, p, rows_of(c)] = picked
        if r + 1 < rounds:
            if c < FLIGHT:
                cross_copy(r + 1, c).start()
        else:
            spread(c)

    def on_z(c):
        z_copy(c).wait_recv()
        y_copy(1, c).start()
        core_copy(1, c).start()

    def on_y(i, c):
        y_copy(i, c).wait_recv()
        core_copy(2 + i, c).start()

    for c in range(CHUNKS):
        at = pl.ds(c * part, part)
        real, imag = complex_product(pair[0, 0, at], pair[0, 1, at], high[0], high[1])
        if rounds:
            held[0, c, 0] = real.astype(BF16)
            held[0, c, 1] = imag.astype(BF16)
            if c < FLIGHT:
                cross_copy(0, c).start()
        else:
            branches[member, 0, rows_of(c)] = real.astype(BF16)
            branches[member, 1, rows_of(c)] = imag.astype(BF16)
            spread(c)

    for r in range(rounds - 1):
        for c in range(CHUNKS):
            select(r, c)
    for c in range(CHUNKS + 2):
        if rounds and c < CHUNKS:
            select(rounds - 1, c)
        if 1 <= c <= CHUNKS:
            on_z(c - 1)
            on_y(0, c - 1)
        if c >= 2:
            on_y(1, c - 2)
    stem_copy.wait()
    for c in range(CHUNKS):
        for i in range(4):
            core_copy(i, c).wait_recv()
    last_copy = pltpu.make_async_copy(branches.at[GROUP - 1], last_out, local_sem.at[3])
    last_copy.start()

    def columns(block):
        return pl.ds(pl.multiple_of(block * half, half), half)

    def swapped(step, index, read, target):
        copy = remote(swap.at[index], target.at[core], swap_s.at[index], swap_r.at[index], other)
        for keep in range(2):
            block = core if keep else 1 - core

            def tile(t, carry, keep=keep, block=block):
                at = pl.ds(pl.multiple_of(t * half, half), half)
                nr, ni = read(at)
                real, imag = complex_product(
                    nr, ni, branches[step, 0, :, columns(block)], branches[step, 1, :, columns(block)]
                )
                place = target.at[core] if keep else swap.at[index]
                place[0, at] = real.astype(BF16)
                place[1, at] = imag.astype(BF16)
                return carry

            lax.fori_loop(0, rows // half, tile, 0)
            if not keep:
                copy.start()
        copy.wait()

    def plain(step, source, target):
        for block in range(width // half):
            across = pl.ds(block * half, half)

            def tile(t, carry, across=across):
                at = pl.ds(pl.multiple_of(t * half, half), half)
                real, imag = complex_product(
                    jnp.concatenate([source[0, 0, at], source[1, 0, at]], axis=1),
                    jnp.concatenate([source[0, 1, at], source[1, 1, at]], axis=1),
                    branches[step, 0, :, across], branches[step, 1, :, across],
                )
                target[0, at, across] = real.astype(target.dtype)
                target[1, at, across] = imag.astype(target.dtype)
                return carry

            lax.fori_loop(0, rows // half, tile, 0)

    swapped(0, 0, lambda at: (stem[0, at].astype(BF16), stem[1, at].astype(BF16)), net1)
    plain(1, net1, net2)
    swapped(2, 1, lambda at: (net2[0, at], net2[1, at]), net3)
    net_copy = pltpu.make_async_copy(net3, net_out, local_sem.at[4])
    net_copy.start()
    net_copy.wait()
    last_copy.wait()

    leaf_copies[1].wait_send()
    pair_copy.wait_send()
    for c in range(CHUNKS):
        z_copy(c).wait_send()
        for i in range(2):
            y_copy(i, c).wait_send()
        for i in range(4):
            core_copy(i, c).wait_send()


def finish(net, branch, out):
    half = net.shape[3]
    for block in range(branch.shape[2] // half):
        across = pl.ds(block * half, half)
        real, imag = complex_product(
            jnp.concatenate([net[0, 0], net[1, 0]], axis=1),
            jnp.concatenate([net[0, 1], net[1, 1]], axis=1),
            branch[0, :, across], branch[1, :, across],
        )
        out[0, :, across] = real
        out[1, :, across] = imag


PARTS = 8
SPREAD = 8
ACROSS = 4


def dot_transposed(x, y):
    return lax.dot_general(x, y, (((1,), (1,)), ((), ())), preferred_element_type=F32)


def complex_product_transposed(ar, ai, br, bi):
    left = jnp.concatenate([ar, ai], axis=1)
    return (
        dot_transposed(left, jnp.concatenate([br, -bi], axis=1)),
        dot_transposed(left, jnp.concatenate([bi, br], axis=1)),
    )


def each(n, body):
    def step(i, carry):
        body(i)
        return carry

    lax.fori_loop(0, n, step, 0)


def matching(roots, group):
    seen = jnp.int32(0)
    found = []
    for k in range(roots.shape[0]):
        holds = jnp.where(roots[k] // GROUP == group, 1, 0)
        found.append((holds, seen))
        seen = seen + holds
    return found


def step_of(roots, group, rank):
    total = jnp.int32(0)
    for k, (holds, seen) in enumerate(matching(roots, group)):
        total = total + jnp.where(seen == rank, holds * k, 0)
    return total


def two_groups(
    third, roots, orders, stem_in, leaves_in, net_out, last_out,
    leaf, outgoing, arrived, mine, chosen, pair, branches, stem, stems, net1, net2, net3, swap, final,
    local_sem, leaf_s, leaf_r, pair_s, pair_r, whole_s, whole_r,
    y_s, y_r, core_s, core_r, mid_s, end_s, far_r, stem_s, stem_r, swap_s, swap_r,
):
    width = stem.shape[2]
    half = width // 2
    core = lax.axis_index("narrow")
    wide = lax.axis_index("wide")
    group = wide // GROUP
    member = wide % GROUP
    y = member % 2
    z = member // 2
    inner = group + z == 1
    other = {"narrow": 1 - core}
    over_y = {"wide": wide + 1 - 2 * y}
    over_z = {"wide": wide + 2 - 4 * z}
    over_mid = {"wide": wide + 2 - 4 * group}
    MESH = pl.DeviceIdType.MESH
    sets = 2 if third else 1
    left = group == 1 if third else group >= 0

    fetch = pltpu.make_async_copy(leaves_in.at[0], leaf, local_sem.at[0])
    stem_copy = pltpu.make_async_copy(stem_in, stem, local_sem.at[1])
    fetch.start()
    barrier = pltpu.get_barrier_semaphore()
    for peer in [other, over_y, over_z]:
        pl.semaphore_signal(barrier, inc=1, device_id=peer, device_id_type=MESH)

    @pl.when(inner)
    def _():
        pl.semaphore_signal(barrier, inc=1, device_id=over_mid, device_id_type=MESH)

    k_right = step_of(roots, group, 0)
    k_left = [step_of(roots, group, 1 + e) for e in range(sets)]

    def own_rows(j=0, n=1):
        size = half // n
        return pl.ds(pl.multiple_of(core * half + j * size, size), size)

    def one_hot(k):
        column = lax.broadcasted_iota(jnp.int32, (8, width), 1)
        source = jnp.zeros((8, width), jnp.int32)
        for b in range(orders.shape[1]):
            weight = jnp.left_shift(jnp.int32(1), orders[k, b])
            source = source + (jnp.right_shift(column, b) & 1) * weight

        def tile(i, carry):
            row = lax.broadcasted_iota(jnp.int32, (TILE, width), 0) + i * TILE
            at = pl.ds(pl.multiple_of(i * TILE, TILE), TILE)
            same = row == jnp.broadcast_to(source[0:1], (TILE, width))
            chosen[at] = jnp.where(same, 1.0, 0.0).astype(F32).astype(BF16)
            return carry

        lax.fori_loop(0, width // TILE, tile, 0)

    def one_hot_transposed(k):
        lanes = 128
        column = lax.broadcasted_iota(jnp.int32, (half, lanes), 0) + core * half
        source = jnp.zeros((half, lanes), jnp.int32)
        for b in range(orders.shape[1]):
            weight = jnp.where(z == 1, jnp.left_shift(jnp.int32(1), orders[k, b]), 1 << b)
            source = source + (jnp.right_shift(column, b) & 1) * weight
        for i in range(width // lanes):
            same = lax.broadcasted_iota(jnp.int32, (half, lanes), 1) + i * lanes == source
            chosen[:half, i * lanes : (i + 1) * lanes] = jnp.where(same, 1.0, 0.0).astype(F32).astype(BF16)

    def leaf_copy(e, j):
        size = half // PARTS
        at = pl.ds(pl.multiple_of(j * size, size), size)
        return remote(
            outgoing.at[e, :, at], arrived.at[e, :, own_rows(j, PARTS)], leaf_s.at[e], leaf_r.at[e, j], over_y
        )

    @pl.when(inner)
    def _():
        pl.semaphore_wait(barrier, 4)

    @pl.when(jnp.logical_not(inner))
    def _():
        pl.semaphore_wait(barrier, 3)

    @pl.when(y == 0)
    def _():
        fetch.wait()
        for c in range(2):
            outgoing[0, c] = leaf[k_right, c, own_rows()]
        each(PARTS, lambda j: leaf_copy(0, j).start())
        for e in range(sets):
            for c in range(2):
                mine[e, c] = leaf[k_left[e], c]

    @pl.when(y == 1)
    def _():
        if third:
            fetch.wait()

        @pl.when(left)
        def _():
            for e in range(sets):
                one_hot_transposed(k_left[e])
                if not third:
                    fetch.wait()
                for c in range(2):
                    outgoing[e, c] = dot_transposed(chosen[:half], leaf[k_left[e], c]).astype(BF16)
                each(PARTS, lambda j, e=e: leaf_copy(e, j).start())

        @pl.when(z == 0)
        def _():
            for c in range(2):
                mine[0, c] = leaf[k_right, c]

        @pl.when(z == 1)
        def _():
            one_hot(k_right)
            for c in range(2):
                mine[0, c] = dot(leaf[k_right, c], chosen[...]).astype(BF16)

    stem_copy.start()
    stem_copy.wait()
    for c in range(2):
        stems[core, c] = stem[c].astype(BF16)
    stem_share = remote(stems.at[core], stems.at[core], stem_s, stem_r, other)
    stem_share.start()

    def pair_copy(e, j):
        place = pair.at[e, z, :, own_rows(j, PARTS)]
        return remote(place, place, pair_s.at[e], pair_r.at[e, j], over_z)

    def whole_copy(e, j):
        place = pair.at[e, y, :, own_rows(j, PARTS)]
        return remote(place, place, whole_s.at[e], whole_r.at[e], other)

    def pairs(e, first, last):
        def turn(j):
            leaf_copy(e, j).wait_recv()
            at = own_rows(j, PARTS)

            def put(real, imag):
                pair[e, z, 0, at] = real.astype(BF16)
                pair[e, z, 1, at] = imag.astype(BF16)

            if e == 0:

                @pl.when(y == 1)
                def _():
                    put(*complex_product(arrived[e, 0, at], arrived[e, 1, at], mine[e, 0], mine[e, 1]))

            @pl.when(y == 0)
            def _():
                put(*complex_product_transposed(arrived[e, 0, at], arrived[e, 1, at], mine[e, 0], mine[e, 1]))

            pair_copy(e, j).start()

            @pl.when(z == y)
            def _():
                whole_copy(e, j).start()

        each(last - first, lambda j: turn(j + first))

    def half_pair(e):
        return pair.at[e, 0, :, own_rows()]

    def join(e):
        def arrive(j):
            pair_copy(e, j).wait_recv()

            @pl.when(z != y)
            def _():
                whole_copy(e, j).start()

        each(PARTS, arrive)
        remote(half_pair(e), half_pair(e), whole_s.at[e], whole_r.at[e], other).wait_recv()

    A, C, D, E = range(4)

    def rows_first(t):
        return t in (A, C)

    def place(t, r, n=1):
        if rows_first(t):
            size = half // SPREAD
            return branches.at[t, :, pl.ds(pl.multiple_of(core * half + r * size, size), n * size)]
        size = width // SPREAD
        return branches.at[t, :, pl.ds(pl.multiple_of(r * size, size), n * size), own_rows()]

    def y_copy(t, r, n=1):
        return remote(place(t, r, n), place(t, r, n), y_s.at[t], y_r.at[t, r], over_y)

    def core_copy(t, r, n=1):
        return remote(place(t, r, n), place(t, r, n), core_s.at[t], core_r.at[t], other)

    def mid_copy(t, r, n=1):
        return remote(place(t, r, n), place(t, r, n), mid_s.at[t], far_r.at[t, r], over_mid)

    def end_copy(t, r, n=1):
        return remote(place(t, r, n), place(t, r, n), end_s.at[t], far_r.at[t, r], over_z)

    sent = {}

    def send(copy, t, r, n):
        if copy in (mid_copy, end_copy):

            @pl.when(inner)
            def _():
                copy(t, r).start()

        else:
            copy(t, r).start()
        sent[copy, t, n] = True

    def ship(t, r):
        send(mid_copy, t, r, (0, SPREAD))
        send(y_copy, t, r, (0, SPREAD))
        send(core_copy, t, r, (0, SPREAD))

    def own(e, t):
        def turn(b):
            at = own_rows(b, 2)
            real, imag = complex_product(
                pair[e, 1 - y, 0, at], pair[e, 1 - y, 1, at], pair[e, y, 0], pair[e, y, 1]
            )
            if rows_first(t):
                branches[t, 0, at] = real.astype(BF16)
                branches[t, 1, at] = imag.astype(BF16)
                each(SPREAD // 2, lambda i: ship(t, b * (SPREAD // 2) + i))
            else:
                branches[t, 0, :, at] = real.T.astype(BF16)
                branches[t, 1, :, at] = imag.T.astype(BF16)

        each(2, turn)
        if not rows_first(t):
            each(SPREAD, lambda r: ship(t, r))

    def receive(first, last, *turns):
        def turn(i):
            for t, origin, onward, shift in turns:
                r = i + first + shift
                span = (first + shift, last + shift)
                if origin == "z":
                    mid_copy(t, r).wait_recv()
                else:
                    y_copy(t, r).wait_recv()
                for letter, copy in (("e", end_copy), ("m", mid_copy), ("y", y_copy)):
                    if letter in onward:
                        send(copy, t, r, span)
                send(core_copy, t, r, span)

        each(last - first, turn)

    def exchange(far, beside, beyond):
        receive(0, ACROSS, (far, "z", "ey", 0), (beside, "y", "", 0))
        receive(ACROSS, SPREAD, (far, "z", "e", 0), (beside, "y", "m", 0))
        if 2 * ACROSS == SPREAD:
            receive(0, ACROSS, (beyond, "y", "", 0), (beyond, "z", "e", ACROSS))
        else:
            receive(0, ACROSS, (beyond, "y", "", 0))
            receive(ACROSS, SPREAD, (beyond, "z", "e", 0))

    def build(t):
        pairs(0, 0, PARTS)
        join(0)
        own(0, t)

    def role_right_low():
        build(A)
        if third:
            receive(0, SPREAD, (C, "z", "ey", 0))
            receive(0, SPREAD, (E, "y", "", 0))
            receive(0, SPREAD, (D, "y", "", 0))
        else:
            exchange(C, D, E)

    def role_right_high():
        build(C)
        if third:
            receive(0, SPREAD, (A, "z", "e", 0), (E, "y", "", 0))
            receive(0, SPREAD, (D, "y", "", 0))
        else:
            exchange(A, E, D)

    def role_left_low():
        if third:
            receive(0, SPREAD, (A, "y", "m", 0), (E, "z", "ey", 0))
            receive(0, SPREAD, (C, "y", "", 0), (D, "z", "ey", 0))
        else:
            build(D)
            exchange(E, A, C)

    def role_left_high():
        if third:
            pairs(0, 0, PARTS)
            pairs(1, 0, 2)
            join(0)
            own(0, E)
            pairs(1, 2, PARTS)
            join(1)
            own(1, D)
            receive(0, SPREAD, (A, "z", "e", 0))
            receive(0, SPREAD, (C, "y", "", 0))
        else:
            build(E)
            exchange(D, C, A)

    roles = [(1, 0, role_right_low), (1, 1, role_right_high), (0, 0, role_left_low), (0, 1, role_left_high)]
    drains = []
    for at_y, at_group, role in roles:
        sent.clear()
        here = jnp.logical_and(y == at_y, group == at_group)
        pl.when(here)(role)
        drains.append((here, list(sent)))

    stem_share.wait()
    for t in range(4):
        core_copy(t, 0, SPREAD).wait_recv()

    zeros = matching(roots, 0)
    ones = matching(roots, 1)
    source = []
    for k in range(roots.shape[0]):
        high = jnp.where(ones[k][1] == 2, D, C + 2 * ones[k][1])
        at = jnp.where(zeros[k][0] == 1, A + 2 * zeros[k][1], high)
        source.append(jnp.minimum(at, 3))

    def columns(block):
        return pl.ds(pl.multiple_of(block * half, half), half)

    for c in range(2):
        final[c] = branches[source[3], c]
    last_copy = pltpu.make_async_copy(final, last_out, local_sem.at[2])
    last_copy.start()

    def first(i, carry):
        real, imag = complex_product(
            stems[i, 0], stems[i, 1],
            branches[source[0], 0, :, columns(core)], branches[source[0], 1, :, columns(core)],
        )
        net1[i, 0] = real.astype(BF16)
        net1[i, 1] = imag.astype(BF16)
        return carry

    lax.fori_loop(0, 2, first, 0)

    def second(block, carry):
        real, imag = complex_product(
            jnp.concatenate([net1[0, 0], net1[1, 0]], axis=1),
            jnp.concatenate([net1[0, 1], net1[1, 1]], axis=1),
            branches[source[1], 0, :, columns(block)], branches[source[1], 1, :, columns(block)],
        )
        net2[0, :, columns(block)] = real.astype(BF16)
        net2[1, :, columns(block)] = imag.astype(BF16)
        return carry

    lax.fori_loop(0, 2, second, 0)

    swap_copy = remote(swap.at[0], net3, swap_s, swap_r, other)
    kept = pltpu.make_async_copy(swap.at[1], net_out.at[core], local_sem.at[3])
    came = pltpu.make_async_copy(net3, net_out.at[1 - core], local_sem.at[0])

    def third_step(i):
        block = core + (1 - i) * (1 - 2 * core)
        real, imag = complex_product(
            net2[0], net2[1], branches[source[2], 0, :, columns(block)], branches[source[2], 1, :, columns(block)]
        )
        swap[i, 0] = real.astype(BF16)
        swap[i, 1] = imag.astype(BF16)

        @pl.when(i == 0)
        def _():
            swap_copy.start()

    each(2, third_step)
    kept.start()
    swap_copy.wait()
    came.start()
    kept.wait()
    came.wait()
    last_copy.wait()

    def drain(e):
        place = half_pair(e)
        remote(place, place, pair_s.at[e], pair_r.at[e, 0], over_z).wait_send()
        remote(place, place, whole_s.at[e], whole_r.at[e], other).wait_send()

    def drain_leaf(e):
        place = arrived.at[e, :, own_rows()]
        remote(outgoing.at[e], place, leaf_s.at[e], leaf_r.at[e, 0], over_y).wait_send()

    @pl.when(y == 0)
    def _():
        drain_leaf(0)

        @pl.when(left)
        def _():
            for e in range(sets):
                drain(e)

    @pl.when(y == 1)
    def _():
        drain(0)

        @pl.when(left)
        def _():
            for e in range(sets):
                drain_leaf(e)

    for here, copies in drains:
        totals = {}
        for copy, t, (low, high) in copies:
            totals[copy, t] = totals.get((copy, t), 0) + high - low

        @pl.when(here)
        def _(totals=totals):
            for (copy, t), n in totals.items():
                if copy not in (mid_copy, end_copy):
                    copy(t, 0, n).wait_send()

            @pl.when(inner)
            def _():
                for (copy, t), n in totals.items():
                    if copy in (mid_copy, end_copy):
                        copy(t, 0, n).wait_send()


def general(stem_tensor, leaves, root_devices, mode_orders):
    _, rows, width = stem_tensor.shape
    half = width // 2
    part = half // CHUNKS
    groups = lax.axis_size("wide") // GROUP
    rounds = groups.bit_length() - 1
    vmem = pltpu.VMEM
    dma = pltpu.SemaphoreType.DMA
    network, last = pl.pallas_call(
        functools.partial(kernel, rounds),
        out_shape=(
            jax.ShapeDtypeStruct((2, 2, rows, half), BF16),
            jax.ShapeDtypeStruct((2, width, width), BF16),
        ),
        in_specs=[pl.BlockSpec(memory_space=pltpu.SMEM)] * 2
        + [pl.BlockSpec(memory_space=pl.ANY)] * 2,
        out_specs=[pl.BlockSpec(memory_space=pl.ANY)] * 2,
        scratch_shapes=[
            vmem((2, 2, 2, width, width), BF16),
            vmem((2, 2, half, width), BF16),
            vmem((2, half, width), BF16),
            vmem((2, width, width), BF16),
            vmem((width, width), BF16),
            vmem((max(rounds, 1), CHUNKS, 2, part, width), BF16),
            vmem((max(rounds, 1), CHUNKS, 2, part, width), BF16),
            vmem((GROUP, 2, width, width), BF16),
            vmem((2, rows, width), F32),
            vmem((2, 2, rows, half), BF16),
            vmem((2, rows, width), BF16),
            vmem((2, 2, rows, half), BF16),
            vmem((2, 2, rows, half), BF16),
            dma((5,)),
            dma((2,)), dma((2,)), dma((2,)), dma((2,)),
            dma, dma, dma, dma,
            dma((max(rounds, 1), CHUNKS)), dma((max(rounds, 1), CHUNKS)),
            dma((CHUNKS,)), dma((CHUNKS,)),
            dma((2, CHUNKS)), dma((2, CHUNKS)),
            dma((4, CHUNKS)), dma((4, CHUNKS)),
            dma((2,)), dma((2,)),
        ],
        compiler_params=pltpu.CompilerParams(collective_id=0, has_side_effects=True),
    )(root_devices, mode_orders, stem_tensor, leaves)
    return network, last


def closing(network, last, stem_tensor):
    _, rows, width = stem_tensor.shape
    half = width // 2
    return pl.pallas_call(
        finish,
        grid=(rows // half,),
        out_shape=jax.ShapeDtypeStruct(stem_tensor.shape, F32),
        in_specs=[
            pl.BlockSpec((2, 2, half, half), lambda i: (0, 0, i, 0)),
            pl.BlockSpec((2, width, width), lambda i: (0, 0, 0)),
        ],
        out_specs=pl.BlockSpec((2, half, width), lambda i: (0, i, 0)),
    )(network, last)


def split(third, stem_tensor, leaves, root_devices, mode_orders):
    _, rows, width = stem_tensor.shape
    half = width // 2
    sets = 2 if third else 1
    vmem = pltpu.VMEM
    dma = pltpu.SemaphoreType.DMA
    return pl.pallas_call(
        functools.partial(two_groups, third),
        out_shape=(
            jax.ShapeDtypeStruct((2, 2, rows, half), BF16),
            jax.ShapeDtypeStruct((2, width, width), BF16),
        ),
        in_specs=[pl.BlockSpec(memory_space=pltpu.SMEM)] * 2
        + [pl.BlockSpec(memory_space=pl.ANY)] * 2,
        out_specs=[pl.BlockSpec(memory_space=pl.ANY)] * 2,
        scratch_shapes=[
            vmem((leaves.shape[1], 2, width, width), BF16),
            vmem((sets, 2, half, width), BF16),
            vmem((sets, 2, width, width), BF16),
            vmem((sets, 2, width, width), BF16),
            vmem((width, width), BF16),
            vmem((sets, 2, 2, width, width), BF16),
            vmem((4, 2, width, width), BF16),
            vmem((2, rows, width), F32),
            vmem((2, 2, rows, width), BF16),
            vmem((2, 2, rows, half), BF16),
            vmem((2, rows, width), BF16),
            vmem((2, rows, half), BF16),
            vmem((2, 2, rows, half), BF16),
            vmem((2, width, width), BF16),
            dma((4,)),
        ]
        + [dma((sets,)), dma((sets, PARTS)), dma((sets,)), dma((sets, PARTS)), dma((sets,)), dma((sets,))]
        + [dma((4,)), dma((4, SPREAD)), dma((4,)), dma((4,)), dma((4,)), dma((4,)), dma((4, SPREAD))]
        + [dma] * 4,
        compiler_params=pltpu.CompilerParams(collective_id=2 if third else 1, has_side_effects=True),
    )(root_devices, mode_orders, stem_tensor, leaves)


def local(stem_tensor, leaves, root_devices, mode_orders):
    arrays = (stem_tensor, leaves, root_devices, mode_orders)
    if lax.axis_size("wide") // GROUP == 2:
        even = jnp.sum((root_devices // GROUP).astype(jnp.int32)) == 2
        network, last = lax.cond(
            even, functools.partial(split, False), functools.partial(split, True), *arrays
        )
    else:
        network, last = general(*arrays)
    return closing(network, last, stem_tensor)


def solution(mesh):
    stem_spec = P(None, ("cuts", "wide", "narrow"), None)
    return jax.shard_map(
        local,
        mesh=mesh,
        in_specs=(stem_spec, P(("cuts", "wide"), None, None, None, None), P(), P()),
        out_specs=stem_spec,
        check_vma=False,
    )
```

```python
import functools

import jax
import jax.numpy as jnp
from jax import lax
from jax.experimental import pallas as pl
from jax.experimental.pallas import tpu as pltpu
from jax.sharding import PartitionSpec as P

GROUP = 4
CHUNKS = 8
FLIGHT = 2
TILE = 128
BF16 = jnp.bfloat16
F32 = jnp.float32


def dot(x, y):
    return jnp.dot(x, y, preferred_element_type=F32)


def complex_product(ar, ai, br, bi):
    left = jnp.concatenate([ar, ai], axis=1)
    return (
        dot(left, jnp.concatenate([br, -bi], axis=0)),
        dot(left, jnp.concatenate([bi, br], axis=0)),
    )


def remote(src, dst, send_sem, recv_sem, device):
    return pltpu.make_async_remote_copy(
        src_ref=src,
        dst_ref=dst,
        send_sem=send_sem,
        recv_sem=recv_sem,
        device_id=device,
        device_id_type=pl.DeviceIdType.MESH,
    )


def kernel(
    rounds, roots, orders, stem_in, leaves_in, net_out, last_out,
    leaf, pair, away, high, chosen, held, crossed, branches, stem, net1, net2, net3, swap,
    local_sem, leaf_s, leaf_r, fwd_s, fwd_r, pair_s, pair_r, high_s, high_r,
    cross_s, cross_r, z_s, z_r, y_s, y_r, core_s, core_r, swap_s, swap_r,
):
    width = stem.shape[2]
    rows = stem.shape[1]
    half = width // 2
    part = half // CHUNKS
    core = lax.axis_index("narrow")
    wide = lax.axis_index("wide")
    member = wide % GROUP
    y = member % 2
    z = member // 2
    other = {"narrow": 1 - core}
    over_y = {"wide": wide + 1 - 2 * y}
    over_z = {"wide": wide + 2 - 4 * z}
    bits = [(wide // (GROUP << r)) % 2 for r in range(rounds)]
    over_group = [{"wide": wide + (GROUP << r) * (1 - 2 * bits[r])} for r in range(rounds)]

    barrier = pltpu.get_barrier_semaphore()
    for peer in [other, over_y, over_z] + over_group:
        pl.semaphore_signal(barrier, inc=1, device_id=peer, device_id_type=pl.DeviceIdType.MESH)
    own_rows = pl.ds(pl.multiple_of(core * half, half), half)
    own_copies = [
        pltpu.make_async_copy(leaves_in.at[0, 2 * s + y], leaf.at[s, y], local_sem.at[s])
        for s in range(2)
    ]
    stem_copy = pltpu.make_async_copy(stem_in, stem, local_sem.at[2])
    pl.semaphore_wait(barrier, 3 + rounds)

    phases = [1 - z, z]
    leaf_copies = []
    for i, s in enumerate(phases):
        copy = remote(
            leaves_in.at[0, 2 * s + 1 - y, :, own_rows],
            leaf.at[s, y, :, own_rows],
            leaf_s.at[i], leaf_r.at[i], over_y,
        )
        leaf_copies.append(copy)
    leaf_copies[0].start()
    for copy in own_copies:
        copy.start()
    stem_copy.start()

    def choose(i, carry):
        column = lax.broadcasted_iota(jnp.int32, (TILE, width), 1)
        source = jnp.zeros((TILE, width), jnp.int32)
        for b in range(orders.shape[1]):
            weight = jnp.left_shift(jnp.int32(1), orders[member, b])
            source = source + (jnp.right_shift(column, b) & 1) * weight
        row = lax.broadcasted_iota(jnp.int32, (TILE, width), 0) + i * TILE
        at = pl.ds(pl.multiple_of(i * TILE, TILE), TILE)
        chosen[at] = jnp.where(row == source, 1.0, 0.0).astype(F32).astype(BF16)
        return carry

    lax.fori_loop(0, width // TILE, choose, 0)
    for copy in own_copies:
        copy.wait()

    pair_copy = remote(away, pair.at[z], pair_s, pair_r, over_z)
    leaf_copies[0].wait_send()
    leaf_copies[1].start()
    for i, s in enumerate(phases):
        leaf_copies[i].wait_recv()
        forward = remote(
            leaf.at[s, 1 - y, :, own_rows], leaf.at[s, 1 - y, :, own_rows],
            fwd_s.at[i], fwd_r.at[i], other,
        )
        forward.start()
        forward.wait()

        def pair_tile(t, carry, s=s, i=i):
            at = pl.ds(pl.multiple_of(t * half, half), half)
            real, imag = complex_product(
                leaf[s, 0, 0, own_rows], leaf[s, 0, 1, own_rows],
                leaf[s, 1, 0, :, at], leaf[s, 1, 1, :, at],
            )
            target = away if i == 0 else pair.at[z]
            target[0, :, at] = real.astype(BF16)
            target[1, :, at] = imag.astype(BF16)
            return carry

        lax.fori_loop(0, width // half, pair_tile, 0)
        if i == 0:
            pair_copy.start()
    pair_copy.wait_recv()

    def high_tile(t, carry):
        at = pl.ds(pl.multiple_of(t * half, half), half)
        for c in range(2):
            high[c, own_rows, at] = dot(pair[1, c], chosen[:, at]).astype(BF16)
        return carry

    lax.fori_loop(0, width // half, high_tile, 0)
    high_copy = remote(high.at[:, own_rows], high.at[:, own_rows], high_s, high_r, other)
    high_copy.start()
    high_copy.wait()

    def rows_of(c):
        return pl.ds(pl.multiple_of(core * half + c * part, part), part)

    def cross_copy(r, c):
        return remote(held.at[r, c], crossed.at[r, c], cross_s.at[r, c], cross_r.at[r, c], over_group[r])

    def place(origin, c):
        return branches.at[origin, :, rows_of(c)]

    origins = [member, member + 2 - 4 * z, member + 1 - 2 * y, GROUP - 1 - member]

    def z_copy(c):
        return remote(place(origins[0], c), place(origins[0], c), z_s.at[c], z_r.at[c], over_z)

    def y_copy(i, c):
        return remote(place(origins[i], c), place(origins[i], c), y_s.at[i, c], y_r.at[i, c], over_y)

    def core_copy(i, c):
        return remote(place(origins[i], c), place(origins[i], c), core_s.at[i, c], core_r.at[i, c], other)

    def spread(c):
        z_copy(c).start()
        y_copy(0, c).start()
        core_copy(0, c).start()

    def select(r, c):
        cross_copy(r, c).wait_recv()
        cross_copy(r, c).wait_send()
        if c + FLIGHT < CHUNKS:
            cross_copy(r, c + FLIGHT).start()
        root_bit = (roots[member] // (GROUP << r)) % 2
        for p in range(2):
            here = held[r, c, p].astype(F32)
            there = crossed[r, c, p].astype(F32)
            same = jnp.full(here.shape, root_bit, jnp.int32) == bits[r]
            picked = jnp.where(same, here, there).astype(BF16)
            if r + 1 < rounds:
                held[r + 1, c, p] = picked
            else:
                branches[member, p, rows_of(c)] = picked
        if r + 1 < rounds:
            if c < FLIGHT:
                cross_copy(r + 1, c).start()
        else:
            spread(c)

    def on_z(c):
        z_copy(c).wait_recv()
        y_copy(1, c).start()
        core_copy(1, c).start()

    def on_y(i, c):
        y_copy(i, c).wait_recv()
        core_copy(2 + i, c).start()

    for c in range(CHUNKS):
        at = pl.ds(c * part, part)
        real, imag = complex_product(pair[0, 0, at], pair[0, 1, at], high[0], high[1])
        if rounds:
            held[0, c, 0] = real.astype(BF16)
            held[0, c, 1] = imag.astype(BF16)
            if c < FLIGHT:
                cross_copy(0, c).start()
        else:
            branches[member, 0, rows_of(c)] = real.astype(BF16)
            branches[member, 1, rows_of(c)] = imag.astype(BF16)
            spread(c)

    for r in range(rounds - 1):
        for c in range(CHUNKS):
            select(r, c)
    for c in range(CHUNKS + 2):
        if rounds and c < CHUNKS:
            select(rounds - 1, c)
        if 1 <= c <= CHUNKS:
            on_z(c - 1)
            on_y(0, c - 1)
        if c >= 2:
            on_y(1, c - 2)
    stem_copy.wait()
    for c in range(CHUNKS):
        for i in range(4):
            core_copy(i, c).wait_recv()
    last_copy = pltpu.make_async_copy(branches.at[GROUP - 1], last_out, local_sem.at[3])
    last_copy.start()

    def columns(block):
        return pl.ds(pl.multiple_of(block * half, half), half)

    def swapped(step, index, read, target):
        copy = remote(swap.at[index], target.at[core], swap_s.at[index], swap_r.at[index], other)
        for keep in range(2):
            block = core if keep else 1 - core

            def tile(t, carry, keep=keep, block=block):
                at = pl.ds(pl.multiple_of(t * half, half), half)
                nr, ni = read(at)
                real, imag = complex_product(
                    nr, ni, branches[step, 0, :, columns(block)], branches[step, 1, :, columns(block)]
                )
                place = target.at[core] if keep else swap.at[index]
                place[0, at] = real.astype(BF16)
                place[1, at] = imag.astype(BF16)
                return carry

            lax.fori_loop(0, rows // half, tile, 0)
            if not keep:
                copy.start()
        copy.wait()

    def plain(step, source, target):
        for block in range(width // half):
            across = pl.ds(block * half, half)

            def tile(t, carry, across=across):
                at = pl.ds(pl.multiple_of(t * half, half), half)
                real, imag = complex_product(
                    jnp.concatenate([source[0, 0, at], source[1, 0, at]], axis=1),
                    jnp.concatenate([source[0, 1, at], source[1, 1, at]], axis=1),
                    branches[step, 0, :, across], branches[step, 1, :, across],
                )
                target[0, at, across] = real.astype(target.dtype)
                target[1, at, across] = imag.astype(target.dtype)
                return carry

            lax.fori_loop(0, rows // half, tile, 0)

    swapped(0, 0, lambda at: (stem[0, at].astype(BF16), stem[1, at].astype(BF16)), net1)
    plain(1, net1, net2)
    swapped(2, 1, lambda at: (net2[0, at], net2[1, at]), net3)
    net_copy = pltpu.make_async_copy(net3, net_out, local_sem.at[4])
    net_copy.start()
    net_copy.wait()
    last_copy.wait()

    leaf_copies[1].wait_send()
    pair_copy.wait_send()
    for c in range(CHUNKS):
        z_copy(c).wait_send()
        for i in range(2):
            y_copy(i, c).wait_send()
        for i in range(4):
            core_copy(i, c).wait_send()


def finish(net, branch, out):
    half = net.shape[3]
    for block in range(branch.shape[2] // half):
        across = pl.ds(block * half, half)
        real, imag = complex_product(
            jnp.concatenate([net[0, 0], net[1, 0]], axis=1),
            jnp.concatenate([net[0, 1], net[1, 1]], axis=1),
            branch[0, :, across], branch[1, :, across],
        )
        out[0, :, across] = real
        out[1, :, across] = imag


PARTS = 8
SPREAD = 8
ACROSS = 6
HALVE = 4
STAGES = 1


def dot_transposed(x, y):
    return lax.dot_general(x, y, (((1,), (1,)), ((), ())), preferred_element_type=F32)


def complex_product_transposed(ar, ai, br, bi):
    left = jnp.concatenate([ar, ai], axis=1)
    return (
        dot_transposed(left, jnp.concatenate([br, -bi], axis=1)),
        dot_transposed(left, jnp.concatenate([bi, br], axis=1)),
    )


def each(n, body):
    def step(i, carry):
        body(i)
        return carry

    lax.fori_loop(0, n, step, 0)


def matching(roots, group):
    seen = jnp.int32(0)
    found = []
    for k in range(roots.shape[0]):
        holds = jnp.where(roots[k] // GROUP == group, 1, 0)
        found.append((holds, seen))
        seen = seen + holds
    return found


def step_of(roots, group, rank):
    total = jnp.int32(0)
    for k, (holds, seen) in enumerate(matching(roots, group)):
        total = total + jnp.where(seen == rank, holds * k, 0)
    return total


def two_groups(
    third, roots_in, orders_in, stem_in, leaves_in, net_out, last_out, roots, orders,
    leaf, outgoing, arrived, mine, chosen, pair, branches, stem, stems, net1, net2, net3, final,
    local_sem, leaf_s, leaf_r, pair_s, pair_r, whole_s, whole_r,
    y_s, y_r, core_s, core_r, mid_s, end_s, far_r, stem_s, stem_r, swap_s, swap_r,
):
    width = stem.shape[2]
    half = width // 2
    core = lax.axis_index("narrow")
    wide = lax.axis_index("wide")
    group = wide // GROUP
    member = wide % GROUP
    y = member % 2
    z = member // 2
    inner = group + z == 1
    other = {"narrow": 1 - core}
    over_y = {"wide": wide + 1 - 2 * y}
    over_z = {"wide": wide + 2 - 4 * z}
    over_mid = {"wide": wide + 2 - 4 * group}
    MESH = pl.DeviceIdType.MESH
    sets = 2 if third else 1
    left = group == 1 if third else group >= 0

    fetch = pltpu.make_async_copy(leaves_in.at[0], leaf, local_sem.at[0])
    stem_copy = pltpu.make_async_copy(stem_in, stem, local_sem.at[1])
    fetch.start()
    barrier = pltpu.get_barrier_semaphore()
    for peer in [other, over_y, over_z]:
        pl.semaphore_signal(barrier, inc=1, device_id=peer, device_id_type=MESH)

    @pl.when(inner)
    def _():
        pl.semaphore_signal(barrier, inc=1, device_id=over_mid, device_id_type=MESH)

    scalars = [
        pltpu.make_async_copy(roots_in, roots, local_sem.at[2]),
        pltpu.make_async_copy(orders_in, orders, local_sem.at[3]),
    ]
    for copy in scalars:
        copy.start()
    for copy in scalars:
        copy.wait()
    k_right = step_of(roots, group, 0)
    k_left = [step_of(roots, group, 1 + e) for e in range(sets)]

    def own_rows(j=0, n=1):
        size = half // n
        return pl.ds(pl.multiple_of(core * half + j * size, size), size)

    def one_hot(k):
        column = lax.broadcasted_iota(jnp.int32, (8, width), 1)
        source = jnp.zeros((8, width), jnp.int32)
        for b in range(orders.shape[1]):
            weight = jnp.left_shift(jnp.int32(1), orders[k, b])
            source = source + (jnp.right_shift(column, b) & 1) * weight

        def tile(i, carry):
            row = lax.broadcasted_iota(jnp.int32, (TILE, width), 0) + i * TILE
            at = pl.ds(pl.multiple_of(i * TILE, TILE), TILE)
            same = row == jnp.broadcast_to(source[0:1], (TILE, width))
            chosen[at] = jnp.where(same, 1.0, 0.0).astype(F32).astype(BF16)
            return carry

        lax.fori_loop(0, width // TILE, tile, 0)

    def one_hot_transposed(k):
        lanes = 128
        column = lax.broadcasted_iota(jnp.int32, (half, lanes), 0) + core * half
        source = jnp.zeros((half, lanes), jnp.int32)
        for b in range(orders.shape[1]):
            weight = jnp.where(z == 1, jnp.left_shift(jnp.int32(1), orders[k, b]), 1 << b)
            source = source + (jnp.right_shift(column, b) & 1) * weight
        for i in range(width // lanes):
            same = lax.broadcasted_iota(jnp.int32, (half, lanes), 1) + i * lanes == source
            chosen[:half, i * lanes : (i + 1) * lanes] = jnp.where(same, 1.0, 0.0).astype(F32).astype(BF16)

    def leaf_copy(e, j):
        size = half // PARTS
        at = pl.ds(pl.multiple_of(j * size, size), size)
        return remote(
            outgoing.at[e, :, at], arrived.at[e, :, own_rows(j, PARTS)], leaf_s.at[e], leaf_r.at[e, j], over_y
        )

    @pl.when(y == 1)
    def _():
        @pl.when(left)
        def _():
            one_hot_transposed(k_left[0])

    @pl.when(inner)
    def _():
        pl.semaphore_wait(barrier, 4)

    @pl.when(jnp.logical_not(inner))
    def _():
        pl.semaphore_wait(barrier, 3)

    @pl.when(y == 0)
    def _():
        fetch.wait()
        for c in range(2):
            outgoing[0, c] = leaf[k_right, c, own_rows()]
        each(PARTS, lambda j: leaf_copy(0, j).start())
        for e in range(sets):
            for c in range(2):
                mine[e, c] = leaf[k_left[e], c]

    @pl.when(y == 1)
    def _():
        fetch.wait()

        @pl.when(left)
        def _():
            for e in range(sets):
                if e:
                    one_hot_transposed(k_left[e])

                def stage(i, e=e):
                    size = half // STAGES
                    at = pl.ds(pl.multiple_of(i * size, size), size)
                    for c in range(2):
                        outgoing[e, c, at] = dot_transposed(chosen[at], leaf[k_left[e], c]).astype(BF16)
                    each(PARTS // STAGES, lambda j: leaf_copy(e, i * (PARTS // STAGES) + j).start())

                each(STAGES, stage)

        @pl.when(z == 0)
        def _():
            for c in range(2):
                mine[0, c] = leaf[k_right, c]

        @pl.when(z == 1)
        def _():
            one_hot(k_right)
            for c in range(2):
                mine[0, c] = dot(leaf[k_right, c], chosen[...]).astype(BF16)

    stem_copy.start()
    stem_copy.wait()
    for c in range(2):
        stems[core, c] = stem[c].astype(BF16)
    stem_share = remote(stems.at[core], stems.at[core], stem_s, stem_r, other)
    stem_share.start()

    def pair_copy(e, j):
        place = pair.at[e, z, :, own_rows(j, PARTS)]
        return remote(place, place, pair_s.at[e], pair_r.at[e, j], over_z)

    def whole_copy(e, j):
        place = pair.at[e, y, :, own_rows(j, PARTS)]
        return remote(place, place, whole_s.at[e], whole_r.at[e], other)

    def pairs(e, first, last):
        def turn(j):
            leaf_copy(e, j).wait_recv()
            at = own_rows(j, PARTS)

            def put(real, imag):
                pair[e, z, 0, at] = real.astype(BF16)
                pair[e, z, 1, at] = imag.astype(BF16)

            if e == 0:

                @pl.when(y == 1)
                def _():
                    put(*complex_product(arrived[e, 0, at], arrived[e, 1, at], mine[e, 0], mine[e, 1]))

            @pl.when(y == 0)
            def _():
                put(*complex_product_transposed(arrived[e, 0, at], arrived[e, 1, at], mine[e, 0], mine[e, 1]))

            pair_copy(e, j).start()

            @pl.when(z == y)
            def _():
                whole_copy(e, j).start()

        each(last - first, lambda j: turn(j + first))

    def half_pair(e):
        return pair.at[e, 0, :, own_rows()]

    def join(e):
        def arrive(j):
            pair_copy(e, j).wait_recv()

            @pl.when(z != y)
            def _():
                whole_copy(e, j).start()

        each(PARTS, arrive)
        remote(half_pair(e), half_pair(e), whole_s.at[e], whole_r.at[e], other).wait_recv()

    A, C, D, E = range(4)

    def rows_first(t):
        return t in (A, C)

    def place(t, r, n=1):
        if rows_first(t):
            size = half // SPREAD
            return branches.at[t, :, pl.ds(pl.multiple_of(core * half + r * size, size), n * size)]
        size = width // SPREAD
        if n > 1:
            return branches.at[t, :, : n * size, own_rows()]
        row = (r % (SPREAD // 2)) * (2 * size)
        return branches.at[t, :, pl.ds(pl.multiple_of(row, size), 2 * size), own_rows(r // (SPREAD // 2), 2)]

    def y_copy(t, r, n=1):
        return remote(place(t, r, n), place(t, r, n), y_s.at[t], y_r.at[t, r], over_y)

    def core_copy(t, r, n=1):
        return remote(place(t, r, n), place(t, r, n), core_s.at[t], core_r.at[t], other)

    def mid_copy(t, r, n=1):
        return remote(place(t, r, n), place(t, r, n), mid_s.at[t], far_r.at[t, r], over_mid)

    def end_copy(t, r, n=1):
        return remote(place(t, r, n), place(t, r, n), end_s.at[t], far_r.at[t, r], over_z)

    sent = {}

    def send(copy, t, r, n):
        if copy in (mid_copy, end_copy):

            @pl.when(inner)
            def _():
                copy(t, r).start()

        else:
            copy(t, r).start()
        sent[copy, t, n] = True

    def ship(t, r):
        send(mid_copy, t, r, (0, SPREAD))
        send(y_copy, t, r, (0, SPREAD))
        send(core_copy, t, r, (0, SPREAD))

    def own(e, t):
        def turn(b):
            at = own_rows(b, 2)
            real, imag = complex_product(
                pair[e, 1 - y, 0, at], pair[e, 1 - y, 1, at], pair[e, y, 0], pair[e, y, 1]
            )
            if rows_first(t):
                branches[t, 0, at] = real.astype(BF16)
                branches[t, 1, at] = imag.astype(BF16)
                each(SPREAD // 2, lambda i: ship(t, b * (SPREAD // 2) + i))
            else:
                branches[t, 0, :, at] = real.T.astype(BF16)
                branches[t, 1, :, at] = imag.T.astype(BF16)
                if not e:
                    each(SPREAD // 2, lambda i: ship(t, b * (SPREAD // 2) + i))

        each(2, turn)
        if e:
            each(HALVE, lambda r: send(mid_copy, t, r, (0, HALVE)))

            def turn_sent(i):
                r = (i + HALVE) % SPREAD
                send(y_copy, t, r, (0, SPREAD))
                send(core_copy, t, r, (0, SPREAD))

            each(SPREAD, turn_sent)

    def receive(first, last, *turns):
        def turn(i):
            for t, origin, onward, shift in turns:
                r = i + first + shift
                span = (first + shift, last + shift)
                if origin == "z":
                    mid_copy(t, r).wait_recv()
                else:
                    y_copy(t, r).wait_recv()
                for letter, copy in (("e", end_copy), ("m", mid_copy), ("y", y_copy)):
                    if letter in onward:
                        send(copy, t, r, span)
                send(core_copy, t, r, span)

        each(last - first, turn)

    def exchange(far, beside, beyond):
        receive(0, ACROSS, (far, "z", "ey", 0), (beside, "y", "", 0))
        receive(ACROSS, SPREAD, (far, "z", "e", 0), (beside, "y", "m", 0))
        if 2 * ACROSS == SPREAD:
            receive(0, ACROSS, (beyond, "y", "", 0), (beyond, "z", "e", ACROSS))
        else:
            receive(ACROSS, SPREAD, (beyond, "z", "e", 0))
            receive(0, ACROSS, (beyond, "y", "", 0))

    def build(t):
        pairs(0, 0, PARTS)
        join(0)
        own(0, t)

    def role_right_low():
        build(A)
        if third:
            receive(0, SPREAD, (C, "z", "ey", 0))
            receive(0, SPREAD, (E, "y", "", 0))
        else:
            exchange(C, D, E)

    def role_right_high():
        build(C)
        if third:
            receive(0, SPREAD, (A, "z", "e", 0), (E, "y", "", 0))
        else:
            exchange(A, E, D)

    def role_left_low():
        if third:
            receive(0, SPREAD, (A, "y", "m", 0), (E, "z", "ey", 0))
            receive(0, SPREAD, (C, "y", "", 0))
        else:
            build(D)
            exchange(E, A, C)

    def role_left_high():
        if third:
            pairs(0, 0, PARTS)
            pairs(1, 0, PARTS // 4)
            join(0)
            own(0, E)
            pairs(1, PARTS // 4, PARTS)
            join(1)
            own(1, D)
            receive(0, SPREAD, (A, "z", "e", 0))
            receive(0, SPREAD, (C, "y", "", 0))
        else:
            build(E)
            exchange(D, C, A)

    def last_right_low():
        receive(HALVE, SPREAD, (D, "z", "ey", 0))
        receive(0, HALVE, (D, "y", "", 0))

    def last_right_high():
        receive(HALVE, SPREAD, (D, "y", "m", 0))
        receive(0, HALVE, (D, "y", "", 0))

    def last_left_low():
        receive(0, HALVE, (D, "z", "ey", 0))
        receive(HALVE, SPREAD, (D, "y", "", 0))

    drains = []

    def play(roles):
        for at_y, at_group, role in roles:
            sent.clear()
            here = jnp.logical_and(y == at_y, group == at_group)
            pl.when(here)(role)
            drains.append((here, list(sent)))

    def columns(block):
        return pl.ds(pl.multiple_of(block * half, half), half)

    zeros = matching(roots, 0)
    ones = matching(roots, 1)
    source = []
    for k in range(roots.shape[0]):
        high = jnp.where(ones[k][1] == 2, D, C + 2 * ones[k][1])
        at = jnp.where(zeros[k][0] == 1, A + 2 * zeros[k][1], high)
        source.append(jnp.minimum(at, 3))

    def first():
        def turn(i):
            picked = []
            for c in range(2):
                one = branches[A, c, :, columns(core)]
                two = branches[C, c, :, columns(core)]
                if third:
                    picked.append(jnp.where(jnp.full(one.shape, source[0], jnp.int32) == A, one, two))
                else:
                    picked.append(branches[source[0], c, :, columns(core)])
            real, imag = complex_product(stems[i, 0], stems[i, 1], *picked)
            net1[i, 0] = real.astype(BF16)
            net1[i, 1] = imag.astype(BF16)

        each(2, turn)

    play([(1, 0, role_right_low), (1, 1, role_right_high), (0, 0, role_left_low), (0, 1, role_left_high)])
    stem_share.wait()
    for t in (A, C):
        core_copy(t, 0, SPREAD).wait_recv()
    if third:
        first()
        play([(1, 0, last_right_low), (1, 1, last_right_high), (0, 0, last_left_low)])
    for t in (D, E):
        core_copy(t, 0, SPREAD).wait_recv()
    for c in range(2):
        final[c] = branches[source[3], c]
    last_copy = pltpu.make_async_copy(final, last_out, local_sem.at[2])
    last_copy.start()
    if not third:
        first()

    def exchange_copy(i):
        at = pl.ds(pl.multiple_of(i * TILE, TILE), TILE)
        return remote(net2.at[core, :, at], net2.at[core, :, at], swap_s, swap_r.at[i], other)

    def second(i):
        at = pl.ds(pl.multiple_of(i * TILE, TILE), TILE)
        real, imag = complex_product(
            jnp.concatenate([net1[0, 0, at], net1[1, 0, at]], axis=1),
            jnp.concatenate([net1[0, 1, at], net1[1, 1, at]], axis=1),
            branches[source[1], 0], branches[source[1], 1],
        )
        net2[core, 0, at] = real.astype(BF16)
        net2[core, 1, at] = imag.astype(BF16)
        exchange_copy(i).start()

    tiles = net2.shape[2] // TILE
    each(tiles, second)

    def net_copy(i):
        return pltpu.make_async_copy(net3.at[i], net_out.at[i], local_sem.at[3 * i])

    def third_step(i):
        whose = core + i * (1 - 2 * core)

        @pl.when(i == 1)
        def _():
            each(tiles, lambda j: exchange_copy(j).wait_recv())

        real, imag = complex_product(
            net2[whose, 0], net2[whose, 1],
            branches[source[2], 0, :, columns(core)], branches[source[2], 1, :, columns(core)],
        )
        net3[whose, 0] = real.astype(BF16)
        net3[whose, 1] = imag.astype(BF16)

        @pl.when(i == 0)
        def _():
            net_copy(core).start()

    each(2, third_step)
    net_copy(1 - core).start()
    net_copy(core).wait()
    net_copy(1 - core).wait()
    remote(net2.at[core], net2.at[core], swap_s, swap_r.at[0], other).wait_send()
    last_copy.wait()

    def drain(e):
        place = half_pair(e)
        remote(place, place, pair_s.at[e], pair_r.at[e, 0], over_z).wait_send()
        remote(place, place, whole_s.at[e], whole_r.at[e], other).wait_send()

    def drain_leaf(e):
        place = arrived.at[e, :, own_rows()]
        remote(outgoing.at[e], place, leaf_s.at[e], leaf_r.at[e, 0], over_y).wait_send()

    @pl.when(y == 0)
    def _():
        drain_leaf(0)

        @pl.when(left)
        def _():
            for e in range(sets):
                drain(e)

    @pl.when(y == 1)
    def _():
        drain(0)

        @pl.when(left)
        def _():
            for e in range(sets):
                drain_leaf(e)

    for here, copies in drains:
        totals = {}
        for copy, t, (low, high) in copies:
            totals[copy, t] = totals.get((copy, t), 0) + high - low

        @pl.when(here)
        def _(totals=totals):
            for (copy, t), n in totals.items():
                if copy not in (mid_copy, end_copy):
                    copy(t, 0, n).wait_send()

            @pl.when(inner)
            def _():
                for (copy, t), n in totals.items():
                    if copy in (mid_copy, end_copy):
                        copy(t, 0, n).wait_send()


def general(stem_tensor, leaves, root_devices, mode_orders):
    _, rows, width = stem_tensor.shape
    half = width // 2
    part = half // CHUNKS
    groups = lax.axis_size("wide") // GROUP
    rounds = groups.bit_length() - 1
    vmem = pltpu.VMEM
    dma = pltpu.SemaphoreType.DMA
    network, last = pl.pallas_call(
        functools.partial(kernel, rounds),
        out_shape=(
            jax.ShapeDtypeStruct((2, 2, rows, half), BF16),
            jax.ShapeDtypeStruct((2, width, width), BF16),
        ),
        in_specs=[pl.BlockSpec(memory_space=pltpu.SMEM)] * 2
        + [pl.BlockSpec(memory_space=pl.ANY)] * 2,
        out_specs=[pl.BlockSpec(memory_space=pl.ANY)] * 2,
        scratch_shapes=[
            vmem((2, 2, 2, width, width), BF16),
            vmem((2, 2, half, width), BF16),
            vmem((2, half, width), BF16),
            vmem((2, width, width), BF16),
            vmem((width, width), BF16),
            vmem((max(rounds, 1), CHUNKS, 2, part, width), BF16),
            vmem((max(rounds, 1), CHUNKS, 2, part, width), BF16),
            vmem((GROUP, 2, width, width), BF16),
            vmem((2, rows, width), F32),
            vmem((2, 2, rows, half), BF16),
            vmem((2, rows, width), BF16),
            vmem((2, 2, rows, half), BF16),
            vmem((2, 2, rows, half), BF16),
            dma((5,)),
            dma((2,)), dma((2,)), dma((2,)), dma((2,)),
            dma, dma, dma, dma,
            dma((max(rounds, 1), CHUNKS)), dma((max(rounds, 1), CHUNKS)),
            dma((CHUNKS,)), dma((CHUNKS,)),
            dma((2, CHUNKS)), dma((2, CHUNKS)),
            dma((4, CHUNKS)), dma((4, CHUNKS)),
            dma((2,)), dma((2,)),
        ],
        compiler_params=pltpu.CompilerParams(collective_id=0, has_side_effects=True),
    )(root_devices, mode_orders, stem_tensor, leaves)
    return network, last


def closing(network, last, stem_tensor):
    _, rows, width = stem_tensor.shape
    half = width // 2
    return pl.pallas_call(
        finish,
        grid=(rows // half,),
        out_shape=jax.ShapeDtypeStruct(stem_tensor.shape, F32),
        in_specs=[
            pl.BlockSpec((2, 2, half, half), lambda i: (0, 0, i, 0)),
            pl.BlockSpec((2, width, width), lambda i: (0, 0, 0)),
        ],
        out_specs=pl.BlockSpec((2, half, width), lambda i: (0, i, 0)),
    )(network, last)


def split(third, stem_tensor, leaves, root_devices, mode_orders):
    _, rows, width = stem_tensor.shape
    half = width // 2
    sets = 2 if third else 1
    vmem = pltpu.VMEM
    dma = pltpu.SemaphoreType.DMA
    return pl.pallas_call(
        functools.partial(two_groups, third),
        out_shape=(
            jax.ShapeDtypeStruct((2, 2, rows, half), BF16),
            jax.ShapeDtypeStruct((2, width, width), BF16),
        ),
        in_specs=[pl.BlockSpec(memory_space=pl.ANY)] * 4,
        out_specs=[pl.BlockSpec(memory_space=pl.ANY)] * 2,
        scratch_shapes=[
            pltpu.SMEM(root_devices.shape, jnp.int32),
            pltpu.SMEM(mode_orders.shape, jnp.int32),
            vmem((leaves.shape[1], 2, width, width), BF16),
            vmem((sets, 2, half, width), BF16),
            vmem((sets, 2, width, width), BF16),
            vmem((sets, 2, width, width), BF16),
            vmem((width, width), BF16),
            vmem((sets, 2, 2, width, width), BF16),
            vmem((4, 2, width, width), BF16),
            vmem((2, rows, width), F32),
            vmem((2, 2, rows, width), BF16),
            vmem((2, 2, rows, half), BF16),
            vmem((2, 2, rows, width), BF16),
            vmem((2, 2, rows, half), BF16),
            vmem((2, width, width), BF16),
            dma((4,)),
        ]
        + [dma((sets,)), dma((sets, PARTS)), dma((sets,)), dma((sets, PARTS)), dma((sets,)), dma((sets,))]
        + [dma((4,)), dma((4, SPREAD)), dma((4,)), dma((4,)), dma((4,)), dma((4,)), dma((4, SPREAD))]
        + [dma, dma, dma, dma((rows // TILE,))],
        compiler_params=pltpu.CompilerParams(collective_id=2 if third else 1, has_side_effects=True),
    )(root_devices, mode_orders, stem_tensor, leaves)


def local(stem_tensor, leaves, root_devices, mode_orders):
    arrays = (stem_tensor, leaves, root_devices, mode_orders)
    if lax.axis_size("wide") // GROUP == 2:
        even = jnp.sum((root_devices // GROUP).astype(jnp.int32)) == 2
        network, last = lax.cond(
            even, functools.partial(split, False), functools.partial(split, True), *arrays
        )
    else:
        network, last = general(*arrays)
    return closing(network, last, stem_tensor)


def solution(mesh):
    stem_spec = P(None, ("cuts", "wide", "narrow"), None)
    return jax.shard_map(
        local,
        mesh=mesh,
        in_specs=(stem_spec, P(("cuts", "wide"), None, None, None, None), P(), P()),
        out_specs=stem_spec,
        check_vma=False,
    )
```

```python
import functools

import jax
import jax.numpy as jnp
from jax import lax
from jax.experimental import pallas as pl
from jax.experimental.pallas import tpu as pltpu
from jax.sharding import PartitionSpec as P

GROUP = 4
CHUNKS = 8
FLIGHT = 2
TILE = 128
BF16 = jnp.bfloat16
F32 = jnp.float32


def dot(x, y):
    return jnp.dot(x, y, preferred_element_type=F32)


def complex_product(ar, ai, br, bi):
    left = jnp.concatenate([ar, ai], axis=1)
    return (
        dot(left, jnp.concatenate([br, -bi], axis=0)),
        dot(left, jnp.concatenate([bi, br], axis=0)),
    )


def remote(src, dst, send_sem, recv_sem, device):
    return pltpu.make_async_remote_copy(
        src_ref=src,
        dst_ref=dst,
        send_sem=send_sem,
        recv_sem=recv_sem,
        device_id=device,
        device_id_type=pl.DeviceIdType.MESH,
    )


def kernel(
    rounds, roots, orders, stem_in, leaves_in, net_out, last_out,
    leaf, pair, away, high, chosen, held, crossed, branches, stem, net1, net2, net3, swap,
    local_sem, leaf_s, leaf_r, fwd_s, fwd_r, pair_s, pair_r, high_s, high_r,
    cross_s, cross_r, z_s, z_r, y_s, y_r, core_s, core_r, swap_s, swap_r,
):
    width = stem.shape[2]
    rows = stem.shape[1]
    half = width // 2
    part = half // CHUNKS
    core = lax.axis_index("narrow")
    wide = lax.axis_index("wide")
    member = wide % GROUP
    y = member % 2
    z = member // 2
    other = {"narrow": 1 - core}
    over_y = {"wide": wide + 1 - 2 * y}
    over_z = {"wide": wide + 2 - 4 * z}
    bits = [(wide // (GROUP << r)) % 2 for r in range(rounds)]
    over_group = [{"wide": wide + (GROUP << r) * (1 - 2 * bits[r])} for r in range(rounds)]

    barrier = pltpu.get_barrier_semaphore()
    for peer in [other, over_y, over_z] + over_group:
        pl.semaphore_signal(barrier, inc=1, device_id=peer, device_id_type=pl.DeviceIdType.MESH)
    own_rows = pl.ds(pl.multiple_of(core * half, half), half)
    own_copies = [
        pltpu.make_async_copy(leaves_in.at[0, 2 * s + y], leaf.at[s, y], local_sem.at[s])
        for s in range(2)
    ]
    stem_copy = pltpu.make_async_copy(stem_in, stem, local_sem.at[2])
    pl.semaphore_wait(barrier, 3 + rounds)

    phases = [1 - z, z]
    leaf_copies = []
    for i, s in enumerate(phases):
        copy = remote(
            leaves_in.at[0, 2 * s + 1 - y, :, own_rows],
            leaf.at[s, y, :, own_rows],
            leaf_s.at[i], leaf_r.at[i], over_y,
        )
        leaf_copies.append(copy)
    leaf_copies[0].start()
    for copy in own_copies:
        copy.start()
    stem_copy.start()

    def choose(i, carry):
        column = lax.broadcasted_iota(jnp.int32, (TILE, width), 1)
        source = jnp.zeros((TILE, width), jnp.int32)
        for b in range(orders.shape[1]):
            weight = jnp.left_shift(jnp.int32(1), orders[member, b])
            source = source + (jnp.right_shift(column, b) & 1) * weight
        row = lax.broadcasted_iota(jnp.int32, (TILE, width), 0) + i * TILE
        at = pl.ds(pl.multiple_of(i * TILE, TILE), TILE)
        chosen[at] = jnp.where(row == source, 1.0, 0.0).astype(F32).astype(BF16)
        return carry

    lax.fori_loop(0, width // TILE, choose, 0)
    for copy in own_copies:
        copy.wait()

    pair_copy = remote(away, pair.at[z], pair_s, pair_r, over_z)
    leaf_copies[0].wait_send()
    leaf_copies[1].start()
    for i, s in enumerate(phases):
        leaf_copies[i].wait_recv()
        forward = remote(
            leaf.at[s, 1 - y, :, own_rows], leaf.at[s, 1 - y, :, own_rows],
            fwd_s.at[i], fwd_r.at[i], other,
        )
        forward.start()
        forward.wait()

        def pair_tile(t, carry, s=s, i=i):
            at = pl.ds(pl.multiple_of(t * half, half), half)
            real, imag = complex_product(
                leaf[s, 0, 0, own_rows], leaf[s, 0, 1, own_rows],
                leaf[s, 1, 0, :, at], leaf[s, 1, 1, :, at],
            )
            target = away if i == 0 else pair.at[z]
            target[0, :, at] = real.astype(BF16)
            target[1, :, at] = imag.astype(BF16)
            return carry

        lax.fori_loop(0, width // half, pair_tile, 0)
        if i == 0:
            pair_copy.start()
    pair_copy.wait_recv()

    def high_tile(t, carry):
        at = pl.ds(pl.multiple_of(t * half, half), half)
        for c in range(2):
            high[c, own_rows, at] = dot(pair[1, c], chosen[:, at]).astype(BF16)
        return carry

    lax.fori_loop(0, width // half, high_tile, 0)
    high_copy = remote(high.at[:, own_rows], high.at[:, own_rows], high_s, high_r, other)
    high_copy.start()
    high_copy.wait()

    def rows_of(c):
        return pl.ds(pl.multiple_of(core * half + c * part, part), part)

    def cross_copy(r, c):
        return remote(held.at[r, c], crossed.at[r, c], cross_s.at[r, c], cross_r.at[r, c], over_group[r])

    def place(origin, c):
        return branches.at[origin, :, rows_of(c)]

    origins = [member, member + 2 - 4 * z, member + 1 - 2 * y, GROUP - 1 - member]

    def z_copy(c):
        return remote(place(origins[0], c), place(origins[0], c), z_s.at[c], z_r.at[c], over_z)

    def y_copy(i, c):
        return remote(place(origins[i], c), place(origins[i], c), y_s.at[i, c], y_r.at[i, c], over_y)

    def core_copy(i, c):
        return remote(place(origins[i], c), place(origins[i], c), core_s.at[i, c], core_r.at[i, c], other)

    def spread(c):
        z_copy(c).start()
        y_copy(0, c).start()
        core_copy(0, c).start()

    def select(r, c):
        cross_copy(r, c).wait_recv()
        cross_copy(r, c).wait_send()
        if c + FLIGHT < CHUNKS:
            cross_copy(r, c + FLIGHT).start()
        root_bit = (roots[member] // (GROUP << r)) % 2
        for p in range(2):
            here = held[r, c, p].astype(F32)
            there = crossed[r, c, p].astype(F32)
            same = jnp.full(here.shape, root_bit, jnp.int32) == bits[r]
            picked = jnp.where(same, here, there).astype(BF16)
            if r + 1 < rounds:
                held[r + 1, c, p] = picked
            else:
                branches[member, p, rows_of(c)] = picked
        if r + 1 < rounds:
            if c < FLIGHT:
                cross_copy(r + 1, c).start()
        else:
            spread(c)

    def on_z(c):
        z_copy(c).wait_recv()
        y_copy(1, c).start()
        core_copy(1, c).start()

    def on_y(i, c):
        y_copy(i, c).wait_recv()
        core_copy(2 + i, c).start()

    for c in range(CHUNKS):
        at = pl.ds(c * part, part)
        real, imag = complex_product(pair[0, 0, at], pair[0, 1, at], high[0], high[1])
        if rounds:
            held[0, c, 0] = real.astype(BF16)
            held[0, c, 1] = imag.astype(BF16)
            if c < FLIGHT:
                cross_copy(0, c).start()
        else:
            branches[member, 0, rows_of(c)] = real.astype(BF16)
            branches[member, 1, rows_of(c)] = imag.astype(BF16)
            spread(c)

    for r in range(rounds - 1):
        for c in range(CHUNKS):
            select(r, c)
    for c in range(CHUNKS + 2):
        if rounds and c < CHUNKS:
            select(rounds - 1, c)
        if 1 <= c <= CHUNKS:
            on_z(c - 1)
            on_y(0, c - 1)
        if c >= 2:
            on_y(1, c - 2)
    stem_copy.wait()
    for c in range(CHUNKS):
        for i in range(4):
            core_copy(i, c).wait_recv()
    last_copy = pltpu.make_async_copy(branches.at[GROUP - 1], last_out, local_sem.at[3])
    last_copy.start()

    def columns(block):
        return pl.ds(pl.multiple_of(block * half, half), half)

    def swapped(step, index, read, target):
        copy = remote(swap.at[index], target.at[core], swap_s.at[index], swap_r.at[index], other)
        for keep in range(2):
            block = core if keep else 1 - core

            def tile(t, carry, keep=keep, block=block):
                at = pl.ds(pl.multiple_of(t * half, half), half)
                nr, ni = read(at)
                real, imag = complex_product(
                    nr, ni, branches[step, 0, :, columns(block)], branches[step, 1, :, columns(block)]
                )
                place = target.at[core] if keep else swap.at[index]
                place[0, at] = real.astype(BF16)
                place[1, at] = imag.astype(BF16)
                return carry

            lax.fori_loop(0, rows // half, tile, 0)
            if not keep:
                copy.start()
        copy.wait()

    def plain(step, source, target):
        for block in range(width // half):
            across = pl.ds(block * half, half)

            def tile(t, carry, across=across):
                at = pl.ds(pl.multiple_of(t * half, half), half)
                real, imag = complex_product(
                    jnp.concatenate([source[0, 0, at], source[1, 0, at]], axis=1),
                    jnp.concatenate([source[0, 1, at], source[1, 1, at]], axis=1),
                    branches[step, 0, :, across], branches[step, 1, :, across],
                )
                target[0, at, across] = real.astype(target.dtype)
                target[1, at, across] = imag.astype(target.dtype)
                return carry

            lax.fori_loop(0, rows // half, tile, 0)

    swapped(0, 0, lambda at: (stem[0, at].astype(BF16), stem[1, at].astype(BF16)), net1)
    plain(1, net1, net2)
    swapped(2, 1, lambda at: (net2[0, at], net2[1, at]), net3)
    net_copy = pltpu.make_async_copy(net3, net_out, local_sem.at[4])
    net_copy.start()
    net_copy.wait()
    last_copy.wait()

    leaf_copies[1].wait_send()
    pair_copy.wait_send()
    for c in range(CHUNKS):
        z_copy(c).wait_send()
        for i in range(2):
            y_copy(i, c).wait_send()
        for i in range(4):
            core_copy(i, c).wait_send()


def finish(net, branch, out):
    half = net.shape[3]
    for block in range(branch.shape[2] // half):
        across = pl.ds(block * half, half)
        real, imag = complex_product(
            jnp.concatenate([net[0, 0], net[1, 0]], axis=1),
            jnp.concatenate([net[0, 1], net[1, 1]], axis=1),
            branch[0, :, across], branch[1, :, across],
        )
        out[0, :, across] = real
        out[1, :, across] = imag


PARTS = 16
SPREAD = 16
ACROSS = 11
HALVE = 8


def each(n, body):
    def step(i, carry):
        body(i)
        return carry

    lax.fori_loop(0, n, step, 0)


def matching(roots, group):
    seen = jnp.int32(0)
    found = []
    for k in range(roots.shape[0]):
        holds = jnp.where(roots[k] // GROUP == group, 1, 0)
        found.append((holds, seen))
        seen = seen + holds
    return found


def step_of(roots, group, rank):
    total = jnp.int32(0)
    for k, (holds, seen) in enumerate(matching(roots, group)):
        total = total + jnp.where(seen == rank, holds * k, 0)
    return total


def two_groups(
    third, roots_in, orders_in, stem_in, leaves_in, net_out, last_out, roots, orders,
    leaf, outgoing, arrived, mine, chosen, pair, branches, stem, stems, net1, net2, net3, final,
    local_sem, leaf_s, leaf_r, pair_s, pair_r, whole_s, whole_r,
    y_s, y_r, core_s, core_r, mid_s, end_s, far_r, stem_s, stem_r, swap_s, swap_r,
):
    width = stem.shape[2]
    half = width // 2
    core = lax.axis_index("narrow")
    wide = lax.axis_index("wide")
    group = wide // GROUP
    member = wide % GROUP
    y = member % 2
    z = member // 2
    inner = group + z == 1
    other = {"narrow": 1 - core}
    over_y = {"wide": wide + 1 - 2 * y}
    over_z = {"wide": wide + 2 - 4 * z}
    over_mid = {"wide": wide + 2 - 4 * group}
    MESH = pl.DeviceIdType.MESH
    sets = 2 if third else 1
    left = group == 1 if third else group >= 0

    fetch = pltpu.make_async_copy(leaves_in.at[0], leaf, local_sem.at[0])
    stem_copy = pltpu.make_async_copy(stem_in, stem, local_sem.at[1])
    fetch.start()
    barrier = pltpu.get_barrier_semaphore()
    for peer in [other, over_y, over_z]:
        pl.semaphore_signal(barrier, inc=1, device_id=peer, device_id_type=MESH)

    @pl.when(inner)
    def _():
        pl.semaphore_signal(barrier, inc=1, device_id=over_mid, device_id_type=MESH)

    scalars = [
        pltpu.make_async_copy(roots_in, roots, local_sem.at[2]),
        pltpu.make_async_copy(orders_in, orders, local_sem.at[3]),
    ]
    for copy in scalars:
        copy.start()
    for copy in scalars:
        copy.wait()
    k_right = step_of(roots, group, 0)
    k_left = [step_of(roots, group, 1 + e) for e in range(sets)]

    def own_rows(j=0, n=1):
        size = half // n
        return pl.ds(pl.multiple_of(core * half + j * size, size), size)

    def one_hot(k, low, n):
        column = lax.broadcasted_iota(jnp.int32, (8, n), 1) + low
        source = jnp.zeros((8, n), jnp.int32)
        for b in range(orders.shape[1]):
            weight = jnp.left_shift(jnp.int32(1), orders[k, b])
            source = source + (jnp.right_shift(column, b) & 1) * weight

        def tile(i):
            row = lax.broadcasted_iota(jnp.int32, (TILE, n), 0) + i * TILE
            at = pl.ds(pl.multiple_of(i * TILE, TILE), TILE)
            same = row == jnp.broadcast_to(source[0:1], (TILE, n))
            chosen[at, :n] = jnp.where(same, 1.0, 0.0).astype(F32).astype(BF16)

        each(width // TILE, tile)

    def leaf_copy(e, j):
        size = half // PARTS
        at = pl.ds(pl.multiple_of(j * size, size), size)
        return remote(
            outgoing.at[e, :, at], arrived.at[e, :, own_rows(j, PARTS)], leaf_s.at[e], leaf_r.at[e, j], over_y
        )

    @pl.when(jnp.logical_and(y * z == 1, left))
    def _():
        one_hot(k_left[0], core * half, half)

    @pl.when(inner)
    def _():
        pl.semaphore_wait(barrier, 4)

    @pl.when(jnp.logical_not(inner))
    def _():
        pl.semaphore_wait(barrier, 3)

    @pl.when(y == 0)
    def _():
        fetch.wait()
        for c in range(2):
            outgoing[0, c] = leaf[k_right, c, own_rows()]
        each(PARTS, lambda j: leaf_copy(0, j).start())
        for e in range(sets):
            for c in range(2):
                mine[e, c] = leaf[k_left[e], c].T

    @pl.when(y == 1)
    def _():
        fetch.wait()

        @pl.when(left)
        def _():
            for e in range(sets):

                @pl.when(z == 0)
                def _():
                    for c in range(2):
                        outgoing[e, c] = leaf[k_left[e], c, :, own_rows()].T

                @pl.when(z == 1)
                def _():
                    if e:
                        one_hot(k_left[e], core * half, half)
                    for c in range(2):
                        outgoing[e, c] = dot(leaf[k_left[e], c], chosen[:, :half]).astype(BF16).T

                each(PARTS, lambda j, e=e: leaf_copy(e, j).start())

        @pl.when(z == 0)
        def _():
            for c in range(2):
                mine[0, c] = leaf[k_right, c]

        @pl.when(z == 1)
        def _():
            one_hot(k_right, 0, width)
            for c in range(2):
                mine[0, c] = dot(leaf[k_right, c], chosen[...]).astype(BF16)

    stem_copy.start()
    stem_copy.wait()
    for c in range(2):
        stems[core, c] = stem[c].astype(BF16)
    stem_share = remote(stems.at[core], stems.at[core], stem_s, stem_r, other)
    stem_share.start()

    def pair_copy(e, j):
        place = pair.at[e, z, :, own_rows(j, PARTS)]
        return remote(place, place, pair_s.at[e], pair_r.at[e, j], over_z)

    def whole_copy(e, j):
        place = pair.at[e, y, :, own_rows(j, PARTS)]
        return remote(place, place, whole_s.at[e], whole_r.at[e], other)

    def pairs(e, first, last):
        def turn(j):
            leaf_copy(e, j).wait_recv()
            at = own_rows(j, PARTS)

            real, imag = complex_product(arrived[e, 0, at], arrived[e, 1, at], mine[e, 0], mine[e, 1])
            pair[e, z, 0, at] = real.astype(BF16)
            pair[e, z, 1, at] = imag.astype(BF16)
            pair_copy(e, j).start()

            @pl.when(z == y)
            def _():
                whole_copy(e, j).start()

        each(last - first, lambda j: turn(j + first))

    def half_pair(e):
        return pair.at[e, 0, :, own_rows()]

    def join(e):
        def arrive(j):
            pair_copy(e, j).wait_recv()

            @pl.when(z != y)
            def _():
                whole_copy(e, j).start()

        each(PARTS, arrive)
        remote(half_pair(e), half_pair(e), whole_s.at[e], whole_r.at[e], other).wait_recv()

    A, C, D, E = range(4)

    def rows_first(t):
        return t in (A, C)

    def place(t, r, n=1):
        if rows_first(t):
            size = half // SPREAD
            return branches.at[t, :, pl.ds(pl.multiple_of(core * half + r * size, size), n * size)]
        size = width // SPREAD
        if n > 1:
            return branches.at[t, :, : n * size, own_rows()]
        row = (r % (SPREAD // 2)) * (2 * size)
        return branches.at[t, :, pl.ds(pl.multiple_of(row, size), 2 * size), own_rows(r // (SPREAD // 2), 2)]

    def y_copy(t, r, n=1):
        return remote(place(t, r, n), place(t, r, n), y_s.at[t], y_r.at[t, r], over_y)

    def core_copy(t, r, n=1):
        return remote(place(t, r, n), place(t, r, n), core_s.at[t], core_r.at[t], other)

    def mid_copy(t, r, n=1):
        return remote(place(t, r, n), place(t, r, n), mid_s.at[t], far_r.at[t, r], over_mid)

    def end_copy(t, r, n=1):
        return remote(place(t, r, n), place(t, r, n), end_s.at[t], far_r.at[t, r], over_z)

    sent = {}

    def send(copy, t, r, n):
        if copy in (mid_copy, end_copy):

            @pl.when(inner)
            def _():
                copy(t, r).start()

        else:
            copy(t, r).start()
        sent[copy, t, n] = True

    def ship(t, r):
        send(mid_copy, t, r, (0, SPREAD))
        send(y_copy, t, r, (0, SPREAD))
        send(core_copy, t, r, (0, SPREAD))

    def own(e, t):
        def turn(b):
            at = own_rows(b, 2)
            real, imag = complex_product(
                pair[e, 1 - y, 0, at], pair[e, 1 - y, 1, at], pair[e, y, 0], pair[e, y, 1]
            )
            if rows_first(t):
                branches[t, 0, at] = real.astype(BF16)
                branches[t, 1, at] = imag.astype(BF16)
                each(SPREAD // 2, lambda i: ship(t, b * (SPREAD // 2) + i))
            else:
                branches[t, 0, :, at] = real.T.astype(BF16)
                branches[t, 1, :, at] = imag.T.astype(BF16)
                if not e:
                    each(SPREAD // 2, lambda i: ship(t, b * (SPREAD // 2) + i))

        each(2, turn)
        if e:
            each(HALVE, lambda r: send(mid_copy, t, r, (0, HALVE)))

            def turn_sent(i):
                r = (i + HALVE) % SPREAD
                send(y_copy, t, r, (0, SPREAD))
                send(core_copy, t, r, (0, SPREAD))

            each(SPREAD, turn_sent)

    def receive(first, last, *turns):
        def turn(i):
            for t, origin, onward, shift in turns:
                r = i + first + shift
                span = (first + shift, last + shift)
                if origin == "z":
                    mid_copy(t, r).wait_recv()
                else:
                    y_copy(t, r).wait_recv()
                for letter, copy in (("e", end_copy), ("m", mid_copy), ("y", y_copy)):
                    if letter in onward:
                        send(copy, t, r, span)
                send(core_copy, t, r, span)

        each(last - first, turn)

    def exchange(far, beside, beyond):
        receive(0, ACROSS, (far, "z", "ey", 0), (beside, "y", "", 0))
        receive(ACROSS, SPREAD, (far, "z", "e", 0), (beside, "y", "m", 0))
        if 2 * ACROSS == SPREAD:
            receive(0, ACROSS, (beyond, "y", "", 0), (beyond, "z", "e", ACROSS))
        else:
            receive(ACROSS, SPREAD, (beyond, "z", "e", 0))
            receive(0, ACROSS, (beyond, "y", "", 0))

    def build(t):
        pairs(0, 0, PARTS)
        join(0)
        own(0, t)

    def role_right_low():
        build(A)
        if third:
            receive(0, SPREAD, (C, "z", "ey", 0))
            receive(0, SPREAD, (E, "y", "", 0))
        else:
            exchange(C, D, E)

    def role_right_high():
        build(C)
        if third:
            receive(0, SPREAD, (A, "z", "e", 0), (E, "y", "", 0))
        else:
            exchange(A, E, D)

    def role_left_low():
        if third:
            receive(0, SPREAD, (A, "y", "m", 0), (E, "z", "ey", 0))
            receive(0, SPREAD - HALVE, (C, "y", "", 0))
            receive(0, HALVE, (C, "y", "", SPREAD - HALVE), (D, "z", "ey", 0))
        else:
            build(D)
            exchange(E, A, C)

    def role_left_high():
        if third:
            pairs(0, 0, PARTS)
            pairs(1, 0, PARTS // 4)
            join(0)
            own(0, E)
            pairs(1, PARTS // 4, PARTS)
            join(1)
            own(1, D)
            receive(0, SPREAD, (A, "z", "e", 0))
            receive(0, SPREAD, (C, "y", "", 0))
        else:
            build(E)
            exchange(D, C, A)

    def last_right_low():
        receive(HALVE, SPREAD, (D, "z", "ey", 0))
        receive(0, HALVE, (D, "y", "", 0))

    def last_right_high():
        receive(HALVE, SPREAD, (D, "y", "m", 0))
        receive(0, HALVE, (D, "y", "", 0))

    def last_left_low():
        receive(HALVE, SPREAD, (D, "y", "", 0))

    drains = []

    def play(roles):
        for at_y, at_group, role in roles:
            sent.clear()
            here = jnp.logical_and(y == at_y, group == at_group)
            pl.when(here)(role)
            drains.append((here, list(sent)))

    def columns(block):
        return pl.ds(pl.multiple_of(block * half, half), half)

    zeros = matching(roots, 0)
    ones = matching(roots, 1)
    source = []
    for k in range(roots.shape[0]):
        high = jnp.where(ones[k][1] == 2, D, C + 2 * ones[k][1])
        at = jnp.where(zeros[k][0] == 1, A + 2 * zeros[k][1], high)
        source.append(jnp.minimum(at, 3))

    def first():
        def turn(i):
            picked = []
            for c in range(2):
                one = branches[A, c, :, columns(core)]
                two = branches[C, c, :, columns(core)]
                if third:
                    picked.append(jnp.where(jnp.full(one.shape, source[0], jnp.int32) == A, one, two))
                else:
                    picked.append(branches[source[0], c, :, columns(core)])
            real, imag = complex_product(stems[i, 0], stems[i, 1], *picked)
            net1[i, 0] = real.astype(BF16)
            net1[i, 1] = imag.astype(BF16)

        each(2, turn)

    play([(1, 0, role_right_low), (1, 1, role_right_high), (0, 0, role_left_low), (0, 1, role_left_high)])
    stem_share.wait()
    for t in (A, C):
        core_copy(t, 0, SPREAD).wait_recv()
    if third:
        first()
        play([(1, 0, last_right_low), (1, 1, last_right_high), (0, 0, last_left_low)])
    for t in (D, E):
        core_copy(t, 0, SPREAD).wait_recv()
    for c in range(2):
        final[c] = branches[source[3], c]
    last_copy = pltpu.make_async_copy(final, last_out, local_sem.at[2])
    last_copy.start()
    if not third:
        first()

    def exchange_copy(i):
        at = pl.ds(pl.multiple_of(i * TILE, TILE), TILE)
        return remote(net2.at[core, :, at], net2.at[core, :, at], swap_s, swap_r.at[i], other)

    def second(i):
        at = pl.ds(pl.multiple_of(i * TILE, TILE), TILE)
        real, imag = complex_product(
            jnp.concatenate([net1[0, 0, at], net1[1, 0, at]], axis=1),
            jnp.concatenate([net1[0, 1, at], net1[1, 1, at]], axis=1),
            branches[source[1], 0], branches[source[1], 1],
        )
        net2[core, 0, at] = real.astype(BF16)
        net2[core, 1, at] = imag.astype(BF16)
        exchange_copy(i).start()

    tiles = net2.shape[2] // TILE
    each(tiles, second)

    def net_copy(i):
        return pltpu.make_async_copy(net3.at[i], net_out.at[i], local_sem.at[3 * i])

    def third_step(i):
        whose = core + i * (1 - 2 * core)

        @pl.when(i == 1)
        def _():
            each(tiles, lambda j: exchange_copy(j).wait_recv())

        real, imag = complex_product(
            net2[whose, 0], net2[whose, 1],
            branches[source[2], 0, :, columns(core)], branches[source[2], 1, :, columns(core)],
        )
        net3[whose, 0] = real.astype(BF16)
        net3[whose, 1] = imag.astype(BF16)

        @pl.when(i == 0)
        def _():
            net_copy(core).start()

    each(2, third_step)
    net_copy(1 - core).start()
    net_copy(core).wait()
    net_copy(1 - core).wait()
    remote(net2.at[core], net2.at[core], swap_s, swap_r.at[0], other).wait_send()
    last_copy.wait()

    def drain(e):
        place = half_pair(e)
        remote(place, place, pair_s.at[e], pair_r.at[e, 0], over_z).wait_send()
        remote(place, place, whole_s.at[e], whole_r.at[e], other).wait_send()

    def drain_leaf(e):
        place = arrived.at[e, :, own_rows()]
        remote(outgoing.at[e], place, leaf_s.at[e], leaf_r.at[e, 0], over_y).wait_send()

    @pl.when(y == 0)
    def _():
        drain_leaf(0)

        @pl.when(left)
        def _():
            for e in range(sets):
                drain(e)

    @pl.when(y == 1)
    def _():
        drain(0)

        @pl.when(left)
        def _():
            for e in range(sets):
                drain_leaf(e)

    for here, copies in drains:
        totals = {}
        for copy, t, (low, high) in copies:
            totals[copy, t] = totals.get((copy, t), 0) + high - low

        @pl.when(here)
        def _(totals=totals):
            for (copy, t), n in totals.items():
                if copy not in (mid_copy, end_copy):
                    copy(t, 0, n).wait_send()

            @pl.when(inner)
            def _():
                for (copy, t), n in totals.items():
                    if copy in (mid_copy, end_copy):
                        copy(t, 0, n).wait_send()


def general(stem_tensor, leaves, root_devices, mode_orders):
    _, rows, width = stem_tensor.shape
    half = width // 2
    part = half // CHUNKS
    groups = lax.axis_size("wide") // GROUP
    rounds = groups.bit_length() - 1
    vmem = pltpu.VMEM
    dma = pltpu.SemaphoreType.DMA
    network, last = pl.pallas_call(
        functools.partial(kernel, rounds),
        out_shape=(
            jax.ShapeDtypeStruct((2, 2, rows, half), BF16),
            jax.ShapeDtypeStruct((2, width, width), BF16),
        ),
        in_specs=[pl.BlockSpec(memory_space=pltpu.SMEM)] * 2
        + [pl.BlockSpec(memory_space=pl.ANY)] * 2,
        out_specs=[pl.BlockSpec(memory_space=pl.ANY)] * 2,
        scratch_shapes=[
            vmem((2, 2, 2, width, width), BF16),
            vmem((2, 2, half, width), BF16),
            vmem((2, half, width), BF16),
            vmem((2, width, width), BF16),
            vmem((width, width), BF16),
            vmem((max(rounds, 1), CHUNKS, 2, part, width), BF16),
            vmem((max(rounds, 1), CHUNKS, 2, part, width), BF16),
            vmem((GROUP, 2, width, width), BF16),
            vmem((2, rows, width), F32),
            vmem((2, 2, rows, half), BF16),
            vmem((2, rows, width), BF16),
            vmem((2, 2, rows, half), BF16),
            vmem((2, 2, rows, half), BF16),
            dma((5,)),
            dma((2,)), dma((2,)), dma((2,)), dma((2,)),
            dma, dma, dma, dma,
            dma((max(rounds, 1), CHUNKS)), dma((max(rounds, 1), CHUNKS)),
            dma((CHUNKS,)), dma((CHUNKS,)),
            dma((2, CHUNKS)), dma((2, CHUNKS)),
            dma((4, CHUNKS)), dma((4, CHUNKS)),
            dma((2,)), dma((2,)),
        ],
        compiler_params=pltpu.CompilerParams(collective_id=0, has_side_effects=True),
    )(root_devices, mode_orders, stem_tensor, leaves)
    return network, last


def closing(network, last, stem_tensor):
    _, rows, width = stem_tensor.shape
    half = width // 2
    return pl.pallas_call(
        finish,
        grid=(rows // half,),
        out_shape=jax.ShapeDtypeStruct(stem_tensor.shape, F32),
        in_specs=[
            pl.BlockSpec((2, 2, half, half), lambda i: (0, 0, i, 0)),
            pl.BlockSpec((2, width, width), lambda i: (0, 0, 0)),
        ],
        out_specs=pl.BlockSpec((2, half, width), lambda i: (0, i, 0)),
    )(network, last)


def split(third, stem_tensor, leaves, root_devices, mode_orders):
    _, rows, width = stem_tensor.shape
    half = width // 2
    sets = 2 if third else 1
    vmem = pltpu.VMEM
    dma = pltpu.SemaphoreType.DMA
    return pl.pallas_call(
        functools.partial(two_groups, third),
        out_shape=(
            jax.ShapeDtypeStruct((2, 2, rows, half), BF16),
            jax.ShapeDtypeStruct((2, width, width), BF16),
        ),
        in_specs=[pl.BlockSpec(memory_space=pl.ANY)] * 4,
        out_specs=[pl.BlockSpec(memory_space=pl.ANY)] * 2,
        scratch_shapes=[
            pltpu.SMEM(root_devices.shape, jnp.int32),
            pltpu.SMEM(mode_orders.shape, jnp.int32),
            vmem((leaves.shape[1], 2, width, width), BF16),
            vmem((sets, 2, half, width), BF16),
            vmem((sets, 2, width, width), BF16),
            vmem((sets, 2, width, width), BF16),
            vmem((width, width), BF16),
            vmem((sets, 2, 2, width, width), BF16),
            vmem((4, 2, width, width), BF16),
            vmem((2, rows, width), F32),
            vmem((2, 2, rows, width), BF16),
            vmem((2, 2, rows, half), BF16),
            vmem((2, 2, rows, width), BF16),
            vmem((2, 2, rows, half), BF16),
            vmem((2, width, width), BF16),
            dma((4,)),
        ]
        + [dma((sets,)), dma((sets, PARTS)), dma((sets,)), dma((sets, PARTS)), dma((sets,)), dma((sets,))]
        + [dma((4,)), dma((4, SPREAD)), dma((4,)), dma((4,)), dma((4,)), dma((4,)), dma((4, SPREAD))]
        + [dma, dma, dma, dma((rows // TILE,))],
        compiler_params=pltpu.CompilerParams(collective_id=2 if third else 1, has_side_effects=True),
    )(root_devices, mode_orders, stem_tensor, leaves)


def local(stem_tensor, leaves, root_devices, mode_orders):
    arrays = (stem_tensor, leaves, root_devices, mode_orders)
    if lax.axis_size("wide") // GROUP == 2:
        even = jnp.sum((root_devices // GROUP).astype(jnp.int32)) == 2
        network, last = lax.cond(
            even, functools.partial(split, False), functools.partial(split, True), *arrays
        )
    else:
        network, last = general(*arrays)
    return closing(network, last, stem_tensor)


def solution(mesh):
    stem_spec = P(None, ("cuts", "wide", "narrow"), None)
    return jax.shard_map(
        local,
        mesh=mesh,
        in_specs=(stem_spec, P(("cuts", "wide"), None, None, None, None), P(), P()),
        out_specs=stem_spec,
        check_vma=False,
    )
```

```python
import functools

import jax
import jax.numpy as jnp
from jax import lax
from jax.experimental import pallas as pl
from jax.experimental.pallas import tpu as pltpu
from jax.sharding import PartitionSpec as P

GROUP = 4
CHUNKS = 8
FLIGHT = 2
TILE = 128
BF16 = jnp.bfloat16
F32 = jnp.float32


def dot(x, y):
    return jnp.dot(x, y, preferred_element_type=F32)


def complex_product(ar, ai, br, bi):
    left = jnp.concatenate([ar, ai], axis=1)
    return (
        dot(left, jnp.concatenate([br, -bi], axis=0)),
        dot(left, jnp.concatenate([bi, br], axis=0)),
    )


def remote(src, dst, send_sem, recv_sem, device):
    return pltpu.make_async_remote_copy(
        src_ref=src,
        dst_ref=dst,
        send_sem=send_sem,
        recv_sem=recv_sem,
        device_id=device,
        device_id_type=pl.DeviceIdType.MESH,
    )


def kernel(
    rounds, roots, orders, stem_in, leaves_in, net_out, last_out,
    leaf, pair, away, high, chosen, held, crossed, branches, stem, net1, net2, net3, swap,
    local_sem, leaf_s, leaf_r, fwd_s, fwd_r, pair_s, pair_r, high_s, high_r,
    cross_s, cross_r, z_s, z_r, y_s, y_r, core_s, core_r, swap_s, swap_r,
):
    width = stem.shape[2]
    rows = stem.shape[1]
    half = width // 2
    part = half // CHUNKS
    core = lax.axis_index("narrow")
    wide = lax.axis_index("wide")
    member = wide % GROUP
    y = member % 2
    z = member // 2
    other = {"narrow": 1 - core}
    over_y = {"wide": wide + 1 - 2 * y}
    over_z = {"wide": wide + 2 - 4 * z}
    bits = [(wide // (GROUP << r)) % 2 for r in range(rounds)]
    over_group = [{"wide": wide + (GROUP << r) * (1 - 2 * bits[r])} for r in range(rounds)]

    barrier = pltpu.get_barrier_semaphore()
    for peer in [other, over_y, over_z] + over_group:
        pl.semaphore_signal(barrier, inc=1, device_id=peer, device_id_type=pl.DeviceIdType.MESH)
    own_rows = pl.ds(pl.multiple_of(core * half, half), half)
    own_copies = [
        pltpu.make_async_copy(leaves_in.at[0, 2 * s + y], leaf.at[s, y], local_sem.at[s])
        for s in range(2)
    ]
    stem_copy = pltpu.make_async_copy(stem_in, stem, local_sem.at[2])
    pl.semaphore_wait(barrier, 3 + rounds)

    phases = [1 - z, z]
    leaf_copies = []
    for i, s in enumerate(phases):
        copy = remote(
            leaves_in.at[0, 2 * s + 1 - y, :, own_rows],
            leaf.at[s, y, :, own_rows],
            leaf_s.at[i], leaf_r.at[i], over_y,
        )
        leaf_copies.append(copy)
    leaf_copies[0].start()
    for copy in own_copies:
        copy.start()
    stem_copy.start()

    def choose(i, carry):
        column = lax.broadcasted_iota(jnp.int32, (TILE, width), 1)
        source = jnp.zeros((TILE, width), jnp.int32)
        for b in range(orders.shape[1]):
            weight = jnp.left_shift(jnp.int32(1), orders[member, b])
            source = source + (jnp.right_shift(column, b) & 1) * weight
        row = lax.broadcasted_iota(jnp.int32, (TILE, width), 0) + i * TILE
        at = pl.ds(pl.multiple_of(i * TILE, TILE), TILE)
        chosen[at] = jnp.where(row == source, 1.0, 0.0).astype(F32).astype(BF16)
        return carry

    lax.fori_loop(0, width // TILE, choose, 0)
    for copy in own_copies:
        copy.wait()

    pair_copy = remote(away, pair.at[z], pair_s, pair_r, over_z)
    leaf_copies[0].wait_send()
    leaf_copies[1].start()
    for i, s in enumerate(phases):
        leaf_copies[i].wait_recv()
        forward = remote(
            leaf.at[s, 1 - y, :, own_rows], leaf.at[s, 1 - y, :, own_rows],
            fwd_s.at[i], fwd_r.at[i], other,
        )
        forward.start()
        forward.wait()

        def pair_tile(t, carry, s=s, i=i):
            at = pl.ds(pl.multiple_of(t * half, half), half)
            real, imag = complex_product(
                leaf[s, 0, 0, own_rows], leaf[s, 0, 1, own_rows],
                leaf[s, 1, 0, :, at], leaf[s, 1, 1, :, at],
            )
            target = away if i == 0 else pair.at[z]
            target[0, :, at] = real.astype(BF16)
            target[1, :, at] = imag.astype(BF16)
            return carry

        lax.fori_loop(0, width // half, pair_tile, 0)
        if i == 0:
            pair_copy.start()
    pair_copy.wait_recv()

    def high_tile(t, carry):
        at = pl.ds(pl.multiple_of(t * half, half), half)
        for c in range(2):
            high[c, own_rows, at] = dot(pair[1, c], chosen[:, at]).astype(BF16)
        return carry

    lax.fori_loop(0, width // half, high_tile, 0)
    high_copy = remote(high.at[:, own_rows], high.at[:, own_rows], high_s, high_r, other)
    high_copy.start()
    high_copy.wait()

    def rows_of(c):
        return pl.ds(pl.multiple_of(core * half + c * part, part), part)

    def cross_copy(r, c):
        return remote(held.at[r, c], crossed.at[r, c], cross_s.at[r, c], cross_r.at[r, c], over_group[r])

    def place(origin, c):
        return branches.at[origin, :, rows_of(c)]

    origins = [member, member + 2 - 4 * z, member + 1 - 2 * y, GROUP - 1 - member]

    def z_copy(c):
        return remote(place(origins[0], c), place(origins[0], c), z_s.at[c], z_r.at[c], over_z)

    def y_copy(i, c):
        return remote(place(origins[i], c), place(origins[i], c), y_s.at[i, c], y_r.at[i, c], over_y)

    def core_copy(i, c):
        return remote(place(origins[i], c), place(origins[i], c), core_s.at[i, c], core_r.at[i, c], other)

    def spread(c):
        z_copy(c).start()
        y_copy(0, c).start()
        core_copy(0, c).start()

    def select(r, c):
        cross_copy(r, c).wait_recv()
        cross_copy(r, c).wait_send()
        if c + FLIGHT < CHUNKS:
            cross_copy(r, c + FLIGHT).start()
        root_bit = (roots[member] // (GROUP << r)) % 2
        for p in range(2):
            here = held[r, c, p].astype(F32)
            there = crossed[r, c, p].astype(F32)
            same = jnp.full(here.shape, root_bit, jnp.int32) == bits[r]
            picked = jnp.where(same, here, there).astype(BF16)
            if r + 1 < rounds:
                held[r + 1, c, p] = picked
            else:
                branches[member, p, rows_of(c)] = picked
        if r + 1 < rounds:
            if c < FLIGHT:
                cross_copy(r + 1, c).start()
        else:
            spread(c)

    def on_z(c):
        z_copy(c).wait_recv()
        y_copy(1, c).start()
        core_copy(1, c).start()

    def on_y(i, c):
        y_copy(i, c).wait_recv()
        core_copy(2 + i, c).start()

    for c in range(CHUNKS):
        at = pl.ds(c * part, part)
        real, imag = complex_product(pair[0, 0, at], pair[0, 1, at], high[0], high[1])
        if rounds:
            held[0, c, 0] = real.astype(BF16)
            held[0, c, 1] = imag.astype(BF16)
            if c < FLIGHT:
                cross_copy(0, c).start()
        else:
            branches[member, 0, rows_of(c)] = real.astype(BF16)
            branches[member, 1, rows_of(c)] = imag.astype(BF16)
            spread(c)

    for r in range(rounds - 1):
        for c in range(CHUNKS):
            select(r, c)
    for c in range(CHUNKS + 2):
        if rounds and c < CHUNKS:
            select(rounds - 1, c)
        if 1 <= c <= CHUNKS:
            on_z(c - 1)
            on_y(0, c - 1)
        if c >= 2:
            on_y(1, c - 2)
    stem_copy.wait()
    for c in range(CHUNKS):
        for i in range(4):
            core_copy(i, c).wait_recv()
    last_copy = pltpu.make_async_copy(branches.at[GROUP - 1], last_out, local_sem.at[3])
    last_copy.start()

    def columns(block):
        return pl.ds(pl.multiple_of(block * half, half), half)

    def swapped(step, index, read, target):
        copy = remote(swap.at[index], target.at[core], swap_s.at[index], swap_r.at[index], other)
        for keep in range(2):
            block = core if keep else 1 - core

            def tile(t, carry, keep=keep, block=block):
                at = pl.ds(pl.multiple_of(t * half, half), half)
                nr, ni = read(at)
                real, imag = complex_product(
                    nr, ni, branches[step, 0, :, columns(block)], branches[step, 1, :, columns(block)]
                )
                place = target.at[core] if keep else swap.at[index]
                place[0, at] = real.astype(BF16)
                place[1, at] = imag.astype(BF16)
                return carry

            lax.fori_loop(0, rows // half, tile, 0)
            if not keep:
                copy.start()
        copy.wait()

    def plain(step, source, target):
        for block in range(width // half):
            across = pl.ds(block * half, half)

            def tile(t, carry, across=across):
                at = pl.ds(pl.multiple_of(t * half, half), half)
                real, imag = complex_product(
                    jnp.concatenate([source[0, 0, at], source[1, 0, at]], axis=1),
                    jnp.concatenate([source[0, 1, at], source[1, 1, at]], axis=1),
                    branches[step, 0, :, across], branches[step, 1, :, across],
                )
                target[0, at, across] = real.astype(target.dtype)
                target[1, at, across] = imag.astype(target.dtype)
                return carry

            lax.fori_loop(0, rows // half, tile, 0)

    swapped(0, 0, lambda at: (stem[0, at].astype(BF16), stem[1, at].astype(BF16)), net1)
    plain(1, net1, net2)
    swapped(2, 1, lambda at: (net2[0, at], net2[1, at]), net3)
    net_copy = pltpu.make_async_copy(net3, net_out, local_sem.at[4])
    net_copy.start()
    net_copy.wait()
    last_copy.wait()

    leaf_copies[1].wait_send()
    pair_copy.wait_send()
    for c in range(CHUNKS):
        z_copy(c).wait_send()
        for i in range(2):
            y_copy(i, c).wait_send()
        for i in range(4):
            core_copy(i, c).wait_send()


def finish(net, branch, out):
    half = net.shape[3]
    for block in range(branch.shape[2] // half):
        across = pl.ds(block * half, half)
        real, imag = complex_product(
            jnp.concatenate([net[0, 0], net[1, 0]], axis=1),
            jnp.concatenate([net[0, 1], net[1, 1]], axis=1),
            branch[0, :, across], branch[1, :, across],
        )
        out[0, :, across] = real
        out[1, :, across] = imag


PARTS = 16
SPREAD = 16
ACROSS = 11
HALVE = 8


def each(n, body):
    def step(i, carry):
        body(i)
        return carry

    lax.fori_loop(0, n, step, 0)


def matching(roots, group):
    seen = jnp.int32(0)
    found = []
    for k in range(roots.shape[0]):
        holds = jnp.where(roots[k] // GROUP == group, 1, 0)
        found.append((holds, seen))
        seen = seen + holds
    return found


def step_of(roots, group, rank):
    total = jnp.int32(0)
    for k, (holds, seen) in enumerate(matching(roots, group)):
        total = total + jnp.where(seen == rank, holds * k, 0)
    return total


def two_groups(
    third, roots_in, orders_in, stem_in, leaves_in, net_out, last_out, roots, orders,
    leaf, outgoing, arrived, mine, chosen, pair, branches, stem, stems, net1, net2, net3, final,
    local_sem, leaf_s, leaf_r, pair_s, pair_r, whole_s, whole_r,
    y_s, y_r, core_s, core_r, mid_s, end_s, far_r, stem_s, stem_r, swap_s, swap_r,
):
    width = stem.shape[2]
    half = width // 2
    core = lax.axis_index("narrow")
    wide = lax.axis_index("wide")
    group = wide // GROUP
    member = wide % GROUP
    y = member % 2
    z = member // 2
    inner = group + z == 1
    other = {"narrow": 1 - core}
    over_y = {"wide": wide + 1 - 2 * y}
    over_z = {"wide": wide + 2 - 4 * z}
    over_mid = {"wide": wide + 2 - 4 * group}
    MESH = pl.DeviceIdType.MESH
    sets = 2 if third else 1
    left = group == 1 if third else group >= 0

    fetch = pltpu.make_async_copy(leaves_in.at[0], leaf, local_sem.at[0])
    stem_copy = pltpu.make_async_copy(stem_in, stem, local_sem.at[1])
    fetch.start()
    barrier = pltpu.get_barrier_semaphore()
    for peer in [other, over_y, over_z]:
        pl.semaphore_signal(barrier, inc=1, device_id=peer, device_id_type=MESH)

    @pl.when(inner)
    def _():
        pl.semaphore_signal(barrier, inc=1, device_id=over_mid, device_id_type=MESH)

    scalars = [
        pltpu.make_async_copy(roots_in, roots, local_sem.at[2]),
        pltpu.make_async_copy(orders_in, orders, local_sem.at[3]),
    ]
    for copy in scalars:
        copy.start()
    for copy in scalars:
        copy.wait()
    k_right = step_of(roots, group, 0)
    k_left = [step_of(roots, group, 1 + e) for e in range(sets)]

    def own_rows(j=0, n=1):
        size = half // n
        return pl.ds(pl.multiple_of(core * half + j * size, size), size)

    def one_hot(k, low, n):
        column = lax.broadcasted_iota(jnp.int32, (8, n), 1) + low
        source = jnp.zeros((8, n), jnp.int32)
        for b in range(orders.shape[1]):
            weight = jnp.left_shift(jnp.int32(1), orders[k, b])
            source = source + (jnp.right_shift(column, b) & 1) * weight

        def tile(i):
            row = lax.broadcasted_iota(jnp.int32, (TILE, n), 0) + i * TILE
            at = pl.ds(pl.multiple_of(i * TILE, TILE), TILE)
            same = row == jnp.broadcast_to(source[0:1], (TILE, n))
            chosen[at, :n] = jnp.where(same, 1.0, 0.0).astype(F32).astype(BF16)

        each(width // TILE, tile)

    def leaf_copy(e, j):
        size = half // PARTS
        at = pl.ds(pl.multiple_of(j * size, size), size)
        return remote(
            outgoing.at[e, :, at], arrived.at[e, :, own_rows(j, PARTS)], leaf_s.at[e], leaf_r.at[e, j], over_y
        )

    @pl.when(jnp.logical_and(y * z == 1, left))
    def _():
        one_hot(k_left[0], core * half, half)

    @pl.when(inner)
    def _():
        pl.semaphore_wait(barrier, 4)

    @pl.when(jnp.logical_not(inner))
    def _():
        pl.semaphore_wait(barrier, 3)

    @pl.when(y == 0)
    def _():
        fetch.wait()
        for c in range(2):
            outgoing[0, c] = leaf[k_right, c, own_rows()]
        each(PARTS, lambda j: leaf_copy(0, j).start())
        for e in range(sets):
            for c in range(2):
                mine[e, c] = leaf[k_left[e], c].T

    @pl.when(y == 1)
    def _():
        fetch.wait()

        @pl.when(left)
        def _():
            for e in range(sets):

                def launch(i, first, second, e=e):
                    outgoing[e, 0, i * TILE : (i + 1) * TILE] = first.T
                    outgoing[e, 1, i * TILE : (i + 1) * TILE] = second.T
                    n = PARTS * TILE // half
                    each(n, lambda j: leaf_copy(e, i * n + j).start())

                @pl.when(z == 0)
                def _():
                    for i in range(half // TILE):
                        launch(i, *[leaf[k_left[e], c, :, own_rows(i, half // TILE)] for c in range(2)])

                @pl.when(z == 1)
                def _():
                    if e:
                        one_hot(k_left[e], core * half, half)
                    ordered = [dot(leaf[k_left[e], c], chosen[:, :half]).astype(BF16) for c in range(2)]
                    for i in range(half // TILE):
                        launch(i, *[array[:, i * TILE : (i + 1) * TILE] for array in ordered])

        @pl.when(z == 0)
        def _():
            for c in range(2):
                mine[0, c] = leaf[k_right, c]

        @pl.when(z == 1)
        def _():
            one_hot(k_right, 0, width)
            for c in range(2):
                mine[0, c] = dot(leaf[k_right, c], chosen[...]).astype(BF16)

    stem_copy.start()
    stem_copy.wait()
    for c in range(2):
        stems[core, c] = stem[c].astype(BF16)
    stem_share = remote(stems.at[core], stems.at[core], stem_s, stem_r, other)
    stem_share.start()

    def pair_copy(e, j):
        place = pair.at[e, z, :, own_rows(j, PARTS)]
        return remote(place, place, pair_s.at[e], pair_r.at[e, j], over_z)

    def whole_copy(e, j):
        place = pair.at[e, y, :, own_rows(j, PARTS)]
        return remote(place, place, whole_s.at[e], whole_r.at[e], other)

    def pairs(e, first, last):
        def turn(j):
            leaf_copy(e, j).wait_recv()
            at = own_rows(j, PARTS)

            real, imag = complex_product(arrived[e, 0, at], arrived[e, 1, at], mine[e, 0], mine[e, 1])
            pair[e, z, 0, at] = real.astype(BF16)
            pair[e, z, 1, at] = imag.astype(BF16)
            pair_copy(e, j).start()

            @pl.when(z == y)
            def _():
                whole_copy(e, j).start()

        each(last - first, lambda j: turn(j + first))

    def half_pair(e):
        return pair.at[e, 0, :, own_rows()]

    def join(e):
        def arrive(j):
            pair_copy(e, j).wait_recv()

            @pl.when(z != y)
            def _():
                whole_copy(e, j).start()

        each(PARTS, arrive)
        remote(half_pair(e), half_pair(e), whole_s.at[e], whole_r.at[e], other).wait_recv()

    A, C, D, E = range(4)

    def rows_first(t):
        return t in (A, C)

    def place(t, r, n=1):
        if rows_first(t):
            size = half // SPREAD
            return branches.at[t, :, pl.ds(pl.multiple_of(core * half + r * size, size), n * size)]
        size = width // SPREAD
        if n > 1:
            return branches.at[t, :, : n * size, own_rows()]
        row = (r % (SPREAD // 2)) * (2 * size)
        return branches.at[t, :, pl.ds(pl.multiple_of(row, size), 2 * size), own_rows(r // (SPREAD // 2), 2)]

    def y_copy(t, r, n=1):
        return remote(place(t, r, n), place(t, r, n), y_s.at[t], y_r.at[t, r], over_y)

    def core_copy(t, r, n=1):
        return remote(place(t, r, n), place(t, r, n), core_s.at[t], core_r.at[t], other)

    def mid_copy(t, r, n=1):
        return remote(place(t, r, n), place(t, r, n), mid_s.at[t], far_r.at[t, r], over_mid)

    def end_copy(t, r, n=1):
        return remote(place(t, r, n), place(t, r, n), end_s.at[t], far_r.at[t, r], over_z)

    sent = {}

    def send(copy, t, r, n):
        if copy in (mid_copy, end_copy):

            @pl.when(inner)
            def _():
                copy(t, r).start()

        else:
            copy(t, r).start()
        sent[copy, t, n] = True

    def ship(t, r):
        send(mid_copy, t, r, (0, SPREAD))
        send(y_copy, t, r, (0, SPREAD))
        send(core_copy, t, r, (0, SPREAD))

    def own(e, t):
        def turn(b):
            at = own_rows(b, 2)
            real, imag = complex_product(
                pair[e, 1 - y, 0, at], pair[e, 1 - y, 1, at], pair[e, y, 0], pair[e, y, 1]
            )
            if rows_first(t):
                branches[t, 0, at] = real.astype(BF16)
                branches[t, 1, at] = imag.astype(BF16)
                each(SPREAD // 2, lambda i: ship(t, b * (SPREAD // 2) + i))
            else:
                branches[t, 0, :, at] = real.T.astype(BF16)
                branches[t, 1, :, at] = imag.T.astype(BF16)
                if not e:
                    each(SPREAD // 2, lambda i: ship(t, b * (SPREAD // 2) + i))

        each(2, turn)
        if e:
            each(HALVE, lambda r: send(mid_copy, t, r, (0, HALVE)))

            def turn_sent(i):
                r = (i + HALVE) % SPREAD
                send(y_copy, t, r, (0, SPREAD))
                send(core_copy, t, r, (0, SPREAD))

            each(SPREAD, turn_sent)

    def receive(first, last, *turns):
        def turn(i):
            for t, origin, onward, shift in turns:
                r = i + first + shift
                span = (first + shift, last + shift)
                if origin == "z":
                    mid_copy(t, r).wait_recv()
                else:
                    y_copy(t, r).wait_recv()
                for letter, copy in (("e", end_copy), ("m", mid_copy), ("y", y_copy)):
                    if letter in onward:
                        send(copy, t, r, span)
                send(core_copy, t, r, span)

        each(last - first, turn)

    def exchange(far, beside, beyond):
        receive(0, ACROSS, (far, "z", "ey", 0), (beside, "y", "", 0))
        receive(ACROSS, SPREAD, (far, "z", "e", 0), (beside, "y", "m", 0))
        if 2 * ACROSS == SPREAD:
            receive(0, ACROSS, (beyond, "y", "", 0), (beyond, "z", "e", ACROSS))
        else:
            receive(ACROSS, SPREAD, (beyond, "z", "e", 0))
            receive(0, ACROSS, (beyond, "y", "", 0))

    def build(t):
        pairs(0, 0, PARTS)
        join(0)
        own(0, t)

    def role_right_low():
        build(A)
        if third:
            receive(0, SPREAD, (C, "z", "ey", 0))
            receive(0, SPREAD, (E, "y", "", 0))
        else:
            exchange(C, D, E)

    def role_right_high():
        build(C)
        if third:
            receive(0, SPREAD, (A, "z", "e", 0), (E, "y", "", 0))
        else:
            exchange(A, E, D)

    def role_left_low():
        if third:
            receive(0, SPREAD, (A, "y", "m", 0), (E, "z", "ey", 0))
            receive(0, SPREAD - HALVE, (C, "y", "", 0))
            receive(0, HALVE, (C, "y", "", SPREAD - HALVE), (D, "z", "ey", 0))
        else:
            build(D)
            exchange(E, A, C)

    def role_left_high():
        if third:
            pairs(0, 0, PARTS)
            pairs(1, 0, PARTS // 4)
            join(0)
            own(0, E)
            pairs(1, PARTS // 4, PARTS)
            join(1)
            own(1, D)
            receive(0, SPREAD, (A, "z", "e", 0))
            receive(0, SPREAD, (C, "y", "", 0))
        else:
            build(E)
            exchange(D, C, A)

    def last_right_low():
        receive(HALVE, SPREAD, (D, "z", "ey", 0))
        receive(0, HALVE, (D, "y", "", 0))

    def last_right_high():
        receive(HALVE, SPREAD, (D, "y", "m", 0))
        receive(0, HALVE, (D, "y", "", 0))

    def last_left_low():
        receive(HALVE, SPREAD, (D, "y", "", 0))

    drains = []

    def play(roles):
        for at_y, at_group, role in roles:
            sent.clear()
            here = jnp.logical_and(y == at_y, group == at_group)
            pl.when(here)(role)
            drains.append((here, list(sent)))

    def columns(block):
        return pl.ds(pl.multiple_of(block * half, half), half)

    zeros = matching(roots, 0)
    ones = matching(roots, 1)
    source = []
    for k in range(roots.shape[0]):
        high = jnp.where(ones[k][1] == 2, D, C + 2 * ones[k][1])
        at = jnp.where(zeros[k][0] == 1, A + 2 * zeros[k][1], high)
        source.append(jnp.minimum(at, 3))

    def first():
        def turn(i):
            picked = []
            for c in range(2):
                one = branches[A, c, :, columns(core)]
                two = branches[C, c, :, columns(core)]
                if third:
                    picked.append(jnp.where(jnp.full(one.shape, source[0], jnp.int32) == A, one, two))
                else:
                    picked.append(branches[source[0], c, :, columns(core)])
            real, imag = complex_product(stems[i, 0], stems[i, 1], *picked)
            net1[i, 0] = real.astype(BF16)
            net1[i, 1] = imag.astype(BF16)

        each(2, turn)

    play([(1, 0, role_right_low), (1, 1, role_right_high), (0, 0, role_left_low), (0, 1, role_left_high)])
    stem_share.wait()
    for t in (A, C):
        core_copy(t, 0, SPREAD).wait_recv()
    if third:
        first()
        play([(1, 0, last_right_low), (1, 1, last_right_high), (0, 0, last_left_low)])
    for t in (D, E):
        core_copy(t, 0, SPREAD).wait_recv()
    last_copy = pltpu.make_async_copy(final, last_out, local_sem.at[2])
    if not third:
        first()

    spans = [(0, 2 * TILE)] + [(low, TILE) for low in range(2 * TILE, net2.shape[2], TILE)]

    def exchange_copy(i):
        place = net2.at[core, :, pl.ds(*spans[i])]
        return remote(place, place, swap_s, swap_r.at[i], other)

    for i, span in enumerate(spans):
        at = pl.ds(*span)
        real, imag = complex_product(
            jnp.concatenate([net1[0, 0, at], net1[1, 0, at]], axis=1),
            jnp.concatenate([net1[0, 1, at], net1[1, 1, at]], axis=1),
            branches[source[1], 0], branches[source[1], 1],
        )
        net2[core, 0, at] = real.astype(BF16)
        net2[core, 1, at] = imag.astype(BF16)
        exchange_copy(i).start()

    def net_copy(i):
        return pltpu.make_async_copy(net3.at[i], net_out.at[i], local_sem.at[3 * i])

    def third_step(i):
        whose = core + i * (1 - 2 * core)

        @pl.when(i == 1)
        def _():
            for c in range(2):
                final[c] = branches[source[3], c]
            last_copy.start()
            for j in range(len(spans)):
                exchange_copy(j).wait_recv()

        real, imag = complex_product(
            net2[whose, 0], net2[whose, 1],
            branches[source[2], 0, :, columns(core)], branches[source[2], 1, :, columns(core)],
        )
        net3[whose, 0] = real.astype(BF16)
        net3[whose, 1] = imag.astype(BF16)

        @pl.when(i == 0)
        def _():
            net_copy(core).start()

    each(2, third_step)
    net_copy(1 - core).start()
    net_copy(core).wait()
    net_copy(1 - core).wait()
    remote(net2.at[core], net2.at[core], swap_s, swap_r.at[0], other).wait_send()
    last_copy.wait()

    def drain(e):
        place = half_pair(e)
        remote(place, place, pair_s.at[e], pair_r.at[e, 0], over_z).wait_send()
        remote(place, place, whole_s.at[e], whole_r.at[e], other).wait_send()

    def drain_leaf(e):
        place = arrived.at[e, :, own_rows()]
        remote(outgoing.at[e], place, leaf_s.at[e], leaf_r.at[e, 0], over_y).wait_send()

    @pl.when(y == 0)
    def _():
        drain_leaf(0)

        @pl.when(left)
        def _():
            for e in range(sets):
                drain(e)

    @pl.when(y == 1)
    def _():
        drain(0)

        @pl.when(left)
        def _():
            for e in range(sets):
                drain_leaf(e)

    for here, copies in drains:
        totals = {}
        for copy, t, (low, high) in copies:
            totals[copy, t] = totals.get((copy, t), 0) + high - low

        @pl.when(here)
        def _(totals=totals):
            for (copy, t), n in totals.items():
                if copy not in (mid_copy, end_copy):
                    copy(t, 0, n).wait_send()

            @pl.when(inner)
            def _():
                for (copy, t), n in totals.items():
                    if copy in (mid_copy, end_copy):
                        copy(t, 0, n).wait_send()


def general(stem_tensor, leaves, root_devices, mode_orders):
    _, rows, width = stem_tensor.shape
    half = width // 2
    part = half // CHUNKS
    groups = lax.axis_size("wide") // GROUP
    rounds = groups.bit_length() - 1
    vmem = pltpu.VMEM
    dma = pltpu.SemaphoreType.DMA
    network, last = pl.pallas_call(
        functools.partial(kernel, rounds),
        out_shape=(
            jax.ShapeDtypeStruct((2, 2, rows, half), BF16),
            jax.ShapeDtypeStruct((2, width, width), BF16),
        ),
        in_specs=[pl.BlockSpec(memory_space=pltpu.SMEM)] * 2
        + [pl.BlockSpec(memory_space=pl.ANY)] * 2,
        out_specs=[pl.BlockSpec(memory_space=pl.ANY)] * 2,
        scratch_shapes=[
            vmem((2, 2, 2, width, width), BF16),
            vmem((2, 2, half, width), BF16),
            vmem((2, half, width), BF16),
            vmem((2, width, width), BF16),
            vmem((width, width), BF16),
            vmem((max(rounds, 1), CHUNKS, 2, part, width), BF16),
            vmem((max(rounds, 1), CHUNKS, 2, part, width), BF16),
            vmem((GROUP, 2, width, width), BF16),
            vmem((2, rows, width), F32),
            vmem((2, 2, rows, half), BF16),
            vmem((2, rows, width), BF16),
            vmem((2, 2, rows, half), BF16),
            vmem((2, 2, rows, half), BF16),
            dma((5,)),
            dma((2,)), dma((2,)), dma((2,)), dma((2,)),
            dma, dma, dma, dma,
            dma((max(rounds, 1), CHUNKS)), dma((max(rounds, 1), CHUNKS)),
            dma((CHUNKS,)), dma((CHUNKS,)),
            dma((2, CHUNKS)), dma((2, CHUNKS)),
            dma((4, CHUNKS)), dma((4, CHUNKS)),
            dma((2,)), dma((2,)),
        ],
        compiler_params=pltpu.CompilerParams(collective_id=0, has_side_effects=True),
    )(root_devices, mode_orders, stem_tensor, leaves)
    return network, last


def closing(network, last, stem_tensor):
    _, rows, width = stem_tensor.shape
    half = width // 2
    return pl.pallas_call(
        finish,
        grid=(rows // half,),
        out_shape=jax.ShapeDtypeStruct(stem_tensor.shape, F32),
        in_specs=[
            pl.BlockSpec((2, 2, half, half), lambda i: (0, 0, i, 0)),
            pl.BlockSpec((2, width, width), lambda i: (0, 0, 0)),
        ],
        out_specs=pl.BlockSpec((2, half, width), lambda i: (0, i, 0)),
    )(network, last)


def split(third, stem_tensor, leaves, root_devices, mode_orders):
    _, rows, width = stem_tensor.shape
    half = width // 2
    sets = 2 if third else 1
    vmem = pltpu.VMEM
    dma = pltpu.SemaphoreType.DMA
    return pl.pallas_call(
        functools.partial(two_groups, third),
        out_shape=(
            jax.ShapeDtypeStruct((2, 2, rows, half), BF16),
            jax.ShapeDtypeStruct((2, width, width), BF16),
        ),
        in_specs=[pl.BlockSpec(memory_space=pl.ANY)] * 4,
        out_specs=[pl.BlockSpec(memory_space=pl.ANY)] * 2,
        scratch_shapes=[
            pltpu.SMEM(root_devices.shape, jnp.int32),
            pltpu.SMEM(mode_orders.shape, jnp.int32),
            vmem((leaves.shape[1], 2, width, width), BF16),
            vmem((sets, 2, half, width), BF16),
            vmem((sets, 2, width, width), BF16),
            vmem((sets, 2, width, width), BF16),
            vmem((width, width), BF16),
            vmem((sets, 2, 2, width, width), BF16),
            vmem((4, 2, width, width), BF16),
            vmem((2, rows, width), F32),
            vmem((2, 2, rows, width), BF16),
            vmem((2, 2, rows, half), BF16),
            vmem((2, 2, rows, width), BF16),
            vmem((2, 2, rows, half), BF16),
            vmem((2, width, width), BF16),
            dma((4,)),
        ]
        + [dma((sets,)), dma((sets, PARTS)), dma((sets,)), dma((sets, PARTS)), dma((sets,)), dma((sets,))]
        + [dma((4,)), dma((4, SPREAD)), dma((4,)), dma((4,)), dma((4,)), dma((4,)), dma((4, SPREAD))]
        + [dma, dma, dma, dma((rows // TILE,))],
        compiler_params=pltpu.CompilerParams(collective_id=2 if third else 1, has_side_effects=True),
    )(root_devices, mode_orders, stem_tensor, leaves)


def local(stem_tensor, leaves, root_devices, mode_orders):
    arrays = (stem_tensor, leaves, root_devices, mode_orders)
    if lax.axis_size("wide") // GROUP == 2:
        even = jnp.sum((root_devices // GROUP).astype(jnp.int32)) == 2
        network, last = lax.cond(
            even, functools.partial(split, False), functools.partial(split, True), *arrays
        )
    else:
        network, last = general(*arrays)
    return closing(network, last, stem_tensor)


def solution(mesh):
    stem_spec = P(None, ("cuts", "wide", "narrow"), None)
    return jax.shard_map(
        local,
        mesh=mesh,
        in_specs=(stem_spec, P(("cuts", "wide"), None, None, None, None), P(), P()),
        out_specs=stem_spec,
        check_vma=False,
    )
```

```python
import functools

import jax
import jax.numpy as jnp
from jax import lax
from jax.experimental import pallas as pl
from jax.experimental.pallas import tpu as pltpu
from jax.sharding import PartitionSpec as P

GROUP = 4
CHUNKS = 8
FLIGHT = 2
TILE = 128
BF16 = jnp.bfloat16
F32 = jnp.float32


def dot(x, y):
    return jnp.dot(x, y, preferred_element_type=F32)


def complex_product(ar, ai, br, bi):
    left = jnp.concatenate([ar, ai], axis=1)
    return (
        dot(left, jnp.concatenate([br, -bi], axis=0)),
        dot(left, jnp.concatenate([bi, br], axis=0)),
    )


def remote(src, dst, send_sem, recv_sem, device):
    return pltpu.make_async_remote_copy(
        src_ref=src,
        dst_ref=dst,
        send_sem=send_sem,
        recv_sem=recv_sem,
        device_id=device,
        device_id_type=pl.DeviceIdType.MESH,
    )


def kernel(
    rounds, roots, orders, stem_in, leaves_in, net_out, last_out,
    leaf, pair, away, high, chosen, held, crossed, branches, stem, net1, net2, net3, swap,
    local_sem, leaf_s, leaf_r, fwd_s, fwd_r, pair_s, pair_r, high_s, high_r,
    cross_s, cross_r, z_s, z_r, y_s, y_r, core_s, core_r, swap_s, swap_r,
):
    width = stem.shape[2]
    rows = stem.shape[1]
    half = width // 2
    part = half // CHUNKS
    core = lax.axis_index("narrow")
    wide = lax.axis_index("wide")
    member = wide % GROUP
    y = member % 2
    z = member // 2
    other = {"narrow": 1 - core}
    over_y = {"wide": wide + 1 - 2 * y}
    over_z = {"wide": wide + 2 - 4 * z}
    bits = [(wide // (GROUP << r)) % 2 for r in range(rounds)]
    over_group = [{"wide": wide + (GROUP << r) * (1 - 2 * bits[r])} for r in range(rounds)]

    barrier = pltpu.get_barrier_semaphore()
    for peer in [other, over_y, over_z] + over_group:
        pl.semaphore_signal(barrier, inc=1, device_id=peer, device_id_type=pl.DeviceIdType.MESH)
    own_rows = pl.ds(pl.multiple_of(core * half, half), half)
    own_copies = [
        pltpu.make_async_copy(leaves_in.at[0, 2 * s + y], leaf.at[s, y], local_sem.at[s])
        for s in range(2)
    ]
    stem_copy = pltpu.make_async_copy(stem_in, stem, local_sem.at[2])
    pl.semaphore_wait(barrier, 3 + rounds)

    phases = [1 - z, z]
    leaf_copies = []
    for i, s in enumerate(phases):
        copy = remote(
            leaves_in.at[0, 2 * s + 1 - y, :, own_rows],
            leaf.at[s, y, :, own_rows],
            leaf_s.at[i], leaf_r.at[i], over_y,
        )
        leaf_copies.append(copy)
    leaf_copies[0].start()
    for copy in own_copies:
        copy.start()
    stem_copy.start()

    def choose(i, carry):
        column = lax.broadcasted_iota(jnp.int32, (TILE, width), 1)
        source = jnp.zeros((TILE, width), jnp.int32)
        for b in range(orders.shape[1]):
            weight = jnp.left_shift(jnp.int32(1), orders[member, b])
            source = source + (jnp.right_shift(column, b) & 1) * weight
        row = lax.broadcasted_iota(jnp.int32, (TILE, width), 0) + i * TILE
        at = pl.ds(pl.multiple_of(i * TILE, TILE), TILE)
        chosen[at] = jnp.where(row == source, 1.0, 0.0).astype(F32).astype(BF16)
        return carry

    lax.fori_loop(0, width // TILE, choose, 0)
    for copy in own_copies:
        copy.wait()

    pair_copy = remote(away, pair.at[z], pair_s, pair_r, over_z)
    leaf_copies[0].wait_send()
    leaf_copies[1].start()
    for i, s in enumerate(phases):
        leaf_copies[i].wait_recv()
        forward = remote(
            leaf.at[s, 1 - y, :, own_rows], leaf.at[s, 1 - y, :, own_rows],
            fwd_s.at[i], fwd_r.at[i], other,
        )
        forward.start()
        forward.wait()

        def pair_tile(t, carry, s=s, i=i):
            at = pl.ds(pl.multiple_of(t * half, half), half)
            real, imag = complex_product(
                leaf[s, 0, 0, own_rows], leaf[s, 0, 1, own_rows],
                leaf[s, 1, 0, :, at], leaf[s, 1, 1, :, at],
            )
            target = away if i == 0 else pair.at[z]
            target[0, :, at] = real.astype(BF16)
            target[1, :, at] = imag.astype(BF16)
            return carry

        lax.fori_loop(0, width // half, pair_tile, 0)
        if i == 0:
            pair_copy.start()
    pair_copy.wait_recv()

    def high_tile(t, carry):
        at = pl.ds(pl.multiple_of(t * half, half), half)
        for c in range(2):
            high[c, own_rows, at] = dot(pair[1, c], chosen[:, at]).astype(BF16)
        return carry

    lax.fori_loop(0, width // half, high_tile, 0)
    high_copy = remote(high.at[:, own_rows], high.at[:, own_rows], high_s, high_r, other)
    high_copy.start()
    high_copy.wait()

    def rows_of(c):
        return pl.ds(pl.multiple_of(core * half + c * part, part), part)

    def cross_copy(r, c):
        return remote(held.at[r, c], crossed.at[r, c], cross_s.at[r, c], cross_r.at[r, c], over_group[r])

    def place(origin, c):
        return branches.at[origin, :, rows_of(c)]

    origins = [member, member + 2 - 4 * z, member + 1 - 2 * y, GROUP - 1 - member]

    def z_copy(c):
        return remote(place(origins[0], c), place(origins[0], c), z_s.at[c], z_r.at[c], over_z)

    def y_copy(i, c):
        return remote(place(origins[i], c), place(origins[i], c), y_s.at[i, c], y_r.at[i, c], over_y)

    def core_copy(i, c):
        return remote(place(origins[i], c), place(origins[i], c), core_s.at[i, c], core_r.at[i, c], other)

    def spread(c):
        z_copy(c).start()
        y_copy(0, c).start()
        core_copy(0, c).start()

    def select(r, c):
        cross_copy(r, c).wait_recv()
        cross_copy(r, c).wait_send()
        if c + FLIGHT < CHUNKS:
            cross_copy(r, c + FLIGHT).start()
        root_bit = (roots[member] // (GROUP << r)) % 2
        for p in range(2):
            here = held[r, c, p].astype(F32)
            there = crossed[r, c, p].astype(F32)
            same = jnp.full(here.shape, root_bit, jnp.int32) == bits[r]
            picked = jnp.where(same, here, there).astype(BF16)
            if r + 1 < rounds:
                held[r + 1, c, p] = picked
            else:
                branches[member, p, rows_of(c)] = picked
        if r + 1 < rounds:
            if c < FLIGHT:
                cross_copy(r + 1, c).start()
        else:
            spread(c)

    def on_z(c):
        z_copy(c).wait_recv()
        y_copy(1, c).start()
        core_copy(1, c).start()

    def on_y(i, c):
        y_copy(i, c).wait_recv()
        core_copy(2 + i, c).start()

    for c in range(CHUNKS):
        at = pl.ds(c * part, part)
        real, imag = complex_product(pair[0, 0, at], pair[0, 1, at], high[0], high[1])
        if rounds:
            held[0, c, 0] = real.astype(BF16)
            held[0, c, 1] = imag.astype(BF16)
            if c < FLIGHT:
                cross_copy(0, c).start()
        else:
            branches[member, 0, rows_of(c)] = real.astype(BF16)
            branches[member, 1, rows_of(c)] = imag.astype(BF16)
            spread(c)

    for r in range(rounds - 1):
        for c in range(CHUNKS):
            select(r, c)
    for c in range(CHUNKS + 2):
        if rounds and c < CHUNKS:
            select(rounds - 1, c)
        if 1 <= c <= CHUNKS:
            on_z(c - 1)
            on_y(0, c - 1)
        if c >= 2:
            on_y(1, c - 2)
    stem_copy.wait()
    for c in range(CHUNKS):
        for i in range(4):
            core_copy(i, c).wait_recv()
    last_copy = pltpu.make_async_copy(branches.at[GROUP - 1], last_out, local_sem.at[3])
    last_copy.start()

    def columns(block):
        return pl.ds(pl.multiple_of(block * half, half), half)

    def swapped(step, index, read, target):
        copy = remote(swap.at[index], target.at[core], swap_s.at[index], swap_r.at[index], other)
        for keep in range(2):
            block = core if keep else 1 - core

            def tile(t, carry, keep=keep, block=block):
                at = pl.ds(pl.multiple_of(t * half, half), half)
                nr, ni = read(at)
                real, imag = complex_product(
                    nr, ni, branches[step, 0, :, columns(block)], branches[step, 1, :, columns(block)]
                )
                place = target.at[core] if keep else swap.at[index]
                place[0, at] = real.astype(BF16)
                place[1, at] = imag.astype(BF16)
                return carry

            lax.fori_loop(0, rows // half, tile, 0)
            if not keep:
                copy.start()
        copy.wait()

    def plain(step, source, target):
        for block in range(width // half):
            across = pl.ds(block * half, half)

            def tile(t, carry, across=across):
                at = pl.ds(pl.multiple_of(t * half, half), half)
                real, imag = complex_product(
                    jnp.concatenate([source[0, 0, at], source[1, 0, at]], axis=1),
                    jnp.concatenate([source[0, 1, at], source[1, 1, at]], axis=1),
                    branches[step, 0, :, across], branches[step, 1, :, across],
                )
                target[0, at, across] = real.astype(target.dtype)
                target[1, at, across] = imag.astype(target.dtype)
                return carry

            lax.fori_loop(0, rows // half, tile, 0)

    swapped(0, 0, lambda at: (stem[0, at].astype(BF16), stem[1, at].astype(BF16)), net1)
    plain(1, net1, net2)
    swapped(2, 1, lambda at: (net2[0, at], net2[1, at]), net3)
    net_copy = pltpu.make_async_copy(net3, net_out, local_sem.at[4])
    net_copy.start()
    net_copy.wait()
    last_copy.wait()

    leaf_copies[1].wait_send()
    pair_copy.wait_send()
    for c in range(CHUNKS):
        z_copy(c).wait_send()
        for i in range(2):
            y_copy(i, c).wait_send()
        for i in range(4):
            core_copy(i, c).wait_send()


def finish(net, branch, out):
    half = net.shape[3]
    for block in range(branch.shape[2] // half):
        across = pl.ds(block * half, half)
        real, imag = complex_product(
            jnp.concatenate([net[0, 0], net[1, 0]], axis=1),
            jnp.concatenate([net[0, 1], net[1, 1]], axis=1),
            branch[0, :, across], branch[1, :, across],
        )
        out[0, :, across] = real
        out[1, :, across] = imag


PARTS = 16
SPREAD = 16
ACROSS = 11
HALVE = 8


def each(n, body):
    def step(i, carry):
        body(i)
        return carry

    lax.fori_loop(0, n, step, 0)


def matching(roots, group):
    seen = jnp.int32(0)
    found = []
    for k in range(roots.shape[0]):
        holds = jnp.where(roots[k] // GROUP == group, 1, 0)
        found.append((holds, seen))
        seen = seen + holds
    return found


def step_of(roots, group, rank):
    total = jnp.int32(0)
    for k, (holds, seen) in enumerate(matching(roots, group)):
        total = total + jnp.where(seen == rank, holds * k, 0)
    return total


def two_groups(
    third, roots_in, orders_in, stem_in, leaves_in, net_out, last_out, roots, orders,
    leaf, outgoing, arrived, mine, chosen, pair, branches, stem, stems, net1, net2, net3, final,
    local_sem, leaf_s, leaf_r, pair_s, pair_r, whole_s, whole_r,
    y_s, y_r, core_s, core_r, mid_s, end_s, far_r, stem_s, stem_r, swap_s, swap_r,
):
    width = stem.shape[2]
    half = width // 2
    core = lax.axis_index("narrow")
    wide = lax.axis_index("wide")
    group = wide // GROUP
    member = wide % GROUP
    y = member % 2
    z = member // 2
    inner = group + z == 1
    other = {"narrow": 1 - core}
    over_y = {"wide": wide + 1 - 2 * y}
    over_z = {"wide": wide + 2 - 4 * z}
    over_mid = {"wide": wide + 2 - 4 * group}
    MESH = pl.DeviceIdType.MESH
    sets = 2 if third else 1
    left = group == 1 if third else group >= 0

    fetch = pltpu.make_async_copy(leaves_in.at[0], leaf, local_sem.at[0])
    stem_copy = pltpu.make_async_copy(stem_in, stem, local_sem.at[1])
    fetch.start()
    barrier = pltpu.get_barrier_semaphore()
    for peer in [other, over_y, over_z]:
        pl.semaphore_signal(barrier, inc=1, device_id=peer, device_id_type=MESH)

    @pl.when(inner)
    def _():
        pl.semaphore_signal(barrier, inc=1, device_id=over_mid, device_id_type=MESH)

    scalars = [
        pltpu.make_async_copy(roots_in, roots, local_sem.at[2]),
        pltpu.make_async_copy(orders_in, orders, local_sem.at[3]),
    ]
    for copy in scalars:
        copy.start()
    for copy in scalars:
        copy.wait()
    k_right = step_of(roots, group, 0)
    k_left = [step_of(roots, group, 1 + e) for e in range(sets)]

    def own_rows(j=0, n=1):
        size = half // n
        return pl.ds(pl.multiple_of(core * half + j * size, size), size)

    def one_hot(k, low, n):
        column = lax.broadcasted_iota(jnp.int32, (8, n), 1) + low
        source = jnp.zeros((8, n), jnp.int32)
        for b in range(orders.shape[1]):
            weight = jnp.left_shift(jnp.int32(1), orders[k, b])
            source = source + (jnp.right_shift(column, b) & 1) * weight

        def tile(i):
            row = lax.broadcasted_iota(jnp.int32, (TILE, n), 0) + i * TILE
            at = pl.ds(pl.multiple_of(i * TILE, TILE), TILE)
            same = row == jnp.broadcast_to(source[0:1], (TILE, n))
            chosen[at, :n] = jnp.where(same, 1.0, 0.0).astype(F32).astype(BF16)

        each(width // TILE, tile)

    def leaf_copy(e, j):
        size = half // PARTS
        at = pl.ds(pl.multiple_of(j * size, size), size)
        return remote(
            outgoing.at[e, :, at], arrived.at[e, :, own_rows(j, PARTS)], leaf_s.at[e], leaf_r.at[e, j], over_y
        )

    @pl.when(jnp.logical_and(y * z == 1, left))
    def _():
        one_hot(k_left[0], core * half, half)

    @pl.when(inner)
    def _():
        pl.semaphore_wait(barrier, 4)

    @pl.when(jnp.logical_not(inner))
    def _():
        pl.semaphore_wait(barrier, 3)

    @pl.when(y == 0)
    def _():
        fetch.wait()
        stem_copy.start()
        for c in range(2):
            outgoing[0, c] = leaf[k_right, c, own_rows()]
        each(PARTS, lambda j: leaf_copy(0, j).start())
        for e in range(sets):
            for c in range(2):
                mine[e, c] = leaf[k_left[e], c].T

    @pl.when(y == 1)
    def _():
        fetch.wait()
        stem_copy.start()

        @pl.when(left)
        def _():
            for e in range(sets):

                @pl.when(z == 0)
                def _():
                    for c in range(2):
                        outgoing[e, c] = leaf[k_left[e], c, :, own_rows()].T

                @pl.when(z == 1)
                def _():
                    if e:
                        one_hot(k_left[e], core * half, half)
                    for c in range(2):
                        outgoing[e, c] = dot(leaf[k_left[e], c], chosen[:, :half]).astype(BF16).T

                each(PARTS, lambda j, e=e: leaf_copy(e, j).start())

        @pl.when(z == 0)
        def _():
            for c in range(2):
                mine[0, c] = leaf[k_right, c]

        @pl.when(z == 1)
        def _():
            one_hot(k_right, 0, width)
            for c in range(2):
                mine[0, c] = dot(leaf[k_right, c], chosen[...]).astype(BF16)

    stem_copy.wait()
    for c in range(2):
        stems[core, c] = stem[c].astype(BF16)
    stem_share = remote(stems.at[core], stems.at[core], stem_s, stem_r, other)
    stem_share.start()

    def pair_copy(e, j):
        place = pair.at[e, z, :, own_rows(j, PARTS)]
        return remote(place, place, pair_s.at[e], pair_r.at[e, j], over_z)

    def whole_copy(e, j):
        place = pair.at[e, y, :, own_rows(j, PARTS)]
        return remote(place, place, whole_s.at[e], whole_r.at[e], other)

    def pairs(e, first, last):
        def turn(j):
            leaf_copy(e, j).wait_recv()
            at = own_rows(j, PARTS)

            real, imag = complex_product(arrived[e, 0, at], arrived[e, 1, at], mine[e, 0], mine[e, 1])
            pair[e, z, 0, at] = real.astype(BF16)
            pair[e, z, 1, at] = imag.astype(BF16)
            pair_copy(e, j).start()

            @pl.when(z == y)
            def _():
                whole_copy(e, j).start()

        each(last - first, lambda j: turn(j + first))

    def half_pair(e):
        return pair.at[e, 0, :, own_rows()]

    def join(e):
        def arrive(j):
            pair_copy(e, j).wait_recv()

            @pl.when(z != y)
            def _():
                whole_copy(e, j).start()

        each(PARTS, arrive)
        remote(half_pair(e), half_pair(e), whole_s.at[e], whole_r.at[e], other).wait_recv()

    A, C, D, E = range(4)

    def rows_first(t):
        return t in (A, C)

    def place(t, r, n=1):
        if rows_first(t):
            size = half // SPREAD
            return branches.at[t, :, pl.ds(pl.multiple_of(core * half + r * size, size), n * size)]
        size = width // SPREAD
        if n > 1:
            return branches.at[t, :, : n * size, own_rows()]
        row = (r % (SPREAD // 2)) * (2 * size)
        return branches.at[t, :, pl.ds(pl.multiple_of(row, size), 2 * size), own_rows(r // (SPREAD // 2), 2)]

    def y_copy(t, r, n=1):
        return remote(place(t, r, n), place(t, r, n), y_s.at[t], y_r.at[t, r], over_y)

    def core_copy(t, r, n=1):
        return remote(place(t, r, n), place(t, r, n), core_s.at[t], core_r.at[t], other)

    def mid_copy(t, r, n=1):
        return remote(place(t, r, n), place(t, r, n), mid_s.at[t], far_r.at[t, r], over_mid)

    def end_copy(t, r, n=1):
        return remote(place(t, r, n), place(t, r, n), end_s.at[t], far_r.at[t, r], over_z)

    sent = {}

    def send(copy, t, r, n):
        if copy in (mid_copy, end_copy):

            @pl.when(inner)
            def _():
                copy(t, r).start()

        else:
            copy(t, r).start()
        sent[copy, t, n] = True

    def ship(t, r):
        send(mid_copy, t, r, (0, SPREAD))
        send(y_copy, t, r, (0, SPREAD))
        send(core_copy, t, r, (0, SPREAD))

    def own(e, t):
        def turn(b):
            at = own_rows(b, 2)
            real, imag = complex_product(
                pair[e, 1 - y, 0, at], pair[e, 1 - y, 1, at], pair[e, y, 0], pair[e, y, 1]
            )
            if rows_first(t):
                branches[t, 0, at] = real.astype(BF16)
                branches[t, 1, at] = imag.astype(BF16)
                each(SPREAD // 2, lambda i: ship(t, b * (SPREAD // 2) + i))
            else:
                branches[t, 0, :, at] = real.T.astype(BF16)
                branches[t, 1, :, at] = imag.T.astype(BF16)
                if not e:
                    each(SPREAD // 2, lambda i: ship(t, b * (SPREAD // 2) + i))

        each(2, turn)
        if e:
            each(HALVE, lambda r: send(mid_copy, t, r, (0, HALVE)))

            def turn_sent(i):
                r = (i + HALVE) % SPREAD
                send(y_copy, t, r, (0, SPREAD))
                send(core_copy, t, r, (0, SPREAD))

            each(SPREAD, turn_sent)

    def receive(first, last, *turns):
        def turn(i):
            for t, origin, onward, shift in turns:
                r = i + first + shift
                span = (first + shift, last + shift)
                if origin == "z":
                    mid_copy(t, r).wait_recv()
                else:
                    y_copy(t, r).wait_recv()
                for letter, copy in (("e", end_copy), ("m", mid_copy), ("y", y_copy)):
                    if letter in onward:
                        send(copy, t, r, span)
                send(core_copy, t, r, span)

        each(last - first, turn)

    def exchange(far, beside, beyond):
        receive(0, ACROSS, (far, "z", "ey", 0), (beside, "y", "", 0))
        receive(ACROSS, SPREAD, (far, "z", "e", 0), (beside, "y", "m", 0))
        if 2 * ACROSS == SPREAD:
            receive(0, ACROSS, (beyond, "y", "", 0), (beyond, "z", "e", ACROSS))
        else:
            receive(ACROSS, SPREAD, (beyond, "z", "e", 0))
            receive(0, ACROSS, (beyond, "y", "", 0))

    def build(t):
        pairs(0, 0, PARTS)
        join(0)
        own(0, t)

    def role_right_low():
        build(A)
        if third:
            receive(0, SPREAD, (C, "z", "ey", 0))
            receive(0, SPREAD, (E, "y", "", 0))
        else:
            exchange(C, D, E)

    def role_right_high():
        build(C)
        if third:
            receive(0, SPREAD, (A, "z", "e", 0), (E, "y", "", 0))
        else:
            exchange(A, E, D)

    def role_left_low():
        if third:
            receive(0, SPREAD, (A, "y", "m", 0), (E, "z", "ey", 0))
            receive(0, SPREAD - HALVE, (C, "y", "", 0))
            receive(0, HALVE, (C, "y", "", SPREAD - HALVE), (D, "z", "ey", 0))
        else:
            build(D)
            exchange(E, A, C)

    def role_left_high():
        if third:
            pairs(0, 0, PARTS)
            pairs(1, 0, PARTS // 2)
            join(0)
            own(0, E)
            pairs(1, PARTS // 2, PARTS)
            join(1)
            own(1, D)
            receive(0, SPREAD, (A, "z", "e", 0))
            receive(0, SPREAD, (C, "y", "", 0))
        else:
            build(E)
            exchange(D, C, A)

    def last_right_low():
        receive(HALVE, SPREAD, (D, "z", "ey", 0))
        receive(0, HALVE, (D, "y", "", 0))

    def last_right_high():
        receive(HALVE, SPREAD, (D, "y", "m", 0))
        receive(0, HALVE, (D, "y", "", 0))

    def last_left_low():
        receive(HALVE, SPREAD, (D, "y", "", 0))

    drains = []

    def play(roles):
        for at_y, at_group, role in roles:
            sent.clear()
            here = jnp.logical_and(y == at_y, group == at_group)
            pl.when(here)(role)
            drains.append((here, list(sent)))

    def columns(block):
        return pl.ds(pl.multiple_of(block * half, half), half)

    zeros = matching(roots, 0)
    ones = matching(roots, 1)
    source = []
    for k in range(roots.shape[0]):
        high = jnp.where(ones[k][1] == 2, D, C + 2 * ones[k][1])
        at = jnp.where(zeros[k][0] == 1, A + 2 * zeros[k][1], high)
        source.append(jnp.minimum(at, 3))

    def first():
        def turn(i):
            picked = []
            for c in range(2):
                one = branches[A, c, :, columns(core)]
                two = branches[C, c, :, columns(core)]
                if third:
                    picked.append(jnp.where(jnp.full(one.shape, source[0], jnp.int32) == A, one, two))
                else:
                    picked.append(branches[source[0], c, :, columns(core)])
            real, imag = complex_product(stems[i, 0], stems[i, 1], *picked)
            net1[i, 0] = real.astype(BF16)
            net1[i, 1] = imag.astype(BF16)

        each(2, turn)

    play([(1, 0, role_right_low), (1, 1, role_right_high), (0, 0, role_left_low), (0, 1, role_left_high)])
    stem_share.wait()
    for t in (A, C):
        core_copy(t, 0, SPREAD).wait_recv()
    if third:
        first()
        play([(1, 0, last_right_low), (1, 1, last_right_high), (0, 0, last_left_low)])
    for t in (D, E):
        core_copy(t, 0, SPREAD).wait_recv()
    for c in range(2):
        final[c] = branches[source[3], c]
    last_copy = pltpu.make_async_copy(final, last_out, local_sem.at[2])
    last_copy.start()
    if not third:
        first()

    def exchange_copy(i):
        at = pl.ds(pl.multiple_of(i * TILE, TILE), TILE)
        return remote(net2.at[core, :, at], net2.at[core, :, at], swap_s, swap_r.at[i], other)

    def second(i):
        at = pl.ds(pl.multiple_of(i * TILE, TILE), TILE)
        real, imag = complex_product(
            jnp.concatenate([net1[0, 0, at], net1[1, 0, at]], axis=1),
            jnp.concatenate([net1[0, 1, at], net1[1, 1, at]], axis=1),
            branches[source[1], 0], branches[source[1], 1],
        )
        net2[core, 0, at] = real.astype(BF16)
        net2[core, 1, at] = imag.astype(BF16)
        exchange_copy(i).start()

    tiles = net2.shape[2] // TILE
    each(tiles, second)

    def net_copy(i):
        return pltpu.make_async_copy(net3.at[i], net_out.at[i], local_sem.at[3 * i])

    def third_step(i):
        whose = core + i * (1 - 2 * core)

        @pl.when(i == 1)
        def _():
            each(tiles, lambda j: exchange_copy(j).wait_recv())

        real, imag = complex_product(
            net2[whose, 0], net2[whose, 1],
            branches[source[2], 0, :, columns(core)], branches[source[2], 1, :, columns(core)],
        )
        net3[whose, 0] = real.astype(BF16)
        net3[whose, 1] = imag.astype(BF16)

        @pl.when(i == 0)
        def _():
            net_copy(core).start()

    each(2, third_step)
    net_copy(1 - core).start()
    net_copy(core).wait()
    net_copy(1 - core).wait()
    remote(net2.at[core], net2.at[core], swap_s, swap_r.at[0], other).wait_send()
    last_copy.wait()

    def drain(e):
        place = half_pair(e)
        remote(place, place, pair_s.at[e], pair_r.at[e, 0], over_z).wait_send()
        remote(place, place, whole_s.at[e], whole_r.at[e], other).wait_send()

    def drain_leaf(e):
        place = arrived.at[e, :, own_rows()]
        remote(outgoing.at[e], place, leaf_s.at[e], leaf_r.at[e, 0], over_y).wait_send()

    @pl.when(y == 0)
    def _():
        drain_leaf(0)

        @pl.when(left)
        def _():
            for e in range(sets):
                drain(e)

    @pl.when(y == 1)
    def _():
        drain(0)

        @pl.when(left)
        def _():
            for e in range(sets):
                drain_leaf(e)

    for here, copies in drains:
        totals = {}
        for copy, t, (low, high) in copies:
            totals[copy, t] = totals.get((copy, t), 0) + high - low

        @pl.when(here)
        def _(totals=totals):
            for (copy, t), n in totals.items():
                if copy not in (mid_copy, end_copy):
                    copy(t, 0, n).wait_send()

            @pl.when(inner)
            def _():
                for (copy, t), n in totals.items():
                    if copy in (mid_copy, end_copy):
                        copy(t, 0, n).wait_send()


def general(stem_tensor, leaves, root_devices, mode_orders):
    _, rows, width = stem_tensor.shape
    half = width // 2
    part = half // CHUNKS
    groups = lax.axis_size("wide") // GROUP
    rounds = groups.bit_length() - 1
    vmem = pltpu.VMEM
    dma = pltpu.SemaphoreType.DMA
    network, last = pl.pallas_call(
        functools.partial(kernel, rounds),
        out_shape=(
            jax.ShapeDtypeStruct((2, 2, rows, half), BF16),
            jax.ShapeDtypeStruct((2, width, width), BF16),
        ),
        in_specs=[pl.BlockSpec(memory_space=pltpu.SMEM)] * 2
        + [pl.BlockSpec(memory_space=pl.ANY)] * 2,
        out_specs=[pl.BlockSpec(memory_space=pl.ANY)] * 2,
        scratch_shapes=[
            vmem((2, 2, 2, width, width), BF16),
            vmem((2, 2, half, width), BF16),
            vmem((2, half, width), BF16),
            vmem((2, width, width), BF16),
            vmem((width, width), BF16),
            vmem((max(rounds, 1), CHUNKS, 2, part, width), BF16),
            vmem((max(rounds, 1), CHUNKS, 2, part, width), BF16),
            vmem((GROUP, 2, width, width), BF16),
            vmem((2, rows, width), F32),
            vmem((2, 2, rows, half), BF16),
            vmem((2, rows, width), BF16),
            vmem((2, 2, rows, half), BF16),
            vmem((2, 2, rows, half), BF16),
            dma((5,)),
            dma((2,)), dma((2,)), dma((2,)), dma((2,)),
            dma, dma, dma, dma,
            dma((max(rounds, 1), CHUNKS)), dma((max(rounds, 1), CHUNKS)),
            dma((CHUNKS,)), dma((CHUNKS,)),
            dma((2, CHUNKS)), dma((2, CHUNKS)),
            dma((4, CHUNKS)), dma((4, CHUNKS)),
            dma((2,)), dma((2,)),
        ],
        compiler_params=pltpu.CompilerParams(collective_id=0, has_side_effects=True),
    )(root_devices, mode_orders, stem_tensor, leaves)
    return network, last


def closing(network, last, stem_tensor):
    _, rows, width = stem_tensor.shape
    half = width // 2
    return pl.pallas_call(
        finish,
        grid=(rows // half,),
        out_shape=jax.ShapeDtypeStruct(stem_tensor.shape, F32),
        in_specs=[
            pl.BlockSpec((2, 2, half, half), lambda i: (0, 0, i, 0)),
            pl.BlockSpec((2, width, width), lambda i: (0, 0, 0)),
        ],
        out_specs=pl.BlockSpec((2, half, width), lambda i: (0, i, 0)),
    )(network, last)


def split(third, stem_tensor, leaves, root_devices, mode_orders):
    _, rows, width = stem_tensor.shape
    half = width // 2
    sets = 2 if third else 1
    vmem = pltpu.VMEM
    dma = pltpu.SemaphoreType.DMA
    return pl.pallas_call(
        functools.partial(two_groups, third),
        out_shape=(
            jax.ShapeDtypeStruct((2, 2, rows, half), BF16),
            jax.ShapeDtypeStruct((2, width, width), BF16),
        ),
        in_specs=[pl.BlockSpec(memory_space=pl.ANY)] * 4,
        out_specs=[pl.BlockSpec(memory_space=pl.ANY)] * 2,
        scratch_shapes=[
            pltpu.SMEM(root_devices.shape, jnp.int32),
            pltpu.SMEM(mode_orders.shape, jnp.int32),
            vmem((leaves.shape[1], 2, width, width), BF16),
            vmem((sets, 2, half, width), BF16),
            vmem((sets, 2, width, width), BF16),
            vmem((sets, 2, width, width), BF16),
            vmem((width, width), BF16),
            vmem((sets, 2, 2, width, width), BF16),
            vmem((4, 2, width, width), BF16),
            vmem((2, rows, width), F32),
            vmem((2, 2, rows, width), BF16),
            vmem((2, 2, rows, half), BF16),
            vmem((2, 2, rows, width), BF16),
            vmem((2, 2, rows, half), BF16),
            vmem((2, width, width), BF16),
            dma((4,)),
        ]
        + [dma((sets,)), dma((sets, PARTS)), dma((sets,)), dma((sets, PARTS)), dma((sets,)), dma((sets,))]
        + [dma((4,)), dma((4, SPREAD)), dma((4,)), dma((4,)), dma((4,)), dma((4,)), dma((4, SPREAD))]
        + [dma, dma, dma, dma((rows // TILE,))],
        compiler_params=pltpu.CompilerParams(collective_id=2 if third else 1, has_side_effects=True),
    )(root_devices, mode_orders, stem_tensor, leaves)


def local(stem_tensor, leaves, root_devices, mode_orders):
    arrays = (stem_tensor, leaves, root_devices, mode_orders)
    if lax.axis_size("wide") // GROUP == 2:
        even = jnp.sum((root_devices // GROUP).astype(jnp.int32)) == 2
        network, last = lax.cond(
            even, functools.partial(split, False), functools.partial(split, True), *arrays
        )
    else:
        network, last = general(*arrays)
    return closing(network, last, stem_tensor)


def solution(mesh):
    stem_spec = P(None, ("cuts", "wide", "narrow"), None)
    return jax.shard_map(
        local,
        mesh=mesh,
        in_specs=(stem_spec, P(("cuts", "wide"), None, None, None, None), P(), P()),
        out_specs=stem_spec,
        check_vma=False,
    )
```

```python
import functools

import jax
import jax.numpy as jnp
from jax import lax
from jax.experimental import pallas as pl
from jax.experimental.pallas import tpu as pltpu
from jax.sharding import PartitionSpec as P

GROUP = 4
CHUNKS = 8
FLIGHT = 2
TILE = 128
BF16 = jnp.bfloat16
F32 = jnp.float32


def dot(x, y):
    return jnp.dot(x, y, preferred_element_type=F32)


def complex_product(ar, ai, br, bi):
    left = jnp.concatenate([ar, ai], axis=1)
    return (
        dot(left, jnp.concatenate([br, -bi], axis=0)),
        dot(left, jnp.concatenate([bi, br], axis=0)),
    )


def remote(src, dst, send_sem, recv_sem, device):
    return pltpu.make_async_remote_copy(
        src_ref=src,
        dst_ref=dst,
        send_sem=send_sem,
        recv_sem=recv_sem,
        device_id=device,
        device_id_type=pl.DeviceIdType.MESH,
    )


def kernel(
    rounds, roots, orders, stem_in, leaves_in, net_out, last_out,
    leaf, pair, away, high, chosen, held, crossed, branches, stem, net1, net2, net3, swap,
    local_sem, leaf_s, leaf_r, fwd_s, fwd_r, pair_s, pair_r, high_s, high_r,
    cross_s, cross_r, z_s, z_r, y_s, y_r, core_s, core_r, swap_s, swap_r,
):
    width = stem.shape[2]
    rows = stem.shape[1]
    half = width // 2
    part = half // CHUNKS
    core = lax.axis_index("narrow")
    wide = lax.axis_index("wide")
    member = wide % GROUP
    y = member % 2
    z = member // 2
    other = {"narrow": 1 - core}
    over_y = {"wide": wide + 1 - 2 * y}
    over_z = {"wide": wide + 2 - 4 * z}
    bits = [(wide // (GROUP << r)) % 2 for r in range(rounds)]
    over_group = [{"wide": wide + (GROUP << r) * (1 - 2 * bits[r])} for r in range(rounds)]

    barrier = pltpu.get_barrier_semaphore()
    for peer in [other, over_y, over_z] + over_group:
        pl.semaphore_signal(barrier, inc=1, device_id=peer, device_id_type=pl.DeviceIdType.MESH)
    own_rows = pl.ds(pl.multiple_of(core * half, half), half)
    own_copies = [
        pltpu.make_async_copy(leaves_in.at[0, 2 * s + y], leaf.at[s, y], local_sem.at[s])
        for s in range(2)
    ]
    stem_copy = pltpu.make_async_copy(stem_in, stem, local_sem.at[2])
    pl.semaphore_wait(barrier, 3 + rounds)

    phases = [1 - z, z]
    leaf_copies = []
    for i, s in enumerate(phases):
        copy = remote(
            leaves_in.at[0, 2 * s + 1 - y, :, own_rows],
            leaf.at[s, y, :, own_rows],
            leaf_s.at[i], leaf_r.at[i], over_y,
        )
        leaf_copies.append(copy)
    leaf_copies[0].start()
    for copy in own_copies:
        copy.start()
    stem_copy.start()

    def choose(i, carry):
        column = lax.broadcasted_iota(jnp.int32, (TILE, width), 1)
        source = jnp.zeros((TILE, width), jnp.int32)
        for b in range(orders.shape[1]):
            weight = jnp.left_shift(jnp.int32(1), orders[member, b])
            source = source + (jnp.right_shift(column, b) & 1) * weight
        row = lax.broadcasted_iota(jnp.int32, (TILE, width), 0) + i * TILE
        at = pl.ds(pl.multiple_of(i * TILE, TILE), TILE)
        chosen[at] = jnp.where(row == source, 1.0, 0.0).astype(F32).astype(BF16)
        return carry

    lax.fori_loop(0, width // TILE, choose, 0)
    for copy in own_copies:
        copy.wait()

    pair_copy = remote(away, pair.at[z], pair_s, pair_r, over_z)
    leaf_copies[0].wait_send()
    leaf_copies[1].start()
    for i, s in enumerate(phases):
        leaf_copies[i].wait_recv()
        forward = remote(
            leaf.at[s, 1 - y, :, own_rows], leaf.at[s, 1 - y, :, own_rows],
            fwd_s.at[i], fwd_r.at[i], other,
        )
        forward.start()
        forward.wait()

        def pair_tile(t, carry, s=s, i=i):
            at = pl.ds(pl.multiple_of(t * half, half), half)
            real, imag = complex_product(
                leaf[s, 0, 0, own_rows], leaf[s, 0, 1, own_rows],
                leaf[s, 1, 0, :, at], leaf[s, 1, 1, :, at],
            )
            target = away if i == 0 else pair.at[z]
            target[0, :, at] = real.astype(BF16)
            target[1, :, at] = imag.astype(BF16)
            return carry

        lax.fori_loop(0, width // half, pair_tile, 0)
        if i == 0:
            pair_copy.start()
    pair_copy.wait_recv()

    def high_tile(t, carry):
        at = pl.ds(pl.multiple_of(t * half, half), half)
        for c in range(2):
            high[c, own_rows, at] = dot(pair[1, c], chosen[:, at]).astype(BF16)
        return carry

    lax.fori_loop(0, width // half, high_tile, 0)
    high_copy = remote(high.at[:, own_rows], high.at[:, own_rows], high_s, high_r, other)
    high_copy.start()
    high_copy.wait()

    def rows_of(c):
        return pl.ds(pl.multiple_of(core * half + c * part, part), part)

    def cross_copy(r, c):
        return remote(held.at[r, c], crossed.at[r, c], cross_s.at[r, c], cross_r.at[r, c], over_group[r])

    def place(origin, c):
        return branches.at[origin, :, rows_of(c)]

    origins = [member, member + 2 - 4 * z, member + 1 - 2 * y, GROUP - 1 - member]

    def z_copy(c):
        return remote(place(origins[0], c), place(origins[0], c), z_s.at[c], z_r.at[c], over_z)

    def y_copy(i, c):
        return remote(place(origins[i], c), place(origins[i], c), y_s.at[i, c], y_r.at[i, c], over_y)

    def core_copy(i, c):
        return remote(place(origins[i], c), place(origins[i], c), core_s.at[i, c], core_r.at[i, c], other)

    def spread(c):
        z_copy(c).start()
        y_copy(0, c).start()
        core_copy(0, c).start()

    def select(r, c):
        cross_copy(r, c).wait_recv()
        cross_copy(r, c).wait_send()
        if c + FLIGHT < CHUNKS:
            cross_copy(r, c + FLIGHT).start()
        root_bit = (roots[member] // (GROUP << r)) % 2
        for p in range(2):
            here = held[r, c, p].astype(F32)
            there = crossed[r, c, p].astype(F32)
            same = jnp.full(here.shape, root_bit, jnp.int32) == bits[r]
            picked = jnp.where(same, here, there).astype(BF16)
            if r + 1 < rounds:
                held[r + 1, c, p] = picked
            else:
                branches[member, p, rows_of(c)] = picked
        if r + 1 < rounds:
            if c < FLIGHT:
                cross_copy(r + 1, c).start()
        else:
            spread(c)

    def on_z(c):
        z_copy(c).wait_recv()
        y_copy(1, c).start()
        core_copy(1, c).start()

    def on_y(i, c):
        y_copy(i, c).wait_recv()
        core_copy(2 + i, c).start()

    for c in range(CHUNKS):
        at = pl.ds(c * part, part)
        real, imag = complex_product(pair[0, 0, at], pair[0, 1, at], high[0], high[1])
        if rounds:
            held[0, c, 0] = real.astype(BF16)
            held[0, c, 1] = imag.astype(BF16)
            if c < FLIGHT:
                cross_copy(0, c).start()
        else:
            branches[member, 0, rows_of(c)] = real.astype(BF16)
            branches[member, 1, rows_of(c)] = imag.astype(BF16)
            spread(c)

    for r in range(rounds - 1):
        for c in range(CHUNKS):
            select(r, c)
    for c in range(CHUNKS + 2):
        if rounds and c < CHUNKS:
            select(rounds - 1, c)
        if 1 <= c <= CHUNKS:
            on_z(c - 1)
            on_y(0, c - 1)
        if c >= 2:
            on_y(1, c - 2)
    stem_copy.wait()
    for c in range(CHUNKS):
        for i in range(4):
            core_copy(i, c).wait_recv()
    last_copy = pltpu.make_async_copy(branches.at[GROUP - 1], last_out, local_sem.at[3])
    last_copy.start()

    def columns(block):
        return pl.ds(pl.multiple_of(block * half, half), half)

    def swapped(step, index, read, target):
        copy = remote(swap.at[index], target.at[core], swap_s.at[index], swap_r.at[index], other)
        for keep in range(2):
            block = core if keep else 1 - core

            def tile(t, carry, keep=keep, block=block):
                at = pl.ds(pl.multiple_of(t * half, half), half)
                nr, ni = read(at)
                real, imag = complex_product(
                    nr, ni, branches[step, 0, :, columns(block)], branches[step, 1, :, columns(block)]
                )
                place = target.at[core] if keep else swap.at[index]
                place[0, at] = real.astype(BF16)
                place[1, at] = imag.astype(BF16)
                return carry

            lax.fori_loop(0, rows // half, tile, 0)
            if not keep:
                copy.start()
        copy.wait()

    def plain(step, source, target):
        for block in range(width // half):
            across = pl.ds(block * half, half)

            def tile(t, carry, across=across):
                at = pl.ds(pl.multiple_of(t * half, half), half)
                real, imag = complex_product(
                    jnp.concatenate([source[0, 0, at], source[1, 0, at]], axis=1),
                    jnp.concatenate([source[0, 1, at], source[1, 1, at]], axis=1),
                    branches[step, 0, :, across], branches[step, 1, :, across],
                )
                target[0, at, across] = real.astype(target.dtype)
                target[1, at, across] = imag.astype(target.dtype)
                return carry

            lax.fori_loop(0, rows // half, tile, 0)

    swapped(0, 0, lambda at: (stem[0, at].astype(BF16), stem[1, at].astype(BF16)), net1)
    plain(1, net1, net2)
    swapped(2, 1, lambda at: (net2[0, at], net2[1, at]), net3)
    net_copy = pltpu.make_async_copy(net3, net_out, local_sem.at[4])
    net_copy.start()
    net_copy.wait()
    last_copy.wait()

    leaf_copies[1].wait_send()
    pair_copy.wait_send()
    for c in range(CHUNKS):
        z_copy(c).wait_send()
        for i in range(2):
            y_copy(i, c).wait_send()
        for i in range(4):
            core_copy(i, c).wait_send()


def finish(net, branch, out):
    half = net.shape[3]
    for block in range(branch.shape[2] // half):
        across = pl.ds(block * half, half)
        real, imag = complex_product(
            jnp.concatenate([net[0, 0], net[1, 0]], axis=1),
            jnp.concatenate([net[0, 1], net[1, 1]], axis=1),
            branch[0, :, across], branch[1, :, across],
        )
        out[0, :, across] = real
        out[1, :, across] = imag


PARTS = 16
SPREAD = 16
ACROSS = 11
HALVE = 8


def each(n, body):
    def step(i, carry):
        body(i)
        return carry

    lax.fori_loop(0, n, step, 0)


def matching(roots, group):
    seen = jnp.int32(0)
    found = []
    for k in range(roots.shape[0]):
        holds = jnp.where(roots[k] // GROUP == group, 1, 0)
        found.append((holds, seen))
        seen = seen + holds
    return found


def step_of(roots, group, rank):
    total = jnp.int32(0)
    for k, (holds, seen) in enumerate(matching(roots, group)):
        total = total + jnp.where(seen == rank, holds * k, 0)
    return total


def two_groups(
    third, roots_in, orders_in, stem_in, leaves_in, net_out, last_out, roots, orders,
    leaf, outgoing, arrived, mine, chosen, pair, branches, stem, stems, net1, net2, net3, final,
    local_sem, leaf_s, leaf_r, pair_s, pair_r, whole_s, whole_r,
    y_s, y_r, core_s, core_r, mid_s, end_s, far_r, stem_s, stem_r, swap_s, swap_r,
):
    width = stem.shape[2]
    half = width // 2
    core = lax.axis_index("narrow")
    wide = lax.axis_index("wide")
    group = wide // GROUP
    member = wide % GROUP
    y = member % 2
    z = member // 2
    inner = group + z == 1
    other = {"narrow": 1 - core}
    over_y = {"wide": wide + 1 - 2 * y}
    over_z = {"wide": wide + 2 - 4 * z}
    over_mid = {"wide": wide + 2 - 4 * group}
    MESH = pl.DeviceIdType.MESH
    sets = 2 if third else 1
    left = group == 1 if third else group >= 0

    fetch = pltpu.make_async_copy(leaves_in.at[0], leaf, local_sem.at[0])
    stem_copy = pltpu.make_async_copy(stem_in, stem, local_sem.at[1])
    fetch.start()
    barrier = pltpu.get_barrier_semaphore()
    for peer in [other, over_y, over_z]:
        pl.semaphore_signal(barrier, inc=1, device_id=peer, device_id_type=MESH)

    @pl.when(inner)
    def _():
        pl.semaphore_signal(barrier, inc=1, device_id=over_mid, device_id_type=MESH)

    scalars = [
        pltpu.make_async_copy(roots_in, roots, local_sem.at[2]),
        pltpu.make_async_copy(orders_in, orders, local_sem.at[3]),
    ]
    for copy in scalars:
        copy.start()
    for copy in scalars:
        copy.wait()
    k_right = step_of(roots, group, 0)
    k_left = [step_of(roots, group, 1 + e) for e in range(sets)]

    def own_rows(j=0, n=1):
        size = half // n
        return pl.ds(pl.multiple_of(core * half + j * size, size), size)

    def one_hot(k, low, n):
        column = lax.broadcasted_iota(jnp.int32, (8, n), 1) + low
        source = jnp.zeros((8, n), jnp.int32)
        for b in range(orders.shape[1]):
            weight = jnp.left_shift(jnp.int32(1), orders[k, b])
            source = source + (jnp.right_shift(column, b) & 1) * weight

        def tile(i):
            row = lax.broadcasted_iota(jnp.int32, (TILE, n), 0) + i * TILE
            at = pl.ds(pl.multiple_of(i * TILE, TILE), TILE)
            same = row == jnp.broadcast_to(source[0:1], (TILE, n))
            chosen[at, :n] = jnp.where(same, 1.0, 0.0).astype(F32).astype(BF16)

        each(width // TILE, tile)

    def leaf_copy(e, j):
        size = half // PARTS
        at = pl.ds(pl.multiple_of(j * size, size), size)
        return remote(
            outgoing.at[e, :, at], arrived.at[e, :, own_rows(j, PARTS)], leaf_s.at[e], leaf_r.at[e, j], over_y
        )

    @pl.when(jnp.logical_and(y * z == 1, left))
    def _():
        one_hot(k_left[0], core * half, half)

    @pl.when(inner)
    def _():
        pl.semaphore_wait(barrier, 4)

    @pl.when(jnp.logical_not(inner))
    def _():
        pl.semaphore_wait(barrier, 3)

    @pl.when(y == 0)
    def _():
        fetch.wait()
        for c in range(2):
            outgoing[0, c] = leaf[k_right, c, own_rows()]
        each(PARTS, lambda j: leaf_copy(0, j).start())
        for e in range(sets):
            for c in range(2):
                mine[e, c] = leaf[k_left[e], c].T

    @pl.when(y == 1)
    def _():
        fetch.wait()

        @pl.when(left)
        def _():
            for e in range(sets):

                @pl.when(z == 0)
                def _():
                    for c in range(2):
                        outgoing[e, c] = leaf[k_left[e], c, :, own_rows()].T

                @pl.when(z == 1)
                def _():
                    if e:
                        one_hot(k_left[e], core * half, half)
                    for c in range(2):
                        outgoing[e, c] = dot(leaf[k_left[e], c], chosen[:, :half]).astype(BF16).T

                each(PARTS, lambda j, e=e: leaf_copy(e, j).start())

        @pl.when(z == 0)
        def _():
            for c in range(2):
                mine[0, c] = leaf[k_right, c]

        @pl.when(z == 1)
        def _():
            one_hot(k_right, 0, width)
            for c in range(2):
                mine[0, c] = dot(leaf[k_right, c], chosen[...]).astype(BF16)

    stem_copy.start()
    stem_copy.wait()
    for c in range(2):
        stems[core, c] = stem[c].astype(BF16)
    stem_share = remote(stems.at[core], stems.at[core], stem_s, stem_r, other)
    stem_share.start()

    def pair_copy(e, j):
        place = pair.at[e, z, :, own_rows(j, PARTS)]
        return remote(place, place, pair_s.at[e], pair_r.at[e, j], over_z)

    def whole_copy(e, j):
        place = pair.at[e, y, :, own_rows(j, PARTS)]
        return remote(place, place, whole_s.at[e], whole_r.at[e], other)

    def pairs(e, first, last):
        def turn(j):
            leaf_copy(e, j).wait_recv()
            at = own_rows(j, PARTS)

            real, imag = complex_product(arrived[e, 0, at], arrived[e, 1, at], mine[e, 0], mine[e, 1])
            pair[e, z, 0, at] = real.astype(BF16)
            pair[e, z, 1, at] = imag.astype(BF16)
            pair_copy(e, j).start()

            @pl.when(z == y)
            def _():
                whole_copy(e, j).start()

        each(last - first, lambda j: turn(j + first))

    def half_pair(e):
        return pair.at[e, 0, :, own_rows()]

    def join(e):
        def arrive(j):
            pair_copy(e, j).wait_recv()

            @pl.when(z != y)
            def _():
                whole_copy(e, j).start()

        each(PARTS, arrive)
        remote(half_pair(e), half_pair(e), whole_s.at[e], whole_r.at[e], other).wait_recv()

    A, C, D, E = range(4)

    def rows_first(t):
        return t in (A, C)

    def place(t, r, n=1):
        if rows_first(t):
            size = half // SPREAD
            return branches.at[t, :, pl.ds(pl.multiple_of(core * half + r * size, size), n * size)]
        size = width // SPREAD
        if n > 1:
            return branches.at[t, :, : n * size, own_rows()]
        row = (r % (SPREAD // 2)) * (2 * size)
        return branches.at[t, :, pl.ds(pl.multiple_of(row, size), 2 * size), own_rows(r // (SPREAD // 2), 2)]

    def y_copy(t, r, n=1):
        return remote(place(t, r, n), place(t, r, n), y_s.at[t], y_r.at[t, r], over_y)

    def core_copy(t, r, n=1):
        return remote(place(t, r, n), place(t, r, n), core_s.at[t], core_r.at[t], other)

    def mid_copy(t, r, n=1):
        return remote(place(t, r, n), place(t, r, n), mid_s.at[t], far_r.at[t, r], over_mid)

    def end_copy(t, r, n=1):
        return remote(place(t, r, n), place(t, r, n), end_s.at[t], far_r.at[t, r], over_z)

    sent = {}

    def send(copy, t, r, n):
        if copy in (mid_copy, end_copy):

            @pl.when(inner)
            def _():
                copy(t, r).start()

        else:
            copy(t, r).start()
        sent[copy, t, n] = True

    def ship(t, r):
        send(mid_copy, t, r, (0, SPREAD))
        send(y_copy, t, r, (0, SPREAD))
        send(core_copy, t, r, (0, SPREAD))

    def own(e, t):
        def turn(b):
            at = own_rows(b, 2)
            real, imag = complex_product(
                pair[e, 1 - y, 0, at], pair[e, 1 - y, 1, at], pair[e, y, 0], pair[e, y, 1]
            )
            if rows_first(t):
                branches[t, 0, at] = real.astype(BF16)
                branches[t, 1, at] = imag.astype(BF16)
                each(SPREAD // 2, lambda i: ship(t, b * (SPREAD // 2) + i))
            else:
                branches[t, 0, :, at] = real.T.astype(BF16)
                branches[t, 1, :, at] = imag.T.astype(BF16)
                if not e:
                    each(SPREAD // 2, lambda i: ship(t, b * (SPREAD // 2) + i))

        each(2, turn)
        if e:
            each(HALVE, lambda r: send(mid_copy, t, r, (0, HALVE)))

            def turn_sent(i):
                r = (i + HALVE) % SPREAD
                send(y_copy, t, r, (0, SPREAD))
                send(core_copy, t, r, (0, SPREAD))

            each(SPREAD, turn_sent)

    def receive(first, last, *turns):
        def turn(i):
            for t, origin, onward, shift in turns:
                r = i + first + shift
                span = (first + shift, last + shift)
                if origin == "z":
                    mid_copy(t, r).wait_recv()
                else:
                    y_copy(t, r).wait_recv()
                for letter, copy in (("e", end_copy), ("m", mid_copy), ("y", y_copy)):
                    if letter in onward:
                        send(copy, t, r, span)
                send(core_copy, t, r, span)

        each(last - first, turn)

    def exchange(far, beside, beyond):
        receive(0, ACROSS, (far, "z", "ey", 0), (beside, "y", "", 0))
        receive(ACROSS, SPREAD, (far, "z", "e", 0), (beside, "y", "m", 0))
        if 2 * ACROSS == SPREAD:
            receive(0, ACROSS, (beyond, "y", "", 0), (beyond, "z", "e", ACROSS))
        else:
            receive(ACROSS, SPREAD, (beyond, "z", "e", 0))
            receive(0, ACROSS, (beyond, "y", "", 0))

    def build(t):
        pairs(0, 0, PARTS)
        join(0)
        own(0, t)

    def role_right_low():
        build(A)
        if third:
            receive(0, SPREAD, (C, "z", "ey", 0))
            receive(0, SPREAD, (E, "y", "", 0))
        else:
            exchange(C, D, E)

    def role_right_high():
        build(C)
        if third:
            receive(0, SPREAD, (A, "z", "e", 0), (E, "y", "", 0))
        else:
            exchange(A, E, D)

    def role_left_low():
        if third:
            receive(0, SPREAD, (A, "y", "m", 0), (E, "z", "ey", 0))
            receive(0, SPREAD - HALVE, (C, "y", "", 0))
            receive(0, HALVE, (C, "y", "", SPREAD - HALVE), (D, "z", "ey", 0))
        else:
            build(D)
            exchange(E, A, C)

    def role_left_high():
        if third:
            pairs(0, 0, PARTS)
            pairs(1, 0, PARTS // 8)
            join(0)
            own(0, E)
            pairs(1, PARTS // 8, PARTS)
            join(1)
            own(1, D)
            receive(0, SPREAD, (A, "z", "e", 0))
            receive(0, SPREAD, (C, "y", "", 0))
        else:
            build(E)
            exchange(D, C, A)

    def last_right_low():
        receive(HALVE, SPREAD, (D, "z", "ey", 0))
        receive(0, HALVE, (D, "y", "", 0))

    def last_right_high():
        receive(HALVE, SPREAD, (D, "y", "m", 0))
        receive(0, HALVE, (D, "y", "", 0))

    def last_left_low():
        receive(HALVE, SPREAD, (D, "y", "", 0))

    drains = []

    def play(roles):
        for at_y, at_group, role in roles:
            sent.clear()
            here = jnp.logical_and(y == at_y, group == at_group)
            pl.when(here)(role)
            drains.append((here, list(sent)))

    def columns(block):
        return pl.ds(pl.multiple_of(block * half, half), half)

    zeros = matching(roots, 0)
    ones = matching(roots, 1)
    source = []
    for k in range(roots.shape[0]):
        high = jnp.where(ones[k][1] == 2, D, C + 2 * ones[k][1])
        at = jnp.where(zeros[k][0] == 1, A + 2 * zeros[k][1], high)
        source.append(jnp.minimum(at, 3))

    def first():
        def turn(i):
            picked = []
            for c in range(2):
                one = branches[A, c, :, columns(core)]
                two = branches[C, c, :, columns(core)]
                if third:
                    picked.append(jnp.where(jnp.full(one.shape, source[0], jnp.int32) == A, one, two))
                else:
                    picked.append(branches[source[0], c, :, columns(core)])
            real, imag = complex_product(stems[i, 0], stems[i, 1], *picked)
            net1[i, 0] = real.astype(BF16)
            net1[i, 1] = imag.astype(BF16)

        each(2, turn)

    play([(1, 0, role_right_low), (1, 1, role_right_high), (0, 0, role_left_low), (0, 1, role_left_high)])
    stem_share.wait()
    for t in (A, C):
        core_copy(t, 0, SPREAD).wait_recv()
    if third:
        first()
        play([(1, 0, last_right_low), (1, 1, last_right_high), (0, 0, last_left_low)])
    for t in (D, E):
        core_copy(t, 0, SPREAD).wait_recv()
    for c in range(2):
        final[c] = branches[source[3], c]
    last_copy = pltpu.make_async_copy(final, last_out, local_sem.at[2])
    last_copy.start()
    if not third:
        first()

    def exchange_copy(i):
        at = pl.ds(pl.multiple_of(i * TILE, TILE), TILE)
        return remote(net2.at[core, :, at], net2.at[core, :, at], swap_s, swap_r.at[i], other)

    def second(i):
        at = pl.ds(pl.multiple_of(i * TILE, TILE), TILE)
        real, imag = complex_product(
            jnp.concatenate([net1[0, 0, at], net1[1, 0, at]], axis=1),
            jnp.concatenate([net1[0, 1, at], net1[1, 1, at]], axis=1),
            branches[source[1], 0], branches[source[1], 1],
        )
        net2[core, 0, at] = real.astype(BF16)
        net2[core, 1, at] = imag.astype(BF16)
        exchange_copy(i).start()

    tiles = net2.shape[2] // TILE
    each(tiles, second)

    def net_copy(i):
        return pltpu.make_async_copy(net3.at[i], net_out.at[i], local_sem.at[3 * i])

    def third_step(i):
        whose = core + i * (1 - 2 * core)

        @pl.when(i == 1)
        def _():
            each(tiles, lambda j: exchange_copy(j).wait_recv())

        real, imag = complex_product(
            net2[whose, 0], net2[whose, 1],
            branches[source[2], 0, :, columns(core)], branches[source[2], 1, :, columns(core)],
        )
        net3[whose, 0] = real.astype(BF16)
        net3[whose, 1] = imag.astype(BF16)

        @pl.when(i == 0)
        def _():
            net_copy(core).start()

    each(2, third_step)
    net_copy(1 - core).start()
    net_copy(core).wait()
    net_copy(1 - core).wait()
    remote(net2.at[core], net2.at[core], swap_s, swap_r.at[0], other).wait_send()
    last_copy.wait()

    def drain(e):
        place = half_pair(e)
        remote(place, place, pair_s.at[e], pair_r.at[e, 0], over_z).wait_send()
        remote(place, place, whole_s.at[e], whole_r.at[e], other).wait_send()

    def drain_leaf(e):
        place = arrived.at[e, :, own_rows()]
        remote(outgoing.at[e], place, leaf_s.at[e], leaf_r.at[e, 0], over_y).wait_send()

    @pl.when(y == 0)
    def _():
        drain_leaf(0)

        @pl.when(left)
        def _():
            for e in range(sets):
                drain(e)

    @pl.when(y == 1)
    def _():
        drain(0)

        @pl.when(left)
        def _():
            for e in range(sets):
                drain_leaf(e)

    for here, copies in drains:
        totals = {}
        for copy, t, (low, high) in copies:
            totals[copy, t] = totals.get((copy, t), 0) + high - low

        @pl.when(here)
        def _(totals=totals):
            for (copy, t), n in totals.items():
                if copy not in (mid_copy, end_copy):
                    copy(t, 0, n).wait_send()

            @pl.when(inner)
            def _():
                for (copy, t), n in totals.items():
                    if copy in (mid_copy, end_copy):
                        copy(t, 0, n).wait_send()


def general(stem_tensor, leaves, root_devices, mode_orders):
    _, rows, width = stem_tensor.shape
    half = width // 2
    part = half // CHUNKS
    groups = lax.axis_size("wide") // GROUP
    rounds = groups.bit_length() - 1
    vmem = pltpu.VMEM
    dma = pltpu.SemaphoreType.DMA
    network, last = pl.pallas_call(
        functools.partial(kernel, rounds),
        out_shape=(
            jax.ShapeDtypeStruct((2, 2, rows, half), BF16),
            jax.ShapeDtypeStruct((2, width, width), BF16),
        ),
        in_specs=[pl.BlockSpec(memory_space=pltpu.SMEM)] * 2
        + [pl.BlockSpec(memory_space=pl.ANY)] * 2,
        out_specs=[pl.BlockSpec(memory_space=pl.ANY)] * 2,
        scratch_shapes=[
            vmem((2, 2, 2, width, width), BF16),
            vmem((2, 2, half, width), BF16),
            vmem((2, half, width), BF16),
            vmem((2, width, width), BF16),
            vmem((width, width), BF16),
            vmem((max(rounds, 1), CHUNKS, 2, part, width), BF16),
            vmem((max(rounds, 1), CHUNKS, 2, part, width), BF16),
            vmem((GROUP, 2, width, width), BF16),
            vmem((2, rows, width), F32),
            vmem((2, 2, rows, half), BF16),
            vmem((2, rows, width), BF16),
            vmem((2, 2, rows, half), BF16),
            vmem((2, 2, rows, half), BF16),
            dma((5,)),
            dma((2,)), dma((2,)), dma((2,)), dma((2,)),
            dma, dma, dma, dma,
            dma((max(rounds, 1), CHUNKS)), dma((max(rounds, 1), CHUNKS)),
            dma((CHUNKS,)), dma((CHUNKS,)),
            dma((2, CHUNKS)), dma((2, CHUNKS)),
            dma((4, CHUNKS)), dma((4, CHUNKS)),
            dma((2,)), dma((2,)),
        ],
        compiler_params=pltpu.CompilerParams(collective_id=0, has_side_effects=True),
    )(root_devices, mode_orders, stem_tensor, leaves)
    return network, last


def closing(network, last, stem_tensor):
    _, rows, width = stem_tensor.shape
    half = width // 2
    return pl.pallas_call(
        finish,
        grid=(rows // half,),
        out_shape=jax.ShapeDtypeStruct(stem_tensor.shape, F32),
        in_specs=[
            pl.BlockSpec((2, 2, half, half), lambda i: (0, 0, i, 0)),
            pl.BlockSpec((2, width, width), lambda i: (0, 0, 0)),
        ],
        out_specs=pl.BlockSpec((2, half, width), lambda i: (0, i, 0)),
    )(network, last)


def split(third, stem_tensor, leaves, root_devices, mode_orders):
    _, rows, width = stem_tensor.shape
    half = width // 2
    sets = 2 if third else 1
    vmem = pltpu.VMEM
    dma = pltpu.SemaphoreType.DMA
    return pl.pallas_call(
        functools.partial(two_groups, third),
        out_shape=(
            jax.ShapeDtypeStruct((2, 2, rows, half), BF16),
            jax.ShapeDtypeStruct((2, width, width), BF16),
        ),
        in_specs=[pl.BlockSpec(memory_space=pl.ANY)] * 4,
        out_specs=[pl.BlockSpec(memory_space=pl.ANY)] * 2,
        scratch_shapes=[
            pltpu.SMEM(root_devices.shape, jnp.int32),
            pltpu.SMEM(mode_orders.shape, jnp.int32),
            vmem((leaves.shape[1], 2, width, width), BF16),
            vmem((sets, 2, half, width), BF16),
            vmem((sets, 2, width, width), BF16),
            vmem((sets, 2, width, width), BF16),
            vmem((width, width), BF16),
            vmem((sets, 2, 2, width, width), BF16),
            vmem((4, 2, width, width), BF16),
            vmem((2, rows, width), F32),
            vmem((2, 2, rows, width), BF16),
            vmem((2, 2, rows, half), BF16),
            vmem((2, 2, rows, width), BF16),
            vmem((2, 2, rows, half), BF16),
            vmem((2, width, width), BF16),
            dma((4,)),
        ]
        + [dma((sets,)), dma((sets, PARTS)), dma((sets,)), dma((sets, PARTS)), dma((sets,)), dma((sets,))]
        + [dma((4,)), dma((4, SPREAD)), dma((4,)), dma((4,)), dma((4,)), dma((4,)), dma((4, SPREAD))]
        + [dma, dma, dma, dma((rows // TILE,))],
        compiler_params=pltpu.CompilerParams(collective_id=2 if third else 1, has_side_effects=True),
    )(root_devices, mode_orders, stem_tensor, leaves)


def local(stem_tensor, leaves, root_devices, mode_orders):
    arrays = (stem_tensor, leaves, root_devices, mode_orders)
    if lax.axis_size("wide") // GROUP == 2:
        even = jnp.sum((root_devices // GROUP).astype(jnp.int32)) == 2
        network, last = lax.cond(
            even, functools.partial(split, False), functools.partial(split, True), *arrays
        )
    else:
        network, last = general(*arrays)
    return closing(network, last, stem_tensor)


def solution(mesh):
    stem_spec = P(None, ("cuts", "wide", "narrow"), None)
    return jax.shard_map(
        local,
        mesh=mesh,
        in_specs=(stem_spec, P(("cuts", "wide"), None, None, None, None), P(), P()),
        out_specs=stem_spec,
        check_vma=False,
    )
```
